32 devices in a mesh: tm: 8 (over z, y), chan: 4 (over x, core).
Axes of the slice: x: 2, y: 2, z: 4, core: 2. Of those that a mesh axis runs over, the one named last changes fastest.
Arguments:
- coarse: bfloat16 [2, 24576, 4096], P(None, 'tm', 'chan'), may hold values from -6 to 6
- prototype: float32 [16, 1024], replicated, may hold values from -4 to 4
- req_block: int32 [4, 4], replicated, may hold values from 0 to 31, as said below
- req_start: int32 [4, 4], replicated, may hold values from 0 to 8, as said below
- req_frames: int32 [4, 4], replicated, may hold values from 1 to 9
- req_count: int32 [4], replicated, may hold values from 1 to 4, as said below
Outputs:
- spectra: bfloat16 [24, 4, 4, 2, 1024, 128], P('tm', 'chan')
The draws below stay inside these ranges and needn't reach their ends.
Inputs may be any that keep to these rules, and one draw needn't show every extreme that they name: `req_block`: among the live slots of one owner at most 2 name blocks b with the same b // 8; in every draw some owner reaches 2. req_start + req_frames <= 9 in every slot; in every draw some live slot starts at hop 9 - 1 and some live slot spans all 9 frames. Slots q < req_count[c] of owner c are live, the others are empty; in every draw some owner has 4 live slots.
All inputs are finite; a program needn't handle non-finite values.
Results may differ from the reference program's by a relative error of at most 0.001.
Values may be sent and summed in bfloat16 or wider, within the bound.
A program may use at most 256 MiB of HBM per device.

```python
import math
import jax
import jax.numpy as jnp
from jax import lax

CHANNELS = 4096
BLOCKW = 128
NFINE = 1024
TAPS = 16
MAXREQ = 4
PAIR = 2
OWNERS = 4
BPC = 8
TOTHOPS = 24
TIME = 24576
FRMAX = 9


def request_tables(key):
    count_key = jax.random.fold_in(key, 101)
    full_key = jax.random.fold_in(key, 102)
    base_key = jax.random.fold_in(key, 103)
    order_key = jax.random.fold_in(key, 104)
    inner_key = jax.random.fold_in(key, 105)
    frame_key = jax.random.fold_in(key, 106)
    start_key = jax.random.fold_in(key, 107)
    other_key = jax.random.fold_in(key, 108)
    lower_key = jax.random.fold_in(key, 109)
    owner_line = jnp.arange(OWNERS)
    slot_line = jnp.arange(MAXREQ)
    counts = jax.random.randint(count_key, (OWNERS,), 1, MAXREQ + 1)
    fullest = jax.random.randint(full_key, (), 0, OWNERS)
    smaller = (fullest + 1 + jax.random.randint(other_key, (), 0, OWNERS - 1)) % OWNERS
    lower_count = jax.random.randint(lower_key, (), 1, MAXREQ)
    counts = jnp.where(owner_line == smaller, lower_count, counts)
    counts = jnp.where(owner_line == fullest, MAXREQ, counts).astype(jnp.int32)
    bases = jax.random.randint(base_key, (OWNERS, 1), 0, OWNERS)
    order_keys = jax.random.split(order_key, OWNERS)
    orders = jax.vmap(lambda single: jax.random.permutation(single, MAXREQ))(order_keys)
    sources = (bases + orders // PAIR) % OWNERS
    blocks = (sources * BPC + jax.random.randint(inner_key, (OWNERS, MAXREQ), 0, BPC)).astype(jnp.int32)
    frames = jax.random.randint(frame_key, (OWNERS, MAXREQ), 1, FRMAX + 1)
    starts = jax.random.randint(start_key, (OWNERS, MAXREQ), 0, FRMAX + 1 - frames)
    is_full = owner_line[:, None] == fullest
    last_slot = is_full & (slot_line[None, :] == 0)
    whole_slot = is_full & (slot_line[None, :] == 1)
    frames = jnp.where(last_slot, 1, frames)
    frames = jnp.where(whole_slot, FRMAX, frames).astype(jnp.int32)
    starts = jnp.where(last_slot, FRMAX - 1, starts)
    starts = jnp.where(whole_slot, 0, starts).astype(jnp.int32)
    return (blocks, starts, frames, counts)


def draw_req_block(key, part):
    return request_tables(key)[0]


def draw_req_start(key, part):
    return request_tables(key)[1]


def draw_req_frames(key, part):
    return request_tables(key)[2]


def draw_req_count(key, part):
    return request_tables(key)[3]


def block_levels(own_key, extent, cuts, least, top_value):
    def one(dim, blocks):
        heights = jax.random.uniform(jax.random.fold_in(jax.random.fold_in(own_key, 6), dim), (blocks,), jnp.float32, least / len(cuts), top_value / len(cuts))
        return jnp.repeat(jnp.exp(heights), extent[dim] // blocks).reshape((-1,) + (1,) * (len(extent) - dim - 1))

    gain = one(*cuts[0])
    for cut in cuts[1:]:
        gain = gain * one(*cut)
    return gain


def scatter_about(key, extent, width, limit, cuts=(), kind=jnp.bfloat16):
    level = block_levels(key, extent, cuts, -0.22, 0.18) if cuts else 1.0
    values = jax.random.normal(key, extent, jnp.float32) * width * level
    return jnp.minimum(jnp.maximum(values, -limit), limit).astype(kind)


def setup_inputs(seed: int = 0) -> dict:
    seeds = jax.random.split(jax.random.key(seed), 7)
    return {
        "coarse": scatter_about(seeds[0], (2, TIME, CHANNELS), 1.0, 6.0, ((1, 8), (2, 4))),
        "prototype": scatter_about(seeds[1], (TAPS, NFINE), (TAPS ** -0.5), 4.0, (), jnp.float32),
        "req_block": draw_req_block(jax.random.fold_in(seeds[6], 71), 0),
        "req_start": draw_req_start(jax.random.fold_in(seeds[6], 71), 0),
        "req_frames": draw_req_frames(jax.random.fold_in(seeds[6], 71), 0),
        "req_count": draw_req_count(jax.random.fold_in(seeds[6], 71), 0),
    }


def reference(coarse, prototype, req_block, req_start, req_frames, req_count):
    hop_ids = jnp.arange(TOTHOPS, dtype=jnp.int32)
    results = []
    for owner in range(OWNERS):
        for slot_index in range(MAXREQ):
            first_col = (req_block[owner, slot_index] * BLOCKW).astype(jnp.int32)
            block_data = lax.dynamic_slice(coarse, (jnp.int32(0), jnp.int32(0), first_col), (2, TIME, BLOCKW))
            block_data = block_data.astype(jnp.float32).reshape(2, TOTHOPS, NFINE, BLOCKW)
            padding = jnp.zeros((2, TAPS - 1, NFINE, BLOCKW), jnp.float32)
            padded = jnp.concatenate([block_data, padding.astype(block_data.dtype)], axis=1)
            filtered = jnp.zeros((2, TOTHOPS, NFINE, BLOCKW), block_data.dtype)
            for tap_index in range(TAPS):
                weights = prototype[tap_index][None, None, :, None]
                filtered = filtered + weights * padded[:, tap_index:tap_index + TOTHOPS]
            transformed = jnp.fft.fft(filtered[0] + 1j * filtered[1], axis=1) / math.sqrt(NFINE)
            stacked = jnp.stack([jnp.real(transformed), jnp.imag(transformed)], axis=1)
            begin = req_start[owner, slot_index]
            active = (slot_index < req_count[owner]) & (hop_ids >= begin) & (hop_ids < begin + req_frames[owner, slot_index])
            masked = jnp.where(active[:, None, None, None], stacked, jnp.zeros_like(stacked))
            results.append(masked.astype(jnp.bfloat16))
    spectra = jnp.stack(results, axis=1)
    return spectra.reshape(TOTHOPS, OWNERS, MAXREQ, 2, NFINE, BLOCKW)
```

```python
import functools
import math

import jax
import jax.numpy as jnp
import numpy as np
from jax import lax
from jax.experimental import pallas as pl
from jax.experimental.pallas import tpu as pltpu
from jax.sharding import PartitionSpec as P

BLOCKW = 128
NFINE = 1024
TAPS = 16
MAXREQ = 4
PAIR = 2
ROWS = 128
STEP = 16
ANY = pl.BlockSpec(memory_space=pl.ANY)


def build_table():
    line = jnp.arange(NFINE, dtype=jnp.int32)
    products = line[:, None] * line[None, :] % NFINE
    angles = products.astype(jnp.float32) * (2.0 * math.pi / NFINE)
    scale = 1.0 / math.sqrt(NFINE)
    return jnp.concatenate([jnp.cos(angles) * scale, jnp.sin(angles) * scale], axis=0)


def pack_kernel(chosen, coarse_ref, out_ref):
    out_ref[...] = coarse_ref[...].reshape(out_ref.shape)


def pack(coarse, chosen, first, hops):
    count = chosen.shape[0]
    return pl.pallas_call(
        pack_kernel,
        out_shape=jax.ShapeDtypeStruct((count, 2, hops * NFINE, BLOCKW), coarse.dtype),
        grid_spec=pltpu.PrefetchScalarGridSpec(
            num_scalar_prefetch=1,
            grid=(count,),
            in_specs=[pl.BlockSpec((2, hops * NFINE, BLOCKW), lambda i, c: (0, first, c[i]))],
            out_specs=pl.BlockSpec((1, 2, hops * NFINE, BLOCKW), lambda i, c: (i, 0, 0, 0)),
        ),
        cost_estimate=pl.CostEstimate(
            flops=0, transcendentals=0, bytes_accessed=count * 8 * hops * NFINE * BLOCKW
        ),
    )(chosen, coarse)


def select_kernel(pieces, arrival, in_ref, out_ref):
    share = BLOCKW // pieces
    for piece in range(pieces):
        cols = slice(piece * share, (piece + 1) * share)
        out_ref[piece] = jnp.concatenate([in_ref[0, 0, :, cols], in_ref[0, 1, :, cols]], axis=-1)


def select(incoming, arrival, pieces, hops):
    width = 2 * BLOCKW // pieces
    rows = hops * NFINE
    return pl.pallas_call(
        functools.partial(select_kernel, pieces),
        out_shape=jax.ShapeDtypeStruct((MAXREQ * pieces, rows, width), incoming.dtype),
        grid_spec=pltpu.PrefetchScalarGridSpec(
            num_scalar_prefetch=1,
            grid=(MAXREQ, hops),
            in_specs=[pl.BlockSpec((1, 2, NFINE, BLOCKW), lambda q, h, a: (a[q], 0, h, 0))],
            out_specs=pl.BlockSpec((pieces, NFINE, width), lambda q, h, a: (q, h, 0)),
        ),
        cost_estimate=pl.CostEstimate(
            flops=0, transcendentals=0, bytes_accessed=MAXREQ * 8 * rows * BLOCKW
        ),
    )(arrival, incoming)


def exchange_kernel(
    owners, size, a_in, b_in, a_out, b_out, a_tmp, b_tmp, a_send, a_recv, b_send, b_recv, local
):
    column, row = lax.axis_index("chan"), lax.axis_index("tm")
    barrier = pltpu.get_barrier_semaphore()

    @pl.loop(1, owners)
    def _(step):
        other = lax.rem(column + step, owners)
        pl.semaphore_signal(barrier, inc=1, device_id={"chan": other})

    @pl.loop(1, size)
    def _(step):
        other = lax.rem(row + step, size)
        pl.semaphore_signal(barrier, inc=1, device_id={"tm": other})

    pl.semaphore_wait(barrier, owners + size - 2)

    def a_copy(step, source, target, device):
        return pltpu.make_async_remote_copy(
            src_ref=a_in.at[pl.ds(target * PAIR, PAIR)],
            dst_ref=a_out.at[pl.ds(source * PAIR, PAIR)],
            send_sem=a_send.at[step],
            recv_sem=a_recv.at[step],
            device_id={"chan": device},
        )

    def b_copy(step, source, target, device):
        return pltpu.make_async_remote_copy(
            src_ref=b_in.at[target],
            dst_ref=b_out.at[source],
            send_sem=b_send.at[step],
            recv_sem=b_recv.at[step],
            device_id={"tm": device},
        )

    @pl.loop(1, size)
    def _(step):
        target = lax.rem(row + step, size)
        b_copy(step, row, target, target).start()

    @pl.loop(1, owners)
    def _(step):
        target = lax.rem(column + step, owners)
        a_copy(step, column, target, target).start()

    a_read = pltpu.make_async_copy(a_in.at[pl.ds(column * PAIR, PAIR)], a_tmp, local.at[0])
    b_read = pltpu.make_async_copy(b_in.at[row], b_tmp, local.at[1])
    a_read.start()
    b_read.start()
    a_read.wait()
    b_read.wait()
    a_write = pltpu.make_async_copy(a_tmp, a_out.at[pl.ds(column * PAIR, PAIR)], local.at[2])
    b_write = pltpu.make_async_copy(b_tmp, b_out.at[row], local.at[3])
    a_write.start()
    b_write.start()
    a_write.wait()
    b_write.wait()

    @pl.loop(1, owners)
    def _(step):
        source = lax.rem(column + owners - step, owners)
        copy = a_copy(step, source, column, source)
        copy.wait_recv()
        copy.wait_send()

    @pl.loop(1, size)
    def _(step):
        source = lax.rem(row + size - step, size)
        copy = b_copy(step, source, row, source)
        copy.wait_recv()
        copy.wait_send()


def exchange(outgoing, sending, owners, size, collective):
    sem = pltpu.SemaphoreType.DMA
    return pl.pallas_call(
        functools.partial(exchange_kernel, owners, size),
        out_shape=(
            jax.ShapeDtypeStruct(outgoing.shape, outgoing.dtype),
            jax.ShapeDtypeStruct(sending.shape, sending.dtype),
        ),
        in_specs=[ANY, ANY],
        out_specs=(ANY, ANY),
        scratch_shapes=[
            pltpu.VMEM((PAIR,) + outgoing.shape[1:], outgoing.dtype),
            pltpu.VMEM(sending.shape[1:], sending.dtype),
            sem((owners,)),
            sem((owners,)),
            sem((size,)),
            sem((size,)),
            sem((4,)),
        ],
        compiler_params=pltpu.CompilerParams(collective_id=collective, has_side_effects=True),
    )(outgoing, sending)


def filter_kernel(hops, frames, weights_ref, *refs):
    out_ref = refs[-1]
    width = refs[0].shape[-1]

    @pl.loop(0, ROWS // STEP)
    def _(step):
        rows = pl.ds(pl.multiple_of(step * STEP, STEP), STEP)
        weights = [
            jnp.broadcast_to(weights_ref[rows, tap : tap + 1], (STEP, width)) for tap in range(TAPS)
        ]
        for frame in range(frames):
            total = None
            for tap in range(TAPS):
                hop = frame + tap
                term = weights[tap] * refs[hop % hops][hop // hops, rows, :].astype(jnp.float32)
                total = term if total is None else total + term
            out_ref[rows, frame * width : (frame + 1) * width] = total


def polyphase(parts, prototype, frames):
    hops = len(parts)
    size, _, width = parts[0].shape
    return pl.pallas_call(
        functools.partial(filter_kernel, hops, frames),
        out_shape=jax.ShapeDtypeStruct((NFINE, frames * width), jnp.float32),
        grid=(NFINE // ROWS,),
        in_specs=[pl.BlockSpec((ROWS, TAPS), lambda i: (i, 0))]
        + [pl.BlockSpec((size, ROWS, width), lambda i: (0, i, 0))] * hops,
        out_specs=pl.BlockSpec((ROWS, frames * width), lambda i: (i, 0)),
    )(prototype.T, *parts)


def combine_kernel(frames, share, both_ref, out_ref):
    frame = pl.program_id(0)

    @pl.when(frame < frames)
    def _():
        sine = both_ref[1]
        turned = jnp.concatenate([sine[:, share:], -sine[:, :share]], axis=-1)
        out_ref[0] = (both_ref[0] + turned).astype(out_ref.dtype)

    @pl.when(frame >= frames)
    def _():
        out_ref[...] = jnp.zeros_like(out_ref)


def combine(both, frames, padded, width):
    return pl.pallas_call(
        functools.partial(combine_kernel, frames, width // 2),
        out_shape=jax.ShapeDtypeStruct((padded, NFINE, width), jnp.bfloat16),
        grid=(padded,),
        in_specs=[
            pl.BlockSpec((2, NFINE, width), lambda f: (0, 0, jnp.minimum(f, frames - 1))),
        ],
        out_specs=pl.BlockSpec((1, NFINE, width), lambda f: (f, 0, 0)),
    )(both)


def return_kernel(size, keepers, hops, res_ref, out_ref, send_sems, recv_sems):
    me = lax.axis_index("tm")
    barrier = pltpu.get_barrier_semaphore()

    @pl.loop(1, size)
    def _(step):
        other = lax.rem(me + step, size)
        pl.semaphore_signal(barrier, inc=1, device_id={"tm": other})

    pl.semaphore_wait(barrier, size - 1)

    def copy(step):
        target = lax.rem(me + step, size)
        return pltpu.make_async_remote_copy(
            src_ref=res_ref.at[pl.ds(target * hops, hops)],
            dst_ref=out_ref.at[me],
            send_sem=send_sems.at[step],
            recv_sem=recv_sems.at[step],
            device_id={"tm": target},
        )

    def arriving(step):
        source = lax.rem(me + size - step, size)
        return pltpu.make_async_remote_copy(
            src_ref=res_ref.at[pl.ds(0, hops)],
            dst_ref=out_ref.at[source],
            send_sem=send_sems.at[step],
            recv_sem=recv_sems.at[step],
            device_id={"tm": source},
        )

    @pl.loop(1, size)
    def _(step):
        @pl.when(lax.rem(me + step, size) < keepers)
        def _():
            copy(step).start()

    @pl.when(me < keepers)
    def _():
        @pl.loop(1, size)
        def _(step):
            arriving(step).wait_recv()

    @pl.loop(1, size)
    def _(step):
        @pl.when(lax.rem(me + step, size) < keepers)
        def _():
            copy(step).wait_send()


def give_back(result, size, keepers, hops):
    shape = (size, hops) + result.shape[1:]
    return pl.pallas_call(
        functools.partial(return_kernel, size, keepers, hops),
        out_shape=jax.ShapeDtypeStruct(shape, result.dtype),
        in_specs=[ANY],
        out_specs=ANY,
        scratch_shapes=[pltpu.SemaphoreType.DMA((size,)), pltpu.SemaphoreType.DMA((size,))],
        compiler_params=pltpu.CompilerParams(collective_id=0, has_side_effects=True),
    )(result)


def final_kernel(pieces, meta, got_ref, own_ref, out_ref):
    share = BLOCKW // pieces
    slot, hop = pl.program_id(0), pl.program_id(1)
    row = meta[0]
    active = meta[2 + slot * pl.num_programs(1) + hop] > 0

    @pl.when(jnp.logical_not(active))
    def _():
        out_ref[...] = jnp.zeros_like(out_ref)

    @pl.when(active)
    def _():
        data = [
            jnp.where(slot * pieces + piece == row, own_ref[0], got_ref[piece, 0])
            for piece in range(pieces)
        ]
        for part in range(2):
            cols = slice(part * share, (part + 1) * share)
            out_ref[0, 0, part] = jnp.concatenate([d[:, cols] for d in data], axis=-1)


def assemble(got, result, active, row, keepers, pieces):
    size, hops, _, width = got.shape
    base = jnp.minimum(row, keepers - 1) * hops
    meta = jnp.concatenate(
        [jnp.stack([row, base]).astype(jnp.int32), active.astype(jnp.int32).reshape(-1)]
    )
    return pl.pallas_call(
        functools.partial(final_kernel, pieces),
        out_shape=jax.ShapeDtypeStruct((hops, MAXREQ, 2, NFINE, BLOCKW), got.dtype),
        grid_spec=pltpu.PrefetchScalarGridSpec(
            num_scalar_prefetch=1,
            grid=(MAXREQ, hops),
            in_specs=[
                pl.BlockSpec((pieces, 1, NFINE, width), lambda q, h, m: (q, h, 0, 0)),
                pl.BlockSpec((1, NFINE, width), lambda q, h, m: (m[1] + h, 0, 0)),
            ],
            out_specs=pl.BlockSpec((1, 1, 2, NFINE, BLOCKW), lambda q, h, m: (h, q, 0, 0, 0)),
        ),
    )(meta, got, result)


def shards_general(coarse, prototype, req_block, req_start, req_frames, req_count):
    owners = lax.axis_size("chan")
    column = lax.axis_index("chan")
    row = lax.axis_index("tm")
    size = lax.axis_size("tm")
    per_column = coarse.shape[2] // BLOCKW
    hops = coarse.shape[1] // NFINE
    all_hops = hops * size
    frames = all_hops - TAPS + 1
    keepers = -(-frames // hops)
    pieces = size // MAXREQ
    width = 2 * BLOCKW // pieces
    share = BLOCKW // pieces

    slot_ids = jnp.arange(MAXREQ, dtype=jnp.int32)
    live = slot_ids[None, :] < req_count[:, None]
    sources = req_block // per_column
    same = (
        live[:, :, None]
        & live[:, None, :]
        & (sources[:, :, None] == sources[:, None, :])
        & (slot_ids[None, None, :] < slot_ids[None, :, None])
    )
    rank = jnp.sum(same.astype(jnp.int32), axis=2)
    picked = (
        (live & (sources == column))[:, None, :]
        & (rank[:, None, :] == jnp.arange(PAIR, dtype=jnp.int32)[None, :, None])
    )
    local = req_block - column * per_column
    chosen = jnp.sum(jnp.where(picked, local[:, None, :], 0), axis=2).reshape(-1)
    chosen = jnp.clip(chosen, 0, per_column - 1).astype(jnp.int32)
    mine = (jnp.arange(owners, dtype=jnp.int32) == column)[:, None]

    def own(table):
        return jnp.sum(jnp.where(mine, table, 0), axis=0)

    my_live = slot_ids < own(req_count[:, None])[0]
    arrival = jnp.where(my_live, own(sources) * PAIR + own(rank), 0)
    arrival = jnp.clip(arrival, 0, owners * PAIR - 1).astype(jnp.int32)
    my_start, my_frames = own(req_start), own(req_frames)
    hop_ids = row * hops + jnp.arange(hops, dtype=jnp.int32)
    active = (
        my_live[:, None]
        & (hop_ids[None, :] >= my_start[:, None])
        & (hop_ids[None, :] < (my_start + my_frames)[:, None])
    )

    table = build_table()
    outgoing = [pack(coarse, chosen, hop, 1) for hop in range(hops)]
    incoming = lax.all_to_all(outgoing[0], "chan", split_axis=0, concat_axis=0, tiled=True)
    parts = []
    for hop in range(1, hops):
        sending = select(incoming, arrival, pieces, 1)
        incoming, gathered = exchange(outgoing[hop], sending, owners, size, hop)
        parts.append(gathered)
    sending = select(incoming, arrival, pieces, 1)
    parts.append(lax.all_to_all(sending, "tm", split_axis=0, concat_axis=0, tiled=True))
    flat = polyphase(parts, prototype, frames)
    both = jnp.dot(table, flat, precision=lax.Precision.HIGH, preferred_element_type=jnp.float32)
    padded = keepers * hops
    if width % 128 == 0:
        result = combine(both.reshape(2, NFINE, frames * width), frames, padded, width)
    else:
        both = both.reshape(2, NFINE, frames, 2, share)
        cosine, sine = both[0], both[1]
        result = jnp.stack(
            [cosine[:, :, 0] + sine[:, :, 1], cosine[:, :, 1] - sine[:, :, 0]], axis=2
        ).astype(jnp.bfloat16)
        result = result.reshape(NFINE, frames, width).transpose(1, 0, 2)
        if padded > frames:
            zeros = jnp.zeros((padded - frames, NFINE, width), result.dtype)
            result = jnp.concatenate([result, zeros], axis=0)
    got = give_back(result, size, keepers, hops)
    return assemble(got, result, active, row, keepers, pieces)[:, None]


SMEM = pl.BlockSpec(memory_space=pltpu.SMEM)
TOP = 32767.0
RADIX = 4
SUB = NFINE // RADIX


def round_up(value, unit):
    return -(-value // unit) * unit


def tables_kernel(plan, blk, start, nfr, cnt, meta, chosen, reqs, pos, omap, columns, lists):
    row, col = lax.axis_index("tm"), lax.axis_index("chan")
    for i in range(plan.owners):
        columns[i] = 0
    for i in range(plan.keepers * plan.owners):
        lists[i] = 0
    for i in range(plan.hops * MAXREQ):
        omap[i] = -1
    for i in range(plan.fill):
        chosen[i] = 0

    def request(index, carry):
        owner, slot = lax.div(index, MAXREQ), lax.rem(index, MAXREQ)

        def add(carry):
            count, units = carry
            block = blk[owner, slot]
            source = lax.div(block, plan.per_column)
            place = columns[source]
            columns[source] = place + 1
            first = start[owner, slot]
            last = first + nfr[owner, slot]
            reqs[0, count] = source
            reqs[1, count] = place
            reqs[2, count] = first
            reqs[3, count] = last
            reqs[4, count] = units

            @pl.when(source == col)
            def _():
                chosen[place] = block - source * plan.per_column

            def frame(hop, carry):
                keeper = lax.div(hop, plan.hops)
                line = keeper * plan.owners + owner
                entry = lists[line]
                lists[line] = entry + 1
                pos[count * plan.frames + hop] = line * plan.deep + entry

                @pl.when((keeper == row) & (owner == col))
                def _():
                    omap[(hop - keeper * plan.hops) * MAXREQ + slot] = entry

                return carry

            lax.fori_loop(first, last, frame, 0)
            return count + 1, units + last - first

        return lax.cond(slot < cnt[owner], add, lambda carry: carry, carry)

    count, units = lax.fori_loop(
        0, plan.owners * MAXREQ, request, (jnp.int32(0), jnp.int32(0))
    )
    longest, deepest = jnp.int32(0), jnp.int32(0)
    for i in range(plan.owners):
        longest = jnp.maximum(longest, columns[i])
    for i in range(plan.keepers * plan.owners):
        deepest = jnp.maximum(deepest, lists[i])
    meta[0] = columns[col]
    meta[1] = count
    meta[2] = longest
    meta[3] = units
    meta[4] = deepest
    meta[5] = row


def make_tables(plan, req_block, req_start, req_frames, req_count):
    total = plan.owners * MAXREQ
    shape = lambda *dims: jax.ShapeDtypeStruct(dims, jnp.int32)
    return pl.pallas_call(
        functools.partial(tables_kernel, plan),
        out_shape=(
            shape(8),
            shape(plan.fill),
            shape(5, total),
            shape(total * plan.frames),
            shape(plan.hops * MAXREQ),
        ),
        in_specs=[SMEM] * 4,
        out_specs=(SMEM,) * 5,
        scratch_shapes=[
            pltpu.SMEM((plan.owners,), jnp.int32),
            pltpu.SMEM((plan.keepers * plan.owners,), jnp.int32),
        ],
    )(req_block, req_start, req_frames, req_count)


def gather_kernel(plan, meta, chosen, in_ref, out_ref):
    @pl.when(pl.program_id(1) < jnp.maximum(meta[0], 1))
    def _():
        for piece in range(plan.slices):
            out_ref[piece, 0, 0] = in_ref[:, piece * plan.span : (piece + 1) * plan.span, :]


def gather(plan, coarse, meta, chosen):
    def place(i, m):
        return jnp.minimum(i, jnp.maximum(m[0] - 1, 0))

    return pl.pallas_call(
        functools.partial(gather_kernel, plan),
        out_shape=jax.ShapeDtypeStruct(
            (plan.slices, plan.fill, plan.hops, 2, plan.span, BLOCKW), coarse.dtype
        ),
        grid_spec=pltpu.PrefetchScalarGridSpec(
            num_scalar_prefetch=2,
            grid=(plan.hops, plan.fill),
            in_specs=[
                pl.BlockSpec((2, NFINE, BLOCKW), lambda h, i, m, c: (0, h, c[place(i, m)]))
            ],
            out_specs=pl.BlockSpec(
                (plan.slices, 1, 1, 2, plan.span, BLOCKW),
                lambda h, i, m, c: (0, place(i, m), h, 0, 0, 0),
            ),
        ),
    )(meta, chosen, coarse)


def spread_kernel(plan, count, src, dst, tmp, send, recv, local):
    row, col = lax.axis_index("tm"), lax.axis_index("chan")
    size = plan.slices
    base = lax.div(row, plan.half) * plan.half
    me = (row - base) * plan.owners + col
    barrier = pltpu.get_barrier_semaphore()

    def device(index):
        return {"tm": base + lax.div(index, plan.owners), "chan": lax.rem(index, plan.owners)}

    order = plan.masks

    for mask in order:
        pl.semaphore_signal(barrier, inc=1, device_id=device(me ^ mask))
    pl.semaphore_wait(barrier, len(order))

    def copy(place, mask, source, target):
        return pltpu.make_async_remote_copy(
            src_ref=src.at[target, place],
            dst_ref=dst.at[source, place],
            send_sem=send.at[place, mask],
            recv_sem=recv.at[place, mask],
            device_id=device(me ^ mask),
        )

    @pl.loop(0, count)
    def _(place):
        for mask in order:
            copy(place, mask, me, me ^ mask).start()

    read = pltpu.make_async_copy(src.at[me, pl.ds(0, count)], tmp, local.at[0])
    read.start()
    read.wait()
    write = pltpu.make_async_copy(tmp, dst.at[me, pl.ds(0, count)], local.at[1])
    write.start()
    write.wait()

    @pl.loop(0, count)
    def _(place):
        for mask in order:
            copy(place, mask, me ^ mask, me).wait_recv()
            copy(place, mask, me, me ^ mask).wait_send()


def spread(plan, packed, count, collective):
    sem = pltpu.SemaphoreType.DMA
    return pl.pallas_call(
        functools.partial(spread_kernel, plan, count),
        out_shape=jax.ShapeDtypeStruct(packed.shape, packed.dtype),
        in_specs=[ANY],
        out_specs=ANY,
        scratch_shapes=[
            pltpu.VMEM((count,) + packed.shape[2:], packed.dtype),
            sem((count, plan.slices)),
            sem((count, plan.slices)),
            sem((2,)),
        ],
        compiler_params=pltpu.CompilerParams(collective_id=collective, has_side_effects=True),
    )(packed)


def partial_sum(plan, upper, hop, w_ref, in_ref, part):
    first = (plan.half * plan.hops if upper else 0) + plan.frames - 1
    total = None
    for index in range(plan.half * plan.hops):
        source, local = divmod(index, plan.hops)
        term = w_ref[first + index - hop] * in_ref[source, 0, 0, local, part].astype(jnp.float32)
        total = term if total is None else total + term
    return total


def encode(parts, out_ref, scale_ref, place, scale_row):
    top = jnp.max(jnp.maximum(jnp.abs(parts[0]), jnp.abs(parts[1])), axis=0, keepdims=True)
    top = jnp.maximum(top, 1e-30)
    factor = TOP / top
    for part in range(2):
        code = jnp.round(parts[part] * factor).astype(jnp.int32)
        out_ref[place, part] = code.astype(jnp.int16)
    scale_ref[pl.ds(scale_row, 1), :] = top * (1.0 / TOP)


def upper_kernel(plan, meta, reqs, in_ref, w_ref, out_ref, scale_ref):
    index = pl.program_id(0)

    @pl.when((index < meta[1]) & (meta[5] >= plan.half))
    def _():
        first, last, offset = reqs[2, index], reqs[3, index], reqs[4, index]

        @pl.loop(first, last)
        def _(hop):
            parts = [partial_sum(plan, True, hop, w_ref, in_ref, part) for part in range(2)]
            place = offset + hop - first
            encode(parts, out_ref, scale_ref, place, place)


def lower_kernel(plan, meta, reqs, pos, in_ref, w_ref, got_ref, got_scale, out_ref, scale_ref):
    index = pl.program_id(0)

    @pl.when((index < meta[1]) & (meta[5] < plan.half))
    def _():
        first, last, offset = reqs[2, index], reqs[3, index], reqs[4, index]

        @pl.loop(first, last)
        def _(hop):
            unit = offset + hop - first
            scale = got_scale[pl.ds(unit, 1), :]
            parts = []
            for part in range(2):
                other = got_ref[unit, part].astype(jnp.int32).astype(jnp.float32) * scale
                parts.append(partial_sum(plan, False, hop, w_ref, in_ref, part) + other)
            place = pos[index * plan.frames + hop]
            encode(parts, out_ref, scale_ref, place, place)


def filter_specs(plan):
    def request(i, m):
        return jnp.minimum(i, jnp.maximum(m[1] - 1, 0))

    taps = plan.frames - 1 + plan.all_hops
    return [
        pl.BlockSpec(
            (plan.half, 1, 1, plan.hops, 2, plan.span, BLOCKW),
            lambda i, m, r, *_: (0, r[0, request(i, m)], r[1, request(i, m)], 0, 0, 0, 0),
        ),
        pl.BlockSpec((taps, plan.span, BLOCKW), lambda i, *_: (0, 0, 0)),
    ]


def whole(*dims):
    return pl.BlockSpec(dims, lambda i, *_: (0,) * len(dims))


def filter_upper(plan, spreaded, weights, meta, reqs):
    units = plan.units
    return pl.pallas_call(
        functools.partial(upper_kernel, plan),
        out_shape=(
            jax.ShapeDtypeStruct((units, 2, plan.span, BLOCKW), jnp.int16),
            jax.ShapeDtypeStruct((units, BLOCKW), jnp.float32),
        ),
        grid_spec=pltpu.PrefetchScalarGridSpec(
            num_scalar_prefetch=2,
            grid=(plan.owners * MAXREQ,),
            in_specs=filter_specs(plan),
            out_specs=(whole(units, 2, plan.span, BLOCKW), whole(units, BLOCKW)),
        ),
    )(meta, reqs, spreaded, weights)


def filter_lower(plan, spreaded, weights, got, scales, meta, reqs, pos):
    units = plan.units
    rows = plan.keepers * plan.owners * plan.deep
    return pl.pallas_call(
        functools.partial(lower_kernel, plan),
        out_shape=(
            jax.ShapeDtypeStruct((rows, 2, plan.span, BLOCKW), jnp.int16),
            jax.ShapeDtypeStruct((rows, BLOCKW), jnp.float32),
        ),
        grid_spec=pltpu.PrefetchScalarGridSpec(
            num_scalar_prefetch=3,
            grid=(plan.owners * MAXREQ,),
            in_specs=filter_specs(plan)
            + [whole(units, 2, plan.span, BLOCKW), whole(units, BLOCKW)],
            out_specs=(whole(rows, 2, plan.span, BLOCKW), whole(rows, BLOCKW)),
        ),
    )(meta, reqs, pos, spreaded, weights, got, scales)


def lift_kernel(plan, count, src, src_scale, dst, dst_scale, send, recv):
    row = lax.axis_index("tm")
    barrier = pltpu.get_barrier_semaphore()
    upper = row >= plan.half
    other = jnp.where(upper, row - plan.half, row + plan.half)
    pl.semaphore_signal(barrier, inc=1, device_id={"tm": other})
    pl.semaphore_wait(barrier, 1)
    refs = [(src, dst), (src_scale, dst_scale)]
    copies = [
        pltpu.make_async_remote_copy(
            src_ref=source.at[pl.ds(0, count)],
            dst_ref=target.at[pl.ds(0, count)],
            send_sem=send.at[index],
            recv_sem=recv.at[index],
            device_id={"tm": other},
        )
        for index, (source, target) in enumerate(refs)
    ]

    @pl.when(upper)
    def _():
        for copy in copies:
            copy.start()
        for copy in copies:
            copy.wait_send()

    @pl.when(jnp.logical_not(upper))
    def _():
        for copy in copies:
            copy.wait_recv()


def lift(plan, values, scales, count, collective):
    sem = pltpu.SemaphoreType.DMA
    return pl.pallas_call(
        functools.partial(lift_kernel, plan, count),
        out_shape=(
            jax.ShapeDtypeStruct(values.shape, values.dtype),
            jax.ShapeDtypeStruct(scales.shape, scales.dtype),
        ),
        in_specs=[ANY, ANY],
        out_specs=(ANY, ANY),
        scratch_shapes=[sem((2,)), sem((2,))],
        compiler_params=pltpu.CompilerParams(collective_id=collective, has_side_effects=True),
    )(values, scales)


def deliver_kernel(plan, count, src, src_scale, dst, dst_scale, tmp, tmp_scale, send, recv, local):
    row, col = lax.axis_index("tm"), lax.axis_index("chan")
    size, lines = plan.slices, plan.keepers * plan.owners
    me = row * plan.owners + col
    barrier = pltpu.get_barrier_semaphore()

    def device(index):
        return {"tm": lax.div(index, plan.owners), "chan": lax.rem(index, plan.owners)}

    def copies(step, source, target, other):
        values = pltpu.make_async_remote_copy(
            src_ref=src.at[target, pl.ds(0, count)],
            dst_ref=dst.at[source, pl.ds(0, count)],
            send_sem=send.at[0, step],
            recv_sem=recv.at[0, step],
            device_id=device(other),
        )
        scales = pltpu.make_async_remote_copy(
            src_ref=src_scale.at[target],
            dst_ref=dst_scale.at[source],
            send_sem=send.at[1, step],
            recv_sem=recv.at[1, step],
            device_id=device(other),
        )
        return values, scales

    @pl.when(row < plan.half)
    def _():
        @pl.loop(1, size)
        def _(step):
            pl.semaphore_signal(barrier, inc=1, device_id=device(lax.rem(me + step, size)))

        pl.semaphore_wait(barrier, size - 1)

        @pl.loop(1, size)
        def _(step):
            target = lax.rem(me + step, size)

            @pl.when(target < lines)
            def _():
                for copy in copies(step, me, target, target):
                    copy.start()

        @pl.when(me < lines)
        def _():
            moves = [
                (src.at[me, pl.ds(0, count)], tmp, dst.at[me, pl.ds(0, count)]),
                (src_scale.at[me], tmp_scale, dst_scale.at[me]),
            ]
            for index, (source, middle, target) in enumerate(moves):
                read = pltpu.make_async_copy(source, middle, local.at[2 * index])
                read.start()
                read.wait()
                write = pltpu.make_async_copy(middle, target, local.at[2 * index + 1])
                write.start()
                write.wait()

            @pl.loop(1, size)
            def _(step):
                source = lax.rem(me + size - step, size)
                for copy in copies(step, source, me, source):
                    copy.wait_recv()

        @pl.loop(1, size)
        def _(step):
            target = lax.rem(me + step, size)

            @pl.when(target < lines)
            def _():
                for copy in copies(step, me, target, target):
                    copy.wait_send()


def deliver(plan, values, scales, count, collective):
    sem = pltpu.SemaphoreType.DMA
    inner = values.shape[1:]
    return pl.pallas_call(
        functools.partial(deliver_kernel, plan, count),
        out_shape=(
            jax.ShapeDtypeStruct((plan.slices,) + inner, values.dtype),
            jax.ShapeDtypeStruct((plan.slices,) + scales.shape[1:], scales.dtype),
        ),
        in_specs=[ANY, ANY],
        out_specs=(ANY, ANY),
        scratch_shapes=[
            pltpu.VMEM((count,) + inner[1:], values.dtype),
            pltpu.VMEM(scales.shape[1:], scales.dtype),
            sem((2, plan.slices)),
            sem((2, plan.slices)),
            sem((4,)),
        ],
        compiler_params=pltpu.CompilerParams(collective_id=collective, has_side_effects=True),
    )(values, scales)


def transform_kernel(plan, omap, in_ref, scale_ref, high_ref, low_ref, turn_ref, out_ref, yh, yl, zs):
    entry = omap[pl.program_id(0)]

    @pl.when(entry < 0)
    def _():
        out_ref[...] = jnp.zeros_like(out_ref)

    @pl.when(entry >= 0)
    def _():
        chunk = 32

        def load(part, first):
            piece, line = divmod(first, plan.span)
            code = in_ref[piece, 0, part, line : line + chunk, :]
            scale = scale_ref[piece, pl.ds(entry, 1), :]
            return code.astype(jnp.int32).astype(jnp.float32) * scale

        for line in range(0, SUB, chunk):
            re = [load(0, SUB * a + line) for a in range(RADIX)]
            im = [load(1, SUB * a + line) for a in range(RADIX)]
            es, ed = re[0] + re[2], re[0] - re[2]
            fs, fd = im[0] + im[2], im[0] - im[2]
            gs, gd = re[1] + re[3], re[1] - re[3]
            hs, hd = im[1] + im[3], im[1] - im[3]
            mixed = [
                (es + gs, fs + hs),
                (ed + hd, fd - gd),
                (es - gs, fs - hs),
                (ed - hd, fd + gd),
            ]
            rows = slice(line, line + chunk)
            for q in range(RADIX):
                real, imag = mixed[q]
                if q:
                    cosine, sine = turn_ref[0, q - 1, rows, :], turn_ref[1, q - 1, rows, :]
                    real, imag = real * cosine + imag * sine, imag * cosine - real * sine
                for part, value in enumerate((real, imag)):
                    cols = slice(part * BLOCKW, (part + 1) * BLOCKW)
                    high = value.astype(jnp.bfloat16)
                    yh[q, rows, cols] = high
                    yl[q, rows, cols] = (value - high.astype(jnp.float32)).astype(jnp.bfloat16)

        for q in range(RADIX):
            both = jnp.dot(high_ref[...], yh[q], preferred_element_type=jnp.float32)
            both = both + jnp.dot(high_ref[...], yl[q], preferred_element_type=jnp.float32)
            both = both + jnp.dot(low_ref[...], yh[q], preferred_element_type=jnp.float32)
            rows = pl.ds(q, SUB, stride=RADIX)
            zs[0, rows, :] = both[:SUB, :BLOCKW] + both[SUB:, BLOCKW:]
            zs[1, rows, :] = both[:SUB, BLOCKW:] - both[SUB:, :BLOCKW]

        out_ref[0, 0] = zs[...].astype(out_ref.dtype)


def transform_tables():
    line = np.arange(SUB)
    angles = (line[:, None] * line[None, :] % SUB) * (2.0 * np.pi / SUB)
    table = np.concatenate([np.cos(angles), np.sin(angles)], axis=0) / math.sqrt(NFINE)
    table = table.astype(np.float32)
    high = table.astype(jnp.bfloat16)
    low = (table - high.astype(np.float32)).astype(jnp.bfloat16)
    turns = np.arange(1, RADIX)[:, None] * line[None, :] * (2.0 * np.pi / NFINE)
    turn = np.stack([np.cos(turns), np.sin(turns)]).astype(np.float32)
    return high, low, turn


def transform(plan, values, scales, omap):
    high, low, turn = transform_tables()
    turn = jnp.broadcast_to(jnp.asarray(turn)[..., None], turn.shape + (BLOCKW,))
    return pl.pallas_call(
        functools.partial(transform_kernel, plan),
        out_shape=jax.ShapeDtypeStruct((plan.hops, MAXREQ, 2, NFINE, BLOCKW), jnp.bfloat16),
        grid_spec=pltpu.PrefetchScalarGridSpec(
            num_scalar_prefetch=1,
            grid=(plan.hops * MAXREQ,),
            in_specs=[
                pl.BlockSpec(
                    (plan.slices, 1, 2, plan.span, BLOCKW),
                    lambda i, o: (0, jnp.maximum(o[i], 0), 0, 0, 0),
                ),
                whole(*scales.shape),
                whole(2 * SUB, SUB),
                whole(2 * SUB, SUB),
                whole(2, RADIX - 1, SUB, BLOCKW),
            ],
            out_specs=pl.BlockSpec(
                (1, 1, 2, NFINE, BLOCKW), lambda i, o: (i // MAXREQ, i % MAXREQ, 0, 0, 0)
            ),
            scratch_shapes=[
                pltpu.VMEM((RADIX, SUB, 2 * BLOCKW), jnp.bfloat16),
                pltpu.VMEM((RADIX, SUB, 2 * BLOCKW), jnp.bfloat16),
                pltpu.VMEM((2, NFINE, BLOCKW), jnp.float32),
            ],
        ),
    )(omap, values, scales, jnp.asarray(high), jnp.asarray(low), turn)


def owners_power(value):
    return value & (value - 1) == 0


class Plan:
    def __init__(self, size, owners, hops, per_column):
        self.size, self.owners, self.hops, self.per_column = size, owners, hops, per_column
        self.all_hops = hops * size
        self.frames = self.all_hops - TAPS + 1
        self.keepers = -(-self.frames // hops)
        self.half = size // 2
        self.slices = self.half * owners
        self.span = NFINE // self.slices
        self.fill = owners * PAIR
        self.deep = round_up(hops * MAXREQ, 8)
        self.units = round_up(owners * MAXREQ * self.frames, 16)

        spread = sorted(range(2, self.slices), key=lambda mask: bin(mask >> 1).count("1"))
        self.masks = spread + [1]

    def fits(self):
        powers = self.slices & (self.slices - 1) == 0 and owners_power(self.owners)
        even = powers and self.size % 2 == 0 and NFINE % self.slices == 0 and self.span % 32 == 0
        return even and self.keepers <= self.half


def choose(value, sizes, build, first, *operands):
    index = sum((value > size).astype(jnp.int32) for size in sizes[:-1])
    branches = [functools.partial(build, size, first + i) for i, size in enumerate(sizes)]
    return lax.switch(index, branches, *operands)


def shards(coarse, prototype, req_block, req_start, req_frames, req_count):
    owners, size = lax.axis_size("chan"), lax.axis_size("tm")
    plan = Plan(size, owners, coarse.shape[1] // NFINE, coarse.shape[2] // BLOCKW)
    if not plan.fits():
        return shards_general(coarse, prototype, req_block, req_start, req_frames, req_count)
    meta, chosen, reqs, pos, omap = make_tables(plan, req_block, req_start, req_frames, req_count)
    packed = gather(plan, coarse, meta, chosen)

    me = lax.axis_index("tm") % plan.half * owners + lax.axis_index("chan")
    mine = lax.dynamic_slice(prototype, (0, me * plan.span), (TAPS, plan.span))
    mine = jnp.pad(mine, ((plan.frames - 1, plan.all_hops - TAPS), (0, 0)))
    weights = jnp.broadcast_to(mine[:, :, None], mine.shape + (BLOCKW,))

    fills = sorted({max(1, plan.fill * i // 8) for i in (2, 3, 4, 5, 6, 8)})
    spreaded = choose(
        meta[2], fills, lambda n, c, x: spread(plan, x, n, c), 0, packed
    )
    spreaded = spreaded.reshape((plan.half, owners) + spreaded.shape[1:])
    values, scales = filter_upper(plan, spreaded, weights, meta, reqs)
    counts = sorted({round_up(plan.units * i // 9, 16) for i in (2, 3, 4, 5, 6, 9)})
    values, scales = choose(
        meta[3], counts, lambda n, c, *x: lift(plan, *x, n, c), len(fills), values, scales
    )
    values, scales = filter_lower(plan, spreaded, weights, values, scales, meta, reqs, pos)
    lines = plan.keepers * owners
    values = values.reshape((lines, plan.deep) + values.shape[1:])
    scales = scales.reshape((lines, plan.deep) + scales.shape[1:])
    most = plan.hops * MAXREQ
    depths = sorted({-(-most * i // 12) for i in (6, 7, 8, 9, 10, 12)})
    values, scales = choose(
        meta[4],
        depths,
        lambda n, c, *x: deliver(plan, *x, n, c),
        len(fills) + len(counts),
        values,
        scales,
    )
    return transform(plan, values, scales, omap)[:, None]


def solution(mesh):
    return jax.shard_map(
        shards,
        mesh=mesh,
        in_specs=(P(None, "tm", "chan"), P(), P(), P(), P(), P()),
        out_specs=P("tm", "chan", None, None, None, None),
        check_vma=False,
    )
```

```python
import functools
import math

import jax
import jax.numpy as jnp
import numpy as np
from jax import lax
from jax.experimental import pallas as pl
from jax.experimental.pallas import tpu as pltpu
from jax.sharding import PartitionSpec as P

BLOCKW = 128
NFINE = 1024
TAPS = 16
MAXREQ = 4
PAIR = 2
ROWS = 128
STEP = 16
ANY = pl.BlockSpec(memory_space=pl.ANY)


def build_table():
    line = jnp.arange(NFINE, dtype=jnp.int32)
    products = line[:, None] * line[None, :] % NFINE
    angles = products.astype(jnp.float32) * (2.0 * math.pi / NFINE)
    scale = 1.0 / math.sqrt(NFINE)
    return jnp.concatenate([jnp.cos(angles) * scale, jnp.sin(angles) * scale], axis=0)


def pack_kernel(chosen, coarse_ref, out_ref):
    out_ref[...] = coarse_ref[...].reshape(out_ref.shape)


def pack(coarse, chosen, first, hops):
    count = chosen.shape[0]
    return pl.pallas_call(
        pack_kernel,
        out_shape=jax.ShapeDtypeStruct((count, 2, hops * NFINE, BLOCKW), coarse.dtype),
        grid_spec=pltpu.PrefetchScalarGridSpec(
            num_scalar_prefetch=1,
            grid=(count,),
            in_specs=[pl.BlockSpec((2, hops * NFINE, BLOCKW), lambda i, c: (0, first, c[i]))],
            out_specs=pl.BlockSpec((1, 2, hops * NFINE, BLOCKW), lambda i, c: (i, 0, 0, 0)),
        ),
        cost_estimate=pl.CostEstimate(
            flops=0, transcendentals=0, bytes_accessed=count * 8 * hops * NFINE * BLOCKW
        ),
    )(chosen, coarse)


def select_kernel(pieces, arrival, in_ref, out_ref):
    share = BLOCKW // pieces
    for piece in range(pieces):
        cols = slice(piece * share, (piece + 1) * share)
        out_ref[piece] = jnp.concatenate([in_ref[0, 0, :, cols], in_ref[0, 1, :, cols]], axis=-1)


def select(incoming, arrival, pieces, hops):
    width = 2 * BLOCKW // pieces
    rows = hops * NFINE
    return pl.pallas_call(
        functools.partial(select_kernel, pieces),
        out_shape=jax.ShapeDtypeStruct((MAXREQ * pieces, rows, width), incoming.dtype),
        grid_spec=pltpu.PrefetchScalarGridSpec(
            num_scalar_prefetch=1,
            grid=(MAXREQ, hops),
            in_specs=[pl.BlockSpec((1, 2, NFINE, BLOCKW), lambda q, h, a: (a[q], 0, h, 0))],
            out_specs=pl.BlockSpec((pieces, NFINE, width), lambda q, h, a: (q, h, 0)),
        ),
        cost_estimate=pl.CostEstimate(
            flops=0, transcendentals=0, bytes_accessed=MAXREQ * 8 * rows * BLOCKW
        ),
    )(arrival, incoming)


def exchange_kernel(
    owners, size, a_in, b_in, a_out, b_out, a_tmp, b_tmp, a_send, a_recv, b_send, b_recv, local
):
    column, row = lax.axis_index("chan"), lax.axis_index("tm")
    barrier = pltpu.get_barrier_semaphore()

    @pl.loop(1, owners)
    def _(step):
        other = lax.rem(column + step, owners)
        pl.semaphore_signal(barrier, inc=1, device_id={"chan": other})

    @pl.loop(1, size)
    def _(step):
        other = lax.rem(row + step, size)
        pl.semaphore_signal(barrier, inc=1, device_id={"tm": other})

    pl.semaphore_wait(barrier, owners + size - 2)

    def a_copy(step, source, target, device):
        return pltpu.make_async_remote_copy(
            src_ref=a_in.at[pl.ds(target * PAIR, PAIR)],
            dst_ref=a_out.at[pl.ds(source * PAIR, PAIR)],
            send_sem=a_send.at[step],
            recv_sem=a_recv.at[step],
            device_id={"chan": device},
        )

    def b_copy(step, source, target, device):
        return pltpu.make_async_remote_copy(
            src_ref=b_in.at[target],
            dst_ref=b_out.at[source],
            send_sem=b_send.at[step],
            recv_sem=b_recv.at[step],
            device_id={"tm": device},
        )

    @pl.loop(1, size)
    def _(step):
        target = lax.rem(row + step, size)
        b_copy(step, row, target, target).start()

    @pl.loop(1, owners)
    def _(step):
        target = lax.rem(column + step, owners)
        a_copy(step, column, target, target).start()

    a_read = pltpu.make_async_copy(a_in.at[pl.ds(column * PAIR, PAIR)], a_tmp, local.at[0])
    b_read = pltpu.make_async_copy(b_in.at[row], b_tmp, local.at[1])
    a_read.start()
    b_read.start()
    a_read.wait()
    b_read.wait()
    a_write = pltpu.make_async_copy(a_tmp, a_out.at[pl.ds(column * PAIR, PAIR)], local.at[2])
    b_write = pltpu.make_async_copy(b_tmp, b_out.at[row], local.at[3])
    a_write.start()
    b_write.start()
    a_write.wait()
    b_write.wait()

    @pl.loop(1, owners)
    def _(step):
        source = lax.rem(column + owners - step, owners)
        copy = a_copy(step, source, column, source)
        copy.wait_recv()
        copy.wait_send()

    @pl.loop(1, size)
    def _(step):
        source = lax.rem(row + size - step, size)
        copy = b_copy(step, source, row, source)
        copy.wait_recv()
        copy.wait_send()


def exchange(outgoing, sending, owners, size, collective):
    sem = pltpu.SemaphoreType.DMA
    return pl.pallas_call(
        functools.partial(exchange_kernel, owners, size),
        out_shape=(
            jax.ShapeDtypeStruct(outgoing.shape, outgoing.dtype),
            jax.ShapeDtypeStruct(sending.shape, sending.dtype),
        ),
        in_specs=[ANY, ANY],
        out_specs=(ANY, ANY),
        scratch_shapes=[
            pltpu.VMEM((PAIR,) + outgoing.shape[1:], outgoing.dtype),
            pltpu.VMEM(sending.shape[1:], sending.dtype),
            sem((owners,)),
            sem((owners,)),
            sem((size,)),
            sem((size,)),
            sem((4,)),
        ],
        compiler_params=pltpu.CompilerParams(collective_id=collective, has_side_effects=True),
    )(outgoing, sending)


def filter_kernel(hops, frames, weights_ref, *refs):
    out_ref = refs[-1]
    width = refs[0].shape[-1]

    @pl.loop(0, ROWS // STEP)
    def _(step):
        rows = pl.ds(pl.multiple_of(step * STEP, STEP), STEP)
        weights = [
            jnp.broadcast_to(weights_ref[rows, tap : tap + 1], (STEP, width)) for tap in range(TAPS)
        ]
        for frame in range(frames):
            total = None
            for tap in range(TAPS):
                hop = frame + tap
                term = weights[tap] * refs[hop % hops][hop // hops, rows, :].astype(jnp.float32)
                total = term if total is None else total + term
            out_ref[rows, frame * width : (frame + 1) * width] = total


def polyphase(parts, prototype, frames):
    hops = len(parts)
    size, _, width = parts[0].shape
    return pl.pallas_call(
        functools.partial(filter_kernel, hops, frames),
        out_shape=jax.ShapeDtypeStruct((NFINE, frames * width), jnp.float32),
        grid=(NFINE // ROWS,),
        in_specs=[pl.BlockSpec((ROWS, TAPS), lambda i: (i, 0))]
        + [pl.BlockSpec((size, ROWS, width), lambda i: (0, i, 0))] * hops,
        out_specs=pl.BlockSpec((ROWS, frames * width), lambda i: (i, 0)),
    )(prototype.T, *parts)


def combine_kernel(frames, share, both_ref, out_ref):
    frame = pl.program_id(0)

    @pl.when(frame < frames)
    def _():
        sine = both_ref[1]
        turned = jnp.concatenate([sine[:, share:], -sine[:, :share]], axis=-1)
        out_ref[0] = (both_ref[0] + turned).astype(out_ref.dtype)

    @pl.when(frame >= frames)
    def _():
        out_ref[...] = jnp.zeros_like(out_ref)


def combine(both, frames, padded, width):
    return pl.pallas_call(
        functools.partial(combine_kernel, frames, width // 2),
        out_shape=jax.ShapeDtypeStruct((padded, NFINE, width), jnp.bfloat16),
        grid=(padded,),
        in_specs=[
            pl.BlockSpec((2, NFINE, width), lambda f: (0, 0, jnp.minimum(f, frames - 1))),
        ],
        out_specs=pl.BlockSpec((1, NFINE, width), lambda f: (f, 0, 0)),
    )(both)


def return_kernel(size, keepers, hops, res_ref, out_ref, send_sems, recv_sems):
    me = lax.axis_index("tm")
    barrier = pltpu.get_barrier_semaphore()

    @pl.loop(1, size)
    def _(step):
        other = lax.rem(me + step, size)
        pl.semaphore_signal(barrier, inc=1, device_id={"tm": other})

    pl.semaphore_wait(barrier, size - 1)

    def copy(step):
        target = lax.rem(me + step, size)
        return pltpu.make_async_remote_copy(
            src_ref=res_ref.at[pl.ds(target * hops, hops)],
            dst_ref=out_ref.at[me],
            send_sem=send_sems.at[step],
            recv_sem=recv_sems.at[step],
            device_id={"tm": target},
        )

    def arriving(step):
        source = lax.rem(me + size - step, size)
        return pltpu.make_async_remote_copy(
            src_ref=res_ref.at[pl.ds(0, hops)],
            dst_ref=out_ref.at[source],
            send_sem=send_sems.at[step],
            recv_sem=recv_sems.at[step],
            device_id={"tm": source},
        )

    @pl.loop(1, size)
    def _(step):
        @pl.when(lax.rem(me + step, size) < keepers)
        def _():
            copy(step).start()

    @pl.when(me < keepers)
    def _():
        @pl.loop(1, size)
        def _(step):
            arriving(step).wait_recv()

    @pl.loop(1, size)
    def _(step):
        @pl.when(lax.rem(me + step, size) < keepers)
        def _():
            copy(step).wait_send()


def give_back(result, size, keepers, hops):
    shape = (size, hops) + result.shape[1:]
    return pl.pallas_call(
        functools.partial(return_kernel, size, keepers, hops),
        out_shape=jax.ShapeDtypeStruct(shape, result.dtype),
        in_specs=[ANY],
        out_specs=ANY,
        scratch_shapes=[pltpu.SemaphoreType.DMA((size,)), pltpu.SemaphoreType.DMA((size,))],
        compiler_params=pltpu.CompilerParams(collective_id=0, has_side_effects=True),
    )(result)


def final_kernel(pieces, meta, got_ref, own_ref, out_ref):
    share = BLOCKW // pieces
    slot, hop = pl.program_id(0), pl.program_id(1)
    row = meta[0]
    active = meta[2 + slot * pl.num_programs(1) + hop] > 0

    @pl.when(jnp.logical_not(active))
    def _():
        out_ref[...] = jnp.zeros_like(out_ref)

    @pl.when(active)
    def _():
        data = [
            jnp.where(slot * pieces + piece == row, own_ref[0], got_ref[piece, 0])
            for piece in range(pieces)
        ]
        for part in range(2):
            cols = slice(part * share, (part + 1) * share)
            out_ref[0, 0, part] = jnp.concatenate([d[:, cols] for d in data], axis=-1)


def assemble(got, result, active, row, keepers, pieces):
    size, hops, _, width = got.shape
    base = jnp.minimum(row, keepers - 1) * hops
    meta = jnp.concatenate(
        [jnp.stack([row, base]).astype(jnp.int32), active.astype(jnp.int32).reshape(-1)]
    )
    return pl.pallas_call(
        functools.partial(final_kernel, pieces),
        out_shape=jax.ShapeDtypeStruct((hops, MAXREQ, 2, NFINE, BLOCKW), got.dtype),
        grid_spec=pltpu.PrefetchScalarGridSpec(
            num_scalar_prefetch=1,
            grid=(MAXREQ, hops),
            in_specs=[
                pl.BlockSpec((pieces, 1, NFINE, width), lambda q, h, m: (q, h, 0, 0)),
                pl.BlockSpec((1, NFINE, width), lambda q, h, m: (m[1] + h, 0, 0)),
            ],
            out_specs=pl.BlockSpec((1, 1, 2, NFINE, BLOCKW), lambda q, h, m: (h, q, 0, 0, 0)),
        ),
    )(meta, got, result)


def shards_general(coarse, prototype, req_block, req_start, req_frames, req_count):
    owners = lax.axis_size("chan")
    column = lax.axis_index("chan")
    row = lax.axis_index("tm")
    size = lax.axis_size("tm")
    per_column = coarse.shape[2] // BLOCKW
    hops = coarse.shape[1] // NFINE
    all_hops = hops * size
    frames = all_hops - TAPS + 1
    keepers = -(-frames // hops)
    pieces = size // MAXREQ
    width = 2 * BLOCKW // pieces
    share = BLOCKW // pieces

    slot_ids = jnp.arange(MAXREQ, dtype=jnp.int32)
    live = slot_ids[None, :] < req_count[:, None]
    sources = req_block // per_column
    same = (
        live[:, :, None]
        & live[:, None, :]
        & (sources[:, :, None] == sources[:, None, :])
        & (slot_ids[None, None, :] < slot_ids[None, :, None])
    )
    rank = jnp.sum(same.astype(jnp.int32), axis=2)
    picked = (
        (live & (sources == column))[:, None, :]
        & (rank[:, None, :] == jnp.arange(PAIR, dtype=jnp.int32)[None, :, None])
    )
    local = req_block - column * per_column
    chosen = jnp.sum(jnp.where(picked, local[:, None, :], 0), axis=2).reshape(-1)
    chosen = jnp.clip(chosen, 0, per_column - 1).astype(jnp.int32)
    mine = (jnp.arange(owners, dtype=jnp.int32) == column)[:, None]

    def own(table):
        return jnp.sum(jnp.where(mine, table, 0), axis=0)

    my_live = slot_ids < own(req_count[:, None])[0]
    arrival = jnp.where(my_live, own(sources) * PAIR + own(rank), 0)
    arrival = jnp.clip(arrival, 0, owners * PAIR - 1).astype(jnp.int32)
    my_start, my_frames = own(req_start), own(req_frames)
    hop_ids = row * hops + jnp.arange(hops, dtype=jnp.int32)
    active = (
        my_live[:, None]
        & (hop_ids[None, :] >= my_start[:, None])
        & (hop_ids[None, :] < (my_start + my_frames)[:, None])
    )

    table = build_table()
    outgoing = [pack(coarse, chosen, hop, 1) for hop in range(hops)]
    incoming = lax.all_to_all(outgoing[0], "chan", split_axis=0, concat_axis=0, tiled=True)
    parts = []
    for hop in range(1, hops):
        sending = select(incoming, arrival, pieces, 1)
        incoming, gathered = exchange(outgoing[hop], sending, owners, size, hop)
        parts.append(gathered)
    sending = select(incoming, arrival, pieces, 1)
    parts.append(lax.all_to_all(sending, "tm", split_axis=0, concat_axis=0, tiled=True))
    flat = polyphase(parts, prototype, frames)
    both = jnp.dot(table, flat, precision=lax.Precision.HIGH, preferred_element_type=jnp.float32)
    padded = keepers * hops
    if width % 128 == 0:
        result = combine(both.reshape(2, NFINE, frames * width), frames, padded, width)
    else:
        both = both.reshape(2, NFINE, frames, 2, share)
        cosine, sine = both[0], both[1]
        result = jnp.stack(
            [cosine[:, :, 0] + sine[:, :, 1], cosine[:, :, 1] - sine[:, :, 0]], axis=2
        ).astype(jnp.bfloat16)
        result = result.reshape(NFINE, frames, width).transpose(1, 0, 2)
        if padded > frames:
            zeros = jnp.zeros((padded - frames, NFINE, width), result.dtype)
            result = jnp.concatenate([result, zeros], axis=0)
    got = give_back(result, size, keepers, hops)
    return assemble(got, result, active, row, keepers, pieces)[:, None]


SMEM = pl.BlockSpec(memory_space=pltpu.SMEM)
TOP = 32767.0
RADIX = 4
SUB = NFINE // RADIX


def round_up(value, unit):
    return -(-value // unit) * unit


def picked(value, sizes):
    return sum((value > size).astype(jnp.int32) for size in sizes[:-1])


def tables_kernel(
    plan, blk, start, nfr, cnt, meta, chosen, reqs, pos, omap, pick_a, pick_b, pick_c,
    columns, lists, order, places
):
    row, col = lax.axis_index("tm"), lax.axis_index("chan")
    total = plan.owners * MAXREQ
    for i in range(plan.owners):
        columns[i] = 0
    for i in range(plan.keepers * plan.owners):
        lists[i] = 0
    for i in range(plan.hops * MAXREQ):
        omap[i] = -1
    for i in range(plan.fill):
        chosen[i] = 0

    def rank(index, count):
        wanted = plan.frames - lax.div(index, total)
        item = lax.rem(index, total)
        owner, slot = lax.div(item, MAXREQ), lax.rem(item, MAXREQ)

        def add(count):
            source = lax.div(blk[owner, slot], plan.per_column)
            place = columns[source]
            columns[source] = place + 1
            order[count] = item
            places[count] = place

            @pl.when(source == col)
            def _():
                chosen[place] = blk[owner, slot] - source * plan.per_column

            return count + 1

        fresh = (slot < cnt[owner]) & (nfr[owner, slot] == wanted)
        return lax.cond(fresh, add, lambda count: count, count)

    live = lax.fori_loop(0, total * plan.frames, rank, jnp.int32(0))

    def request(index, carry, early):
        item = order[index]
        owner, slot = lax.div(item, MAXREQ), lax.rem(item, MAXREQ)

        def add(carry):
            count, units = carry
            first = start[owner, slot]
            last = first + nfr[owner, slot]
            reqs[0, count] = lax.div(blk[owner, slot], plan.per_column)
            reqs[1, count] = places[index]
            reqs[2, count] = first
            reqs[3, count] = last
            reqs[4, count] = units

            def frame(hop, carry):
                keeper = lax.div(hop, plan.hops)
                line = keeper * plan.owners + owner
                entry = lists[line]
                lists[line] = entry + 1
                pos[count * plan.frames + hop] = line * plan.deep + entry

                @pl.when((keeper == row) & (owner == col))
                def _():
                    omap[(hop - keeper * plan.hops) * MAXREQ + slot] = entry

                return carry

            lax.fori_loop(first, last, frame, 0)
            return count + 1, units + last - first

        return lax.cond((places[index] < plan.lead) == early, add, lambda carry: carry, carry)

    zero = jnp.int32(0)
    early, units = lax.fori_loop(
        0, live, functools.partial(request, early=True), (zero, zero)
    )
    units = jnp.maximum(units, plan.first)
    count, units = lax.fori_loop(
        0, live, functools.partial(request, early=False), (early, units)
    )
    longest, deepest = jnp.int32(0), jnp.int32(0)
    for i in range(plan.owners):
        longest = jnp.maximum(longest, columns[i])
    for i in range(plan.keepers * plan.owners):
        deepest = jnp.maximum(deepest, lists[i])

    def before(index, found):
        return found + (reqs[3, index] - reqs[2, index] + reqs[4, index] <= plan.first).astype(
            jnp.int32
        )

    late = lax.fori_loop(0, early, before, zero)
    meta[0] = columns[col]
    meta[1] = count
    meta[2] = row
    meta[3] = early
    meta[4] = late
    pick_a[0] = picked(longest - plan.lead, plan.fills)
    pick_b[0] = picked(units - plan.first, plan.counts)
    pick_c[0] = picked(deepest, plan.depths)


def make_tables(plan, req_block, req_start, req_frames, req_count):
    total = plan.owners * MAXREQ
    shape = lambda *dims: jax.ShapeDtypeStruct(dims, jnp.int32)
    return pl.pallas_call(
        functools.partial(tables_kernel, plan),
        out_shape=(
            shape(8),
            shape(plan.fill),
            shape(5, total),
            shape(total * plan.frames),
            shape(plan.hops * MAXREQ),
            shape(1),
            shape(1),
            shape(1),
        ),
        in_specs=[SMEM] * 4,
        out_specs=(SMEM,) * 8,
        scratch_shapes=[
            pltpu.SMEM((plan.owners,), jnp.int32),
            pltpu.SMEM((plan.keepers * plan.owners,), jnp.int32),
            pltpu.SMEM((total,), jnp.int32),
            pltpu.SMEM((total,), jnp.int32),
        ],
    )(req_block, req_start, req_frames, req_count)


def gather_kernel(plan, meta, chosen, in_ref, out_ref):
    @pl.when(pl.program_id(1) < jnp.maximum(meta[0], 1))
    def _():
        for piece in range(plan.slices):
            out_ref[piece, 0, 0] = in_ref[:, piece * plan.span : (piece + 1) * plan.span, :]


def gather(plan, coarse, meta, chosen):
    def place(i, m):
        return jnp.minimum(i, jnp.maximum(m[0] - 1, 0))

    return pl.pallas_call(
        functools.partial(gather_kernel, plan),
        out_shape=jax.ShapeDtypeStruct(
            (plan.slices, plan.fill, plan.hops, 2, plan.span, BLOCKW), coarse.dtype
        ),
        grid_spec=pltpu.PrefetchScalarGridSpec(
            num_scalar_prefetch=2,
            grid=(plan.hops, plan.fill),
            in_specs=[
                pl.BlockSpec((2, NFINE, BLOCKW), lambda h, i, m, c: (0, h, c[place(i, m)]))
            ],
            out_specs=pl.BlockSpec(
                (plan.slices, 1, 1, 2, plan.span, BLOCKW),
                lambda h, i, m, c: (0, place(i, m), h, 0, 0, 0),
            ),
        ),
    )(meta, chosen, coarse)


def spread_kernel(plan, begin, count, lifting, *refs):
    if lifting:
        src, _, code, scale, dst, got, got_scale, tmp, send, recv, local, up, down = refs
    else:
        src, dst, tmp, send, recv, local = refs
    row, col = lax.axis_index("tm"), lax.axis_index("chan")
    base = lax.div(row, plan.half) * plan.half
    me = (row - base) * plan.owners + col
    upper = row >= plan.half
    other = jnp.where(upper, row - plan.half, row + plan.half)
    barrier = pltpu.get_barrier_semaphore()
    order = plan.masks

    def device(index):
        return {"tm": base + lax.div(index, plan.owners), "chan": lax.rem(index, plan.owners)}

    for mask in order:
        pl.semaphore_signal(barrier, inc=1, device_id=device(me ^ mask))
    if lifting:
        pl.semaphore_signal(barrier, inc=1, device_id={"tm": other})
    pl.semaphore_wait(barrier, len(order) + int(lifting))

    lifts = []
    if lifting:
        lifts = [
            pltpu.make_async_remote_copy(
                src_ref=source,
                dst_ref=target,
                send_sem=up.at[index],
                recv_sem=down.at[index],
                device_id={"tm": other},
            )
            for index, (source, target) in enumerate([(code, got), (scale, got_scale)])
        ]

        @pl.when(upper)
        def _():
            for copy in lifts:
                copy.start()

    def copy(place, mask, source, target):
        return pltpu.make_async_remote_copy(
            src_ref=src.at[target, begin + place],
            dst_ref=dst.at[source, begin + place],
            send_sem=send.at[place, mask],
            recv_sem=recv.at[place, mask],
            device_id=device(me ^ mask),
        )

    @pl.loop(0, count)
    def _(place):
        for mask in order:
            copy(place, mask, me, me ^ mask).start()

    read = pltpu.make_async_copy(src.at[me, pl.ds(begin, count)], tmp, local.at[0])
    read.start()
    read.wait()
    write = pltpu.make_async_copy(tmp, dst.at[me, pl.ds(begin, count)], local.at[1])
    write.start()
    write.wait()

    @pl.loop(0, count)
    def _(place):
        for mask in order:
            copy(place, mask, me ^ mask, me).wait_recv()
            copy(place, mask, me, me ^ mask).wait_send()

    if lifting:

        @pl.when(upper)
        def _():
            for copy in lifts:
                copy.wait_send()

        @pl.when(jnp.logical_not(upper))
        def _():
            for copy in lifts:
                copy.wait_recv()


def spread(plan, packed, begin, count, collective, *more):
    sem = pltpu.SemaphoreType.DMA
    lifting = bool(more)
    shape = lambda value: jax.ShapeDtypeStruct(value.shape, value.dtype)
    scratch = [
        pltpu.VMEM((count,) + packed.shape[2:], packed.dtype),
        sem((count, plan.slices)),
        sem((count, plan.slices)),
        sem((2,)),
    ]
    if lifting:
        scratch += [sem((2,)), sem((2,))]
    return pl.pallas_call(
        functools.partial(spread_kernel, plan, begin, count, lifting),
        out_shape=tuple(shape(value) for value in (more or (packed,))),
        in_specs=[ANY] * (1 + len(more)),
        out_specs=(ANY,) * max(1, len(more)),
        scratch_shapes=scratch,
        input_output_aliases={1: 0} if lifting else {},
        compiler_params=pltpu.CompilerParams(collective_id=collective, has_side_effects=True),
    )(packed, *more)


def partial_sum(plan, upper, hop, w_ref, in_ref, part):
    first = (plan.half * plan.hops if upper else 0) + plan.frames - 1
    total = None
    for index in range(plan.half * plan.hops):
        source, local = divmod(index, plan.hops)
        term = w_ref[first + index - hop] * in_ref[source, 0, 0, local, part].astype(jnp.float32)
        total = term if total is None else total + term
    return total


def encode(parts, out_ref, scale_ref, place, scale_row):
    top = jnp.max(jnp.maximum(jnp.abs(parts[0]), jnp.abs(parts[1])), axis=0, keepdims=True)
    top = jnp.maximum(top, 1e-30)
    factor = TOP / top
    for part in range(2):
        code = jnp.round(parts[part] * factor).astype(jnp.int32)
        out_ref[place, part] = code.astype(jnp.int16)
    scale_ref[pl.ds(scale_row, 1), :] = top * (1.0 / TOP)


def upper_kernel(plan, late, meta, reqs, in_ref, w_ref, out_ref, scale_ref):
    index = pl.program_id(0)
    begin = plan.first if late else 0

    @pl.when((index < meta[1]) & (meta[2] >= plan.half))
    def _():
        first, last, offset = reqs[2, index], reqs[3, index], reqs[4, index]
        split = jnp.clip(first + plan.first - offset, first, last)

        @pl.loop(split if late else first, last if late else split)
        def _(hop):
            parts = [partial_sum(plan, True, hop, w_ref, in_ref, part) for part in range(2)]
            place = offset + hop - first - begin
            encode(parts, out_ref, scale_ref, place, place)


def lower_kernel(
    plan, meta, reqs, pos, in_ref, w_ref, got_0, scale_0, got_1, scale_1, out_ref, scale_ref
):
    index = pl.program_id(0)

    @pl.when((index < meta[1]) & (meta[2] < plan.half))
    def _():
        first, last, offset = reqs[2, index], reqs[3, index], reqs[4, index]
        split = jnp.clip(first + plan.first - offset, first, last)

        def add(got_ref, got_scale, begin, hop):
            unit = offset + hop - first - begin
            scale = got_scale[pl.ds(unit, 1), :]
            parts = []
            for part in range(2):
                other = got_ref[unit, part].astype(jnp.int32).astype(jnp.float32) * scale
                parts.append(partial_sum(plan, False, hop, w_ref, in_ref, part) + other)
            place = pos[index * plan.frames + hop]
            encode(parts, out_ref, scale_ref, place, place)

        @pl.loop(first, split)
        def _(hop):
            add(got_0, scale_0, 0, hop)

        @pl.loop(split, last)
        def _(hop):
            add(got_1, scale_1, plan.first, hop)


def filter_specs(plan, low, high):
    def request(i, m):
        bottom = m[low] if low else 0
        return jnp.maximum(jnp.clip(i, bottom, m[high] - 1), 0)

    taps = plan.frames - 1 + plan.all_hops
    return [
        pl.BlockSpec(
            (plan.half, 1, 1, plan.hops, 2, plan.span, BLOCKW),
            lambda i, m, r, *_: (0, r[0, request(i, m)], r[1, request(i, m)], 0, 0, 0, 0),
        ),
        pl.BlockSpec((taps, plan.span, BLOCKW), lambda i, *_: (0, 0, 0)),
    ]


def whole(*dims):
    return pl.BlockSpec(dims, lambda i, *_: (0,) * len(dims))


def filter_upper(plan, late, spreaded, weights, meta, reqs):
    units = plan.rest if late else plan.first
    return pl.pallas_call(
        functools.partial(upper_kernel, plan, late),
        out_shape=(
            jax.ShapeDtypeStruct((units, 2, plan.span, BLOCKW), jnp.int16),
            jax.ShapeDtypeStruct((units, BLOCKW), jnp.float32),
        ),
        grid_spec=pltpu.PrefetchScalarGridSpec(
            num_scalar_prefetch=2,
            grid=(plan.owners * MAXREQ,),
            in_specs=filter_specs(plan, 4 if late else 0, 1 if late else 3),
            out_specs=(whole(units, 2, plan.span, BLOCKW), whole(units, BLOCKW)),
        ),
    )(meta, reqs, spreaded, weights)


def filter_lower(plan, spreaded, weights, got, meta, reqs, pos):
    rows = plan.keepers * plan.owners * plan.deep
    return pl.pallas_call(
        functools.partial(lower_kernel, plan),
        out_shape=(
            jax.ShapeDtypeStruct((rows, 2, plan.span, BLOCKW), jnp.int16),
            jax.ShapeDtypeStruct((rows, BLOCKW), jnp.float32),
        ),
        grid_spec=pltpu.PrefetchScalarGridSpec(
            num_scalar_prefetch=3,
            grid=(plan.owners * MAXREQ,),
            in_specs=filter_specs(plan, 0, 1) + [whole(*value.shape) for value in got],
            out_specs=(whole(rows, 2, plan.span, BLOCKW), whole(rows, BLOCKW)),
        ),
    )(meta, reqs, pos, spreaded, weights, *got)


def lift_kernel(plan, count, src, src_scale, dst, dst_scale, send, recv):
    row = lax.axis_index("tm")
    barrier = pltpu.get_barrier_semaphore()
    upper = row >= plan.half
    other = jnp.where(upper, row - plan.half, row + plan.half)
    pl.semaphore_signal(barrier, inc=1, device_id={"tm": other})
    pl.semaphore_wait(barrier, 1)
    refs = [(src, dst), (src_scale, dst_scale)]
    copies = [
        pltpu.make_async_remote_copy(
            src_ref=source.at[pl.ds(0, count)],
            dst_ref=target.at[pl.ds(0, count)],
            send_sem=send.at[index],
            recv_sem=recv.at[index],
            device_id={"tm": other},
        )
        for index, (source, target) in enumerate(refs)
    ]

    @pl.when(upper)
    def _():
        for copy in copies:
            copy.start()
        for copy in copies:
            copy.wait_send()

    @pl.when(jnp.logical_not(upper))
    def _():
        for copy in copies:
            copy.wait_recv()


def lift(plan, values, scales, count, collective):
    sem = pltpu.SemaphoreType.DMA
    return pl.pallas_call(
        functools.partial(lift_kernel, plan, count),
        out_shape=(
            jax.ShapeDtypeStruct(values.shape, values.dtype),
            jax.ShapeDtypeStruct(scales.shape, scales.dtype),
        ),
        in_specs=[ANY, ANY],
        out_specs=(ANY, ANY),
        scratch_shapes=[sem((2,)), sem((2,))],
        compiler_params=pltpu.CompilerParams(collective_id=collective, has_side_effects=True),
    )(values, scales)


def deliver_kernel(plan, count, src, src_scale, dst, dst_scale, tmp, tmp_scale, send, recv, local):
    row, col = lax.axis_index("tm"), lax.axis_index("chan")
    size, lines = plan.slices, plan.keepers * plan.owners
    me = row * plan.owners + col
    barrier = pltpu.get_barrier_semaphore()

    def device(index):
        return {"tm": lax.div(index, plan.owners), "chan": lax.rem(index, plan.owners)}

    def copies(step, source, target, other):
        values = pltpu.make_async_remote_copy(
            src_ref=src.at[target, pl.ds(0, count)],
            dst_ref=dst.at[source, pl.ds(0, count)],
            send_sem=send.at[0, step],
            recv_sem=recv.at[0, step],
            device_id=device(other),
        )
        scales = pltpu.make_async_remote_copy(
            src_ref=src_scale.at[target],
            dst_ref=dst_scale.at[source],
            send_sem=send.at[1, step],
            recv_sem=recv.at[1, step],
            device_id=device(other),
        )
        return values, scales

    @pl.when(row < plan.half)
    def _():
        @pl.loop(1, size)
        def _(step):
            pl.semaphore_signal(barrier, inc=1, device_id=device(lax.rem(me + step, size)))

        pl.semaphore_wait(barrier, size - 1)

        @pl.loop(1, size)
        def _(step):
            target = lax.rem(me + step, size)

            @pl.when(target < lines)
            def _():
                for copy in copies(step, me, target, target):
                    copy.start()

        @pl.when(me < lines)
        def _():
            moves = [
                (src.at[me, pl.ds(0, count)], tmp, dst.at[me, pl.ds(0, count)]),
                (src_scale.at[me], tmp_scale, dst_scale.at[me]),
            ]
            for index, (source, middle, target) in enumerate(moves):
                read = pltpu.make_async_copy(source, middle, local.at[2 * index])
                read.start()
                read.wait()
                write = pltpu.make_async_copy(middle, target, local.at[2 * index + 1])
                write.start()
                write.wait()

            @pl.loop(1, size)
            def _(step):
                source = lax.rem(me + size - step, size)
                for copy in copies(step, source, me, source):
                    copy.wait_recv()

        @pl.loop(1, size)
        def _(step):
            target = lax.rem(me + step, size)

            @pl.when(target < lines)
            def _():
                for copy in copies(step, me, target, target):
                    copy.wait_send()


def deliver(plan, values, scales, count, collective):
    sem = pltpu.SemaphoreType.DMA
    inner = values.shape[1:]
    return pl.pallas_call(
        functools.partial(deliver_kernel, plan, count),
        out_shape=(
            jax.ShapeDtypeStruct((plan.slices,) + inner, values.dtype),
            jax.ShapeDtypeStruct((plan.slices,) + scales.shape[1:], scales.dtype),
        ),
        in_specs=[ANY, ANY],
        out_specs=(ANY, ANY),
        scratch_shapes=[
            pltpu.VMEM((count,) + inner[1:], values.dtype),
            pltpu.VMEM(scales.shape[1:], scales.dtype),
            sem((2, plan.slices)),
            sem((2, plan.slices)),
            sem((4,)),
        ],
        compiler_params=pltpu.CompilerParams(collective_id=collective, has_side_effects=True),
    )(values, scales)


def transform_kernel(plan, omap, in_ref, scale_ref, high_ref, low_ref, turn_ref, out_ref, yh, yl, zs):
    entry = omap[pl.program_id(0)]

    @pl.when(entry < 0)
    def _():
        out_ref[...] = jnp.zeros_like(out_ref)

    @pl.when(entry >= 0)
    def _():
        chunk = 32

        def load(part, first):
            piece, line = divmod(first, plan.span)
            code = in_ref[piece, 0, part, line : line + chunk, :]
            scale = scale_ref[piece, pl.ds(entry, 1), :]
            return code.astype(jnp.int32).astype(jnp.float32) * scale

        for line in range(0, SUB, chunk):
            re = [load(0, SUB * a + line) for a in range(RADIX)]
            im = [load(1, SUB * a + line) for a in range(RADIX)]
            es, ed = re[0] + re[2], re[0] - re[2]
            fs, fd = im[0] + im[2], im[0] - im[2]
            gs, gd = re[1] + re[3], re[1] - re[3]
            hs, hd = im[1] + im[3], im[1] - im[3]
            mixed = [
                (es + gs, fs + hs),
                (ed + hd, fd - gd),
                (es - gs, fs - hs),
                (ed - hd, fd + gd),
            ]
            rows = slice(line, line + chunk)
            for q in range(RADIX):
                real, imag = mixed[q]
                if q:
                    cosine, sine = turn_ref[0, q - 1, rows, :], turn_ref[1, q - 1, rows, :]
                    real, imag = real * cosine + imag * sine, imag * cosine - real * sine
                for part, value in enumerate((real, imag)):
                    cols = slice(part * BLOCKW, (part + 1) * BLOCKW)
                    high = value.astype(jnp.bfloat16)
                    yh[q, rows, cols] = high
                    yl[q, rows, cols] = (value - high.astype(jnp.float32)).astype(jnp.bfloat16)

        for q in range(RADIX):
            both = jnp.dot(high_ref[...], yh[q], preferred_element_type=jnp.float32)
            both = both + jnp.dot(high_ref[...], yl[q], preferred_element_type=jnp.float32)
            both = both + jnp.dot(low_ref[...], yh[q], preferred_element_type=jnp.float32)
            rows = pl.ds(q, SUB, stride=RADIX)
            zs[0, rows, :] = both[:SUB, :BLOCKW] + both[SUB:, BLOCKW:]
            zs[1, rows, :] = both[:SUB, BLOCKW:] - both[SUB:, :BLOCKW]

        out_ref[0, 0] = zs[...].astype(out_ref.dtype)


def transform_tables():
    line = np.arange(SUB)
    angles = (line[:, None] * line[None, :] % SUB) * (2.0 * np.pi / SUB)
    table = np.concatenate([np.cos(angles), np.sin(angles)], axis=0) / math.sqrt(NFINE)
    table = table.astype(np.float32)
    high = table.astype(jnp.bfloat16)
    low = (table - high.astype(np.float32)).astype(jnp.bfloat16)
    turns = np.arange(1, RADIX)[:, None] * line[None, :] * (2.0 * np.pi / NFINE)
    turn = np.stack([np.cos(turns), np.sin(turns)]).astype(np.float32)
    return high, low, turn


def transform(plan, values, scales, omap):
    high, low, turn = transform_tables()
    turn = jnp.asarray(np.ascontiguousarray(np.broadcast_to(turn[..., None], turn.shape + (BLOCKW,))))
    return pl.pallas_call(
        functools.partial(transform_kernel, plan),
        out_shape=jax.ShapeDtypeStruct((plan.hops, MAXREQ, 2, NFINE, BLOCKW), jnp.bfloat16),
        grid_spec=pltpu.PrefetchScalarGridSpec(
            num_scalar_prefetch=1,
            grid=(plan.hops * MAXREQ,),
            in_specs=[
                pl.BlockSpec(
                    (plan.slices, 1, 2, plan.span, BLOCKW),
                    lambda i, o: (0, jnp.maximum(o[i], 0), 0, 0, 0),
                ),
                whole(*scales.shape),
                whole(2 * SUB, SUB),
                whole(2 * SUB, SUB),
                whole(2, RADIX - 1, SUB, BLOCKW),
            ],
            out_specs=pl.BlockSpec(
                (1, 1, 2, NFINE, BLOCKW), lambda i, o: (i // MAXREQ, i % MAXREQ, 0, 0, 0)
            ),
            scratch_shapes=[
                pltpu.VMEM((RADIX, SUB, 2 * BLOCKW), jnp.bfloat16),
                pltpu.VMEM((RADIX, SUB, 2 * BLOCKW), jnp.bfloat16),
                pltpu.VMEM((2, NFINE, BLOCKW), jnp.float32),
            ],
        ),
    )(omap, values, scales, jnp.asarray(high), jnp.asarray(low), turn)


def owners_power(value):
    return value & (value - 1) == 0


class Plan:
    def __init__(self, size, owners, hops, per_column):
        self.size, self.owners, self.hops, self.per_column = size, owners, hops, per_column
        self.all_hops = hops * size
        self.frames = self.all_hops - TAPS + 1
        self.keepers = -(-self.frames // hops)
        self.half = size // 2
        self.slices = self.half * owners
        self.span = NFINE // self.slices
        self.fill = owners * PAIR
        self.deep = round_up(hops * MAXREQ, 8)
        self.lead = min(2, self.fill)
        self.first = 40
        self.rest = round_up(owners * MAXREQ * self.frames, 8)
        more = self.fill - self.lead
        self.fills = sorted({max(1, round_up(more * i, 6) // 6) for i in (1, 2, 3, 4, 6)})
        near = {min(8 * i, self.rest) for i in (1, 2, 3, 4, 5, 7, 9)}
        self.counts = sorted(near | {self.rest})
        most = hops * MAXREQ
        self.depths = sorted({round_up(most * i, 12) // 12 for i in (5, 6, 7, 8, 9, 10, 11, 12)})

        spread = sorted(range(2, self.slices), key=lambda mask: bin(mask >> 1).count("1"))
        self.masks = spread + [1]

    def fits(self):
        powers = self.slices & (self.slices - 1) == 0 and owners_power(self.owners)
        even = powers and self.size % 2 == 0 and NFINE % self.slices == 0 and self.span % 32 == 0
        return even and self.keepers <= self.half


def shards(coarse, prototype, req_block, req_start, req_frames, req_count):
    owners, size = lax.axis_size("chan"), lax.axis_size("tm")
    plan = Plan(size, owners, coarse.shape[1] // NFINE, coarse.shape[2] // BLOCKW)
    if not plan.fits():
        return shards_general(coarse, prototype, req_block, req_start, req_frames, req_count)
    tables = make_tables(plan, req_block, req_start, req_frames, req_count)
    meta, chosen, reqs, pos, omap, pick_a, pick_b, pick_c = tables
    packed = gather(plan, coarse, meta, chosen)

    me = lax.axis_index("tm") % plan.half * owners + lax.axis_index("chan")
    mine = lax.dynamic_slice(prototype, (0, me * plan.span), (TAPS, plan.span))
    mine = jnp.pad(mine, ((plan.frames - 1, plan.all_hops - TAPS), (0, 0)))
    weights = jnp.broadcast_to(mine[:, :, None], mine.shape + (BLOCKW,))

    def split(value):
        return value.reshape((plan.half, owners) + value.shape[1:])

    spreaded = spread(plan, packed, 0, plan.lead, 0)[0]
    early = filter_upper(plan, False, split(spreaded), weights, meta, reqs)

    def second(count, collective, *operands):
        return spread(plan, operands[0], plan.lead, count, collective, *operands[1:])

    branches = [functools.partial(second, size, 1 + i) for i, size in enumerate(plan.fills)]
    spreaded, *got = lax.switch(pick_a[0], branches, packed, spreaded, *early)
    spreaded = split(spreaded)
    late = filter_upper(plan, True, spreaded, weights, meta, reqs)
    base = 1 + len(branches)
    branches = [
        functools.partial(lambda n, c, *x: lift(plan, *x, n, c), size, base + i)
        for i, size in enumerate(plan.counts)
    ]
    got += lax.switch(pick_b[0], branches, *late)
    values, scales = filter_lower(plan, spreaded, weights, got, meta, reqs, pos)
    lines = plan.keepers * owners
    values = values.reshape((lines, plan.deep) + values.shape[1:])
    scales = scales.reshape((lines, plan.deep) + scales.shape[1:])
    base += len(branches)
    branches = [
        functools.partial(lambda n, c, *x: deliver(plan, *x, n, c), size, base + i)
        for i, size in enumerate(plan.depths)
    ]
    values, scales = lax.switch(pick_c[0], branches, values, scales)
    return transform(plan, values, scales, omap)[:, None]


def solution(mesh):
    return jax.shard_map(
        shards,
        mesh=mesh,
        in_specs=(P(None, "tm", "chan"), P(), P(), P(), P(), P()),
        out_specs=P("tm", "chan", None, None, None, None),
        check_vma=False,
    )
```

```python
import functools
import math

import jax
import jax.numpy as jnp
import numpy as np
from jax import lax
from jax.experimental import pallas as pl
from jax.experimental.pallas import tpu as pltpu
from jax.sharding import PartitionSpec as P

BLOCKW = 128
NFINE = 1024
TAPS = 16
MAXREQ = 4
PAIR = 2
ROWS = 128
STEP = 16
ANY = pl.BlockSpec(memory_space=pl.ANY)


def build_table():
    line = jnp.arange(NFINE, dtype=jnp.int32)
    products = line[:, None] * line[None, :] % NFINE
    angles = products.astype(jnp.float32) * (2.0 * math.pi / NFINE)
    scale = 1.0 / math.sqrt(NFINE)
    return jnp.concatenate([jnp.cos(angles) * scale, jnp.sin(angles) * scale], axis=0)


def pack_kernel(chosen, coarse_ref, out_ref):
    out_ref[...] = coarse_ref[...].reshape(out_ref.shape)


def pack(coarse, chosen, first, hops):
    count = chosen.shape[0]
    return pl.pallas_call(
        pack_kernel,
        out_shape=jax.ShapeDtypeStruct((count, 2, hops * NFINE, BLOCKW), coarse.dtype),
        grid_spec=pltpu.PrefetchScalarGridSpec(
            num_scalar_prefetch=1,
            grid=(count,),
            in_specs=[pl.BlockSpec((2, hops * NFINE, BLOCKW), lambda i, c: (0, first, c[i]))],
            out_specs=pl.BlockSpec((1, 2, hops * NFINE, BLOCKW), lambda i, c: (i, 0, 0, 0)),
        ),
        cost_estimate=pl.CostEstimate(
            flops=0, transcendentals=0, bytes_accessed=count * 8 * hops * NFINE * BLOCKW
        ),
    )(chosen, coarse)


def select_kernel(pieces, arrival, in_ref, out_ref):
    share = BLOCKW // pieces
    for piece in range(pieces):
        cols = slice(piece * share, (piece + 1) * share)
        out_ref[piece] = jnp.concatenate([in_ref[0, 0, :, cols], in_ref[0, 1, :, cols]], axis=-1)


def select(incoming, arrival, pieces, hops):
    width = 2 * BLOCKW // pieces
    rows = hops * NFINE
    return pl.pallas_call(
        functools.partial(select_kernel, pieces),
        out_shape=jax.ShapeDtypeStruct((MAXREQ * pieces, rows, width), incoming.dtype),
        grid_spec=pltpu.PrefetchScalarGridSpec(
            num_scalar_prefetch=1,
            grid=(MAXREQ, hops),
            in_specs=[pl.BlockSpec((1, 2, NFINE, BLOCKW), lambda q, h, a: (a[q], 0, h, 0))],
            out_specs=pl.BlockSpec((pieces, NFINE, width), lambda q, h, a: (q, h, 0)),
        ),
        cost_estimate=pl.CostEstimate(
            flops=0, transcendentals=0, bytes_accessed=MAXREQ * 8 * rows * BLOCKW
        ),
    )(arrival, incoming)


def exchange_kernel(
    owners, size, a_in, b_in, a_out, b_out, a_tmp, b_tmp, a_send, a_recv, b_send, b_recv, local
):
    column, row = lax.axis_index("chan"), lax.axis_index("tm")
    barrier = pltpu.get_barrier_semaphore()

    @pl.loop(1, owners)
    def _(step):
        other = lax.rem(column + step, owners)
        pl.semaphore_signal(barrier, inc=1, device_id={"chan": other})

    @pl.loop(1, size)
    def _(step):
        other = lax.rem(row + step, size)
        pl.semaphore_signal(barrier, inc=1, device_id={"tm": other})

    pl.semaphore_wait(barrier, owners + size - 2)

    def a_copy(step, source, target, device):
        return pltpu.make_async_remote_copy(
            src_ref=a_in.at[pl.ds(target * PAIR, PAIR)],
            dst_ref=a_out.at[pl.ds(source * PAIR, PAIR)],
            send_sem=a_send.at[step],
            recv_sem=a_recv.at[step],
            device_id={"chan": device},
        )

    def b_copy(step, source, target, device):
        return pltpu.make_async_remote_copy(
            src_ref=b_in.at[target],
            dst_ref=b_out.at[source],
            send_sem=b_send.at[step],
            recv_sem=b_recv.at[step],
            device_id={"tm": device},
        )

    @pl.loop(1, size)
    def _(step):
        target = lax.rem(row + step, size)
        b_copy(step, row, target, target).start()

    @pl.loop(1, owners)
    def _(step):
        target = lax.rem(column + step, owners)
        a_copy(step, column, target, target).start()

    a_read = pltpu.make_async_copy(a_in.at[pl.ds(column * PAIR, PAIR)], a_tmp, local.at[0])
    b_read = pltpu.make_async_copy(b_in.at[row], b_tmp, local.at[1])
    a_read.start()
    b_read.start()
    a_read.wait()
    b_read.wait()
    a_write = pltpu.make_async_copy(a_tmp, a_out.at[pl.ds(column * PAIR, PAIR)], local.at[2])
    b_write = pltpu.make_async_copy(b_tmp, b_out.at[row], local.at[3])
    a_write.start()
    b_write.start()
    a_write.wait()
    b_write.wait()

    @pl.loop(1, owners)
    def _(step):
        source = lax.rem(column + owners - step, owners)
        copy = a_copy(step, source, column, source)
        copy.wait_recv()
        copy.wait_send()

    @pl.loop(1, size)
    def _(step):
        source = lax.rem(row + size - step, size)
        copy = b_copy(step, source, row, source)
        copy.wait_recv()
        copy.wait_send()


def exchange(outgoing, sending, owners, size, collective):
    sem = pltpu.SemaphoreType.DMA
    return pl.pallas_call(
        functools.partial(exchange_kernel, owners, size),
        out_shape=(
            jax.ShapeDtypeStruct(outgoing.shape, outgoing.dtype),
            jax.ShapeDtypeStruct(sending.shape, sending.dtype),
        ),
        in_specs=[ANY, ANY],
        out_specs=(ANY, ANY),
        scratch_shapes=[
            pltpu.VMEM((PAIR,) + outgoing.shape[1:], outgoing.dtype),
            pltpu.VMEM(sending.shape[1:], sending.dtype),
            sem((owners,)),
            sem((owners,)),
            sem((size,)),
            sem((size,)),
            sem((4,)),
        ],
        compiler_params=pltpu.CompilerParams(collective_id=collective, has_side_effects=True),
    )(outgoing, sending)


def filter_kernel(hops, frames, weights_ref, *refs):
    out_ref = refs[-1]
    width = refs[0].shape[-1]

    @pl.loop(0, ROWS // STEP)
    def _(step):
        rows = pl.ds(pl.multiple_of(step * STEP, STEP), STEP)
        weights = [
            jnp.broadcast_to(weights_ref[rows, tap : tap + 1], (STEP, width)) for tap in range(TAPS)
        ]
        for frame in range(frames):
            total = None
            for tap in range(TAPS):
                hop = frame + tap
                term = weights[tap] * refs[hop % hops][hop // hops, rows, :].astype(jnp.float32)
                total = term if total is None else total + term
            out_ref[rows, frame * width : (frame + 1) * width] = total


def polyphase(parts, prototype, frames):
    hops = len(parts)
    size, _, width = parts[0].shape
    return pl.pallas_call(
        functools.partial(filter_kernel, hops, frames),
        out_shape=jax.ShapeDtypeStruct((NFINE, frames * width), jnp.float32),
        grid=(NFINE // ROWS,),
        in_specs=[pl.BlockSpec((ROWS, TAPS), lambda i: (i, 0))]
        + [pl.BlockSpec((size, ROWS, width), lambda i: (0, i, 0))] * hops,
        out_specs=pl.BlockSpec((ROWS, frames * width), lambda i: (i, 0)),
    )(prototype.T, *parts)


def combine_kernel(frames, share, both_ref, out_ref):
    frame = pl.program_id(0)

    @pl.when(frame < frames)
    def _():
        sine = both_ref[1]
        turned = jnp.concatenate([sine[:, share:], -sine[:, :share]], axis=-1)
        out_ref[0] = (both_ref[0] + turned).astype(out_ref.dtype)

    @pl.when(frame >= frames)
    def _():
        out_ref[...] = jnp.zeros_like(out_ref)


def combine(both, frames, padded, width):
    return pl.pallas_call(
        functools.partial(combine_kernel, frames, width // 2),
        out_shape=jax.ShapeDtypeStruct((padded, NFINE, width), jnp.bfloat16),
        grid=(padded,),
        in_specs=[
            pl.BlockSpec((2, NFINE, width), lambda f: (0, 0, jnp.minimum(f, frames - 1))),
        ],
        out_specs=pl.BlockSpec((1, NFINE, width), lambda f: (f, 0, 0)),
    )(both)


def return_kernel(size, keepers, hops, res_ref, out_ref, send_sems, recv_sems):
    me = lax.axis_index("tm")
    barrier = pltpu.get_barrier_semaphore()

    @pl.loop(1, size)
    def _(step):
        other = lax.rem(me + step, size)
        pl.semaphore_signal(barrier, inc=1, device_id={"tm": other})

    pl.semaphore_wait(barrier, size - 1)

    def copy(step):
        target = lax.rem(me + step, size)
        return pltpu.make_async_remote_copy(
            src_ref=res_ref.at[pl.ds(target * hops, hops)],
            dst_ref=out_ref.at[me],
            send_sem=send_sems.at[step],
            recv_sem=recv_sems.at[step],
            device_id={"tm": target},
        )

    def arriving(step):
        source = lax.rem(me + size - step, size)
        return pltpu.make_async_remote_copy(
            src_ref=res_ref.at[pl.ds(0, hops)],
            dst_ref=out_ref.at[source],
            send_sem=send_sems.at[step],
            recv_sem=recv_sems.at[step],
            device_id={"tm": source},
        )

    @pl.loop(1, size)
    def _(step):
        @pl.when(lax.rem(me + step, size) < keepers)
        def _():
            copy(step).start()

    @pl.when(me < keepers)
    def _():
        @pl.loop(1, size)
        def _(step):
            arriving(step).wait_recv()

    @pl.loop(1, size)
    def _(step):
        @pl.when(lax.rem(me + step, size) < keepers)
        def _():
            copy(step).wait_send()


def give_back(result, size, keepers, hops):
    shape = (size, hops) + result.shape[1:]
    return pl.pallas_call(
        functools.partial(return_kernel, size, keepers, hops),
        out_shape=jax.ShapeDtypeStruct(shape, result.dtype),
        in_specs=[ANY],
        out_specs=ANY,
        scratch_shapes=[pltpu.SemaphoreType.DMA((size,)), pltpu.SemaphoreType.DMA((size,))],
        compiler_params=pltpu.CompilerParams(collective_id=0, has_side_effects=True),
    )(result)


def final_kernel(pieces, meta, got_ref, own_ref, out_ref):
    share = BLOCKW // pieces
    slot, hop = pl.program_id(0), pl.program_id(1)
    row = meta[0]
    active = meta[2 + slot * pl.num_programs(1) + hop] > 0

    @pl.when(jnp.logical_not(active))
    def _():
        out_ref[...] = jnp.zeros_like(out_ref)

    @pl.when(active)
    def _():
        data = [
            jnp.where(slot * pieces + piece == row, own_ref[0], got_ref[piece, 0])
            for piece in range(pieces)
        ]
        for part in range(2):
            cols = slice(part * share, (part + 1) * share)
            out_ref[0, 0, part] = jnp.concatenate([d[:, cols] for d in data], axis=-1)


def assemble(got, result, active, row, keepers, pieces):
    size, hops, _, width = got.shape
    base = jnp.minimum(row, keepers - 1) * hops
    meta = jnp.concatenate(
        [jnp.stack([row, base]).astype(jnp.int32), active.astype(jnp.int32).reshape(-1)]
    )
    return pl.pallas_call(
        functools.partial(final_kernel, pieces),
        out_shape=jax.ShapeDtypeStruct((hops, MAXREQ, 2, NFINE, BLOCKW), got.dtype),
        grid_spec=pltpu.PrefetchScalarGridSpec(
            num_scalar_prefetch=1,
            grid=(MAXREQ, hops),
            in_specs=[
                pl.BlockSpec((pieces, 1, NFINE, width), lambda q, h, m: (q, h, 0, 0)),
                pl.BlockSpec((1, NFINE, width), lambda q, h, m: (m[1] + h, 0, 0)),
            ],
            out_specs=pl.BlockSpec((1, 1, 2, NFINE, BLOCKW), lambda q, h, m: (h, q, 0, 0, 0)),
        ),
    )(meta, got, result)


def shards_general(coarse, prototype, req_block, req_start, req_frames, req_count):
    owners = lax.axis_size("chan")
    column = lax.axis_index("chan")
    row = lax.axis_index("tm")
    size = lax.axis_size("tm")
    per_column = coarse.shape[2] // BLOCKW
    hops = coarse.shape[1] // NFINE
    all_hops = hops * size
    frames = all_hops - TAPS + 1
    keepers = -(-frames // hops)
    pieces = size // MAXREQ
    width = 2 * BLOCKW // pieces
    share = BLOCKW // pieces

    slot_ids = jnp.arange(MAXREQ, dtype=jnp.int32)
    live = slot_ids[None, :] < req_count[:, None]
    sources = req_block // per_column
    same = (
        live[:, :, None]
        & live[:, None, :]
        & (sources[:, :, None] == sources[:, None, :])
        & (slot_ids[None, None, :] < slot_ids[None, :, None])
    )
    rank = jnp.sum(same.astype(jnp.int32), axis=2)
    picked = (
        (live & (sources == column))[:, None, :]
        & (rank[:, None, :] == jnp.arange(PAIR, dtype=jnp.int32)[None, :, None])
    )
    local = req_block - column * per_column
    chosen = jnp.sum(jnp.where(picked, local[:, None, :], 0), axis=2).reshape(-1)
    chosen = jnp.clip(chosen, 0, per_column - 1).astype(jnp.int32)
    mine = (jnp.arange(owners, dtype=jnp.int32) == column)[:, None]

    def own(table):
        return jnp.sum(jnp.where(mine, table, 0), axis=0)

    my_live = slot_ids < own(req_count[:, None])[0]
    arrival = jnp.where(my_live, own(sources) * PAIR + own(rank), 0)
    arrival = jnp.clip(arrival, 0, owners * PAIR - 1).astype(jnp.int32)
    my_start, my_frames = own(req_start), own(req_frames)
    hop_ids = row * hops + jnp.arange(hops, dtype=jnp.int32)
    active = (
        my_live[:, None]
        & (hop_ids[None, :] >= my_start[:, None])
        & (hop_ids[None, :] < (my_start + my_frames)[:, None])
    )

    table = build_table()
    outgoing = [pack(coarse, chosen, hop, 1) for hop in range(hops)]
    incoming = lax.all_to_all(outgoing[0], "chan", split_axis=0, concat_axis=0, tiled=True)
    parts = []
    for hop in range(1, hops):
        sending = select(incoming, arrival, pieces, 1)
        incoming, gathered = exchange(outgoing[hop], sending, owners, size, hop)
        parts.append(gathered)
    sending = select(incoming, arrival, pieces, 1)
    parts.append(lax.all_to_all(sending, "tm", split_axis=0, concat_axis=0, tiled=True))
    flat = polyphase(parts, prototype, frames)
    both = jnp.dot(table, flat, precision=lax.Precision.HIGH, preferred_element_type=jnp.float32)
    padded = keepers * hops
    if width % 128 == 0:
        result = combine(both.reshape(2, NFINE, frames * width), frames, padded, width)
    else:
        both = both.reshape(2, NFINE, frames, 2, share)
        cosine, sine = both[0], both[1]
        result = jnp.stack(
            [cosine[:, :, 0] + sine[:, :, 1], cosine[:, :, 1] - sine[:, :, 0]], axis=2
        ).astype(jnp.bfloat16)
        result = result.reshape(NFINE, frames, width).transpose(1, 0, 2)
        if padded > frames:
            zeros = jnp.zeros((padded - frames, NFINE, width), result.dtype)
            result = jnp.concatenate([result, zeros], axis=0)
    got = give_back(result, size, keepers, hops)
    return assemble(got, result, active, row, keepers, pieces)[:, None]


SMEM = pl.BlockSpec(memory_space=pltpu.SMEM)
TOP = 32767.0
RADIX = 4
SUB = NFINE // RADIX


def round_up(value, unit):
    return -(-value // unit) * unit


def picked(value, sizes):
    return sum((value > size).astype(jnp.int32) for size in sizes[:-1])


def tables_kernel(
    plan, blk, start, nfr, cnt, meta, chosen, reqs, pos, omap, pick_a, pick_b, pick_c,
    columns, lists, order, places, buckets
):
    row, col = lax.axis_index("tm"), lax.axis_index("chan")
    total = plan.owners * MAXREQ
    for i in range(plan.owners):
        columns[i] = 0
    for i in range(plan.keepers * plan.owners):
        lists[i] = 0
    for i in range(plan.hops * MAXREQ):
        omap[i] = -1
    for i in range(plan.fill):
        chosen[i] = 0

    for i in range(plan.frames + 1):
        buckets[i] = 0

    def fresh(item):
        owner, slot = lax.div(item, MAXREQ), lax.rem(item, MAXREQ)
        return slot < cnt[owner], nfr[owner, slot]

    @pl.loop(0, total)
    def _(item):
        alive, size = fresh(item)

        @pl.when(alive)
        def _():
            buckets[size] = buckets[size] + 1

    live = jnp.int32(0)
    for size in range(plan.frames, 0, -1):
        amount = buckets[size]
        buckets[size] = live
        live = live + amount

    @pl.loop(0, total)
    def _(item):
        alive, size = fresh(item)

        @pl.when(alive)
        def _():
            spot = buckets[size]
            buckets[size] = spot + 1
            order[spot] = item

    @pl.loop(0, live)
    def _(index):
        item = order[index]
        block = blk[lax.div(item, MAXREQ), lax.rem(item, MAXREQ)]
        source = lax.div(block, plan.per_column)
        place = columns[source]
        columns[source] = place + 1
        places[index] = place

        @pl.when(source == col)
        def _():
            chosen[place] = block - source * plan.per_column

    def request(index, carry, early):
        item = order[index]
        owner, slot = lax.div(item, MAXREQ), lax.rem(item, MAXREQ)

        def add(carry):
            count, units = carry
            first = start[owner, slot]
            last = first + nfr[owner, slot]
            reqs[0, count] = lax.div(blk[owner, slot], plan.per_column)
            reqs[1, count] = places[index]
            reqs[2, count] = first
            reqs[3, count] = last
            reqs[4, count] = units

            def frame(hop, carry):
                keeper = lax.div(hop, plan.hops)
                line = keeper * plan.owners + owner
                entry = lists[line]
                lists[line] = entry + 1
                pos[count * plan.frames + hop] = line * plan.deep + entry

                @pl.when((keeper == row) & (owner == col))
                def _():
                    omap[(hop - keeper * plan.hops) * MAXREQ + slot] = entry

                return carry

            lax.fori_loop(first, last, frame, 0)
            return count + 1, units + last - first

        return lax.cond((places[index] < plan.lead) == early, add, lambda carry: carry, carry)

    zero = jnp.int32(0)
    early, units = lax.fori_loop(
        0, live, functools.partial(request, early=True), (zero, zero)
    )
    units = jnp.maximum(units, plan.first)
    count, units = lax.fori_loop(
        0, live, functools.partial(request, early=False), (early, units)
    )
    longest, deepest = jnp.int32(0), jnp.int32(0)
    for i in range(plan.owners):
        longest = jnp.maximum(longest, columns[i])
    for i in range(plan.keepers * plan.owners):
        deepest = jnp.maximum(deepest, lists[i])

    def before(index, found):
        return found + (reqs[3, index] - reqs[2, index] + reqs[4, index] <= plan.first).astype(
            jnp.int32
        )

    late = lax.fori_loop(0, early, before, zero)
    meta[0] = columns[col]
    meta[1] = count
    meta[2] = row
    meta[3] = early
    meta[4] = late
    pick_a[0] = picked(longest - plan.lead, plan.fills)
    pick_b[0] = picked(units - plan.first, plan.counts)
    pick_c[0] = picked(deepest, plan.depths)


def make_tables(plan, req_block, req_start, req_frames, req_count):
    total = plan.owners * MAXREQ
    shape = lambda *dims: jax.ShapeDtypeStruct(dims, jnp.int32)
    return pl.pallas_call(
        functools.partial(tables_kernel, plan),
        out_shape=(
            shape(8),
            shape(plan.fill),
            shape(5, total),
            shape(total * plan.frames),
            shape(plan.hops * MAXREQ),
            shape(1),
            shape(1),
            shape(1),
        ),
        in_specs=[SMEM] * 4,
        out_specs=(SMEM,) * 8,
        scratch_shapes=[
            pltpu.SMEM((plan.owners,), jnp.int32),
            pltpu.SMEM((plan.keepers * plan.owners,), jnp.int32),
            pltpu.SMEM((total,), jnp.int32),
            pltpu.SMEM((total,), jnp.int32),
            pltpu.SMEM((plan.frames + 1,), jnp.int32),
        ],
    )(req_block, req_start, req_frames, req_count)


def gather_kernel(plan, meta, chosen, in_ref, out_ref):
    @pl.when(pl.program_id(1) < jnp.maximum(meta[0], 1))
    def _():
        for piece in range(plan.slices):
            out_ref[piece, 0, 0] = in_ref[:, piece * plan.span : (piece + 1) * plan.span, :]


def gather(plan, coarse, meta, chosen):
    def place(i, m):
        return jnp.minimum(i, jnp.maximum(m[0] - 1, 0))

    return pl.pallas_call(
        functools.partial(gather_kernel, plan),
        out_shape=jax.ShapeDtypeStruct(
            (plan.slices, plan.fill, plan.hops, 2, plan.span, BLOCKW), coarse.dtype
        ),
        grid_spec=pltpu.PrefetchScalarGridSpec(
            num_scalar_prefetch=2,
            grid=(plan.hops, plan.fill),
            in_specs=[
                pl.BlockSpec((2, NFINE, BLOCKW), lambda h, i, m, c: (0, h, c[place(i, m)]))
            ],
            out_specs=pl.BlockSpec(
                (plan.slices, 1, 1, 2, plan.span, BLOCKW),
                lambda h, i, m, c: (0, place(i, m), h, 0, 0, 0),
            ),
        ),
    )(meta, chosen, coarse)


def spread_kernel(plan, begin, count, lifting, *refs):
    if lifting:
        src, _, code, scale, dst, got, got_scale, tmp, send, recv, local, up, down = refs
    else:
        src, dst, tmp, send, recv, local = refs
    row, col = lax.axis_index("tm"), lax.axis_index("chan")
    base = lax.div(row, plan.half) * plan.half
    me = (row - base) * plan.owners + col
    upper = row >= plan.half
    other = jnp.where(upper, row - plan.half, row + plan.half)
    barrier = pltpu.get_barrier_semaphore()
    order = plan.masks

    def device(index):
        return {"tm": base + lax.div(index, plan.owners), "chan": lax.rem(index, plan.owners)}

    for mask in order:
        pl.semaphore_signal(barrier, inc=1, device_id=device(me ^ mask))
    if lifting:
        pl.semaphore_signal(barrier, inc=1, device_id={"tm": other})
    pl.semaphore_wait(barrier, len(order) + int(lifting))

    lifts = []
    if lifting:
        lifts = [
            pltpu.make_async_remote_copy(
                src_ref=source,
                dst_ref=target,
                send_sem=up.at[index],
                recv_sem=down.at[index],
                device_id={"tm": other},
            )
            for index, (source, target) in enumerate([(code, got), (scale, got_scale)])
        ]

        @pl.when(upper)
        def _():
            for copy in lifts:
                copy.start()

    def copy(place, mask, source, target):
        return pltpu.make_async_remote_copy(
            src_ref=src.at[target, begin + place],
            dst_ref=dst.at[source, begin + place],
            send_sem=send.at[place, mask],
            recv_sem=recv.at[place, mask],
            device_id=device(me ^ mask),
        )

    @pl.loop(0, count)
    def _(place):
        for mask in order:
            copy(place, mask, me, me ^ mask).start()

    read = pltpu.make_async_copy(src.at[me, pl.ds(begin, count)], tmp, local.at[0])
    read.start()
    read.wait()
    write = pltpu.make_async_copy(tmp, dst.at[me, pl.ds(begin, count)], local.at[1])
    write.start()
    write.wait()

    @pl.loop(0, count)
    def _(place):
        for mask in order:
            copy(place, mask, me ^ mask, me).wait_recv()
            copy(place, mask, me, me ^ mask).wait_send()

    if lifting:

        @pl.when(upper)
        def _():
            for copy in lifts:
                copy.wait_send()

        @pl.when(jnp.logical_not(upper))
        def _():
            for copy in lifts:
                copy.wait_recv()


def spread(plan, packed, begin, count, collective, *more):
    sem = pltpu.SemaphoreType.DMA
    lifting = bool(more)
    shape = lambda value: jax.ShapeDtypeStruct(value.shape, value.dtype)
    scratch = [
        pltpu.VMEM((count,) + packed.shape[2:], packed.dtype),
        sem((count, plan.slices)),
        sem((count, plan.slices)),
        sem((2,)),
    ]
    if lifting:
        scratch += [sem((2,)), sem((2,))]
    return pl.pallas_call(
        functools.partial(spread_kernel, plan, begin, count, lifting),
        out_shape=tuple(shape(value) for value in (more or (packed,))),
        in_specs=[ANY] * (1 + len(more)),
        out_specs=(ANY,) * max(1, len(more)),
        scratch_shapes=scratch,
        input_output_aliases={1: 0} if lifting else {},
        compiler_params=pltpu.CompilerParams(collective_id=collective, has_side_effects=True),
    )(packed, *more)


def partial_sum(plan, upper, hop, w_ref, in_ref, part):
    first = (plan.half * plan.hops if upper else 0) + plan.frames - 1
    total = None
    for index in range(plan.half * plan.hops):
        source, local = divmod(index, plan.hops)
        term = w_ref[first + index - hop] * in_ref[source, 0, 0, local, part].astype(jnp.float32)
        total = term if total is None else total + term
    return total


def encode(parts, out_ref, scale_ref, place, scale_row):
    top = jnp.max(jnp.maximum(jnp.abs(parts[0]), jnp.abs(parts[1])), axis=0, keepdims=True)
    top = jnp.maximum(top, 1e-30)
    factor = TOP / top
    for part in range(2):
        code = jnp.round(parts[part] * factor).astype(jnp.int32)
        out_ref[place, part] = code.astype(jnp.int16)
    scale_ref[pl.ds(scale_row, 1), :] = top * (1.0 / TOP)


def upper_kernel(plan, late, meta, reqs, in_ref, w_ref, out_ref, scale_ref):
    index = pl.program_id(0)
    begin = plan.first if late else 0

    @pl.when((index < meta[1]) & (meta[2] >= plan.half))
    def _():
        first, last, offset = reqs[2, index], reqs[3, index], reqs[4, index]
        split = jnp.clip(first + plan.first - offset, first, last)

        @pl.loop(split if late else first, last if late else split)
        def _(hop):
            parts = [partial_sum(plan, True, hop, w_ref, in_ref, part) for part in range(2)]
            place = offset + hop - first - begin
            encode(parts, out_ref, scale_ref, place, place)


def lower_kernel(
    plan, meta, reqs, pos, in_ref, w_ref, got_0, scale_0, got_1, scale_1, out_ref, scale_ref
):
    index = pl.program_id(0)

    @pl.when((index < meta[1]) & (meta[2] < plan.half))
    def _():
        first, last, offset = reqs[2, index], reqs[3, index], reqs[4, index]
        split = jnp.clip(first + plan.first - offset, first, last)

        def add(got_ref, got_scale, begin, hop):
            unit = offset + hop - first - begin
            scale = got_scale[pl.ds(unit, 1), :]
            parts = []
            for part in range(2):
                other = got_ref[unit, part].astype(jnp.int32).astype(jnp.float32) * scale
                parts.append(partial_sum(plan, False, hop, w_ref, in_ref, part) + other)
            place = pos[index * plan.frames + hop]
            encode(parts, out_ref, scale_ref, place, place)

        @pl.loop(first, split)
        def _(hop):
            add(got_0, scale_0, 0, hop)

        @pl.loop(split, last)
        def _(hop):
            add(got_1, scale_1, plan.first, hop)


def filter_specs(plan, low, high):
    def request(i, m):
        bottom = m[low] if low else 0
        return jnp.maximum(jnp.clip(i, bottom, m[high] - 1), 0)

    taps = plan.frames - 1 + plan.all_hops
    return [
        pl.BlockSpec(
            (plan.half, 1, 1, plan.hops, 2, plan.span, BLOCKW),
            lambda i, m, r, *_: (0, r[0, request(i, m)], r[1, request(i, m)], 0, 0, 0, 0),
        ),
        pl.BlockSpec((taps, plan.span, BLOCKW), lambda i, *_: (0, 0, 0)),
    ]


def whole(*dims):
    return pl.BlockSpec(dims, lambda i, *_: (0,) * len(dims))


def filter_upper(plan, late, spreaded, weights, meta, reqs):
    units = plan.rest if late else plan.first
    return pl.pallas_call(
        functools.partial(upper_kernel, plan, late),
        out_shape=(
            jax.ShapeDtypeStruct((units, 2, plan.span, BLOCKW), jnp.int16),
            jax.ShapeDtypeStruct((units, BLOCKW), jnp.float32),
        ),
        grid_spec=pltpu.PrefetchScalarGridSpec(
            num_scalar_prefetch=2,
            grid=(plan.owners * MAXREQ,),
            in_specs=filter_specs(plan, 4 if late else 0, 1 if late else 3),
            out_specs=(whole(units, 2, plan.span, BLOCKW), whole(units, BLOCKW)),
        ),
    )(meta, reqs, spreaded, weights)


def filter_lower(plan, spreaded, weights, got, meta, reqs, pos):
    rows = plan.keepers * plan.owners * plan.deep
    return pl.pallas_call(
        functools.partial(lower_kernel, plan),
        out_shape=(
            jax.ShapeDtypeStruct((rows, 2, plan.span, BLOCKW), jnp.int16),
            jax.ShapeDtypeStruct((rows, BLOCKW), jnp.float32),
        ),
        grid_spec=pltpu.PrefetchScalarGridSpec(
            num_scalar_prefetch=3,
            grid=(plan.owners * MAXREQ,),
            in_specs=filter_specs(plan, 0, 1) + [whole(*value.shape) for value in got],
            out_specs=(whole(rows, 2, plan.span, BLOCKW), whole(rows, BLOCKW)),
        ),
    )(meta, reqs, pos, spreaded, weights, *got)


def lift_kernel(plan, count, src, src_scale, dst, dst_scale, send, recv):
    row = lax.axis_index("tm")
    barrier = pltpu.get_barrier_semaphore()
    upper = row >= plan.half
    other = jnp.where(upper, row - plan.half, row + plan.half)
    pl.semaphore_signal(barrier, inc=1, device_id={"tm": other})
    pl.semaphore_wait(barrier, 1)
    refs = [(src, dst), (src_scale, dst_scale)]
    copies = [
        pltpu.make_async_remote_copy(
            src_ref=source.at[pl.ds(0, count)],
            dst_ref=target.at[pl.ds(0, count)],
            send_sem=send.at[index],
            recv_sem=recv.at[index],
            device_id={"tm": other},
        )
        for index, (source, target) in enumerate(refs)
    ]

    @pl.when(upper)
    def _():
        for copy in copies:
            copy.start()
        for copy in copies:
            copy.wait_send()

    @pl.when(jnp.logical_not(upper))
    def _():
        for copy in copies:
            copy.wait_recv()


def lift(plan, values, scales, count, collective):
    sem = pltpu.SemaphoreType.DMA
    return pl.pallas_call(
        functools.partial(lift_kernel, plan, count),
        out_shape=(
            jax.ShapeDtypeStruct(values.shape, values.dtype),
            jax.ShapeDtypeStruct(scales.shape, scales.dtype),
        ),
        in_specs=[ANY, ANY],
        out_specs=(ANY, ANY),
        scratch_shapes=[sem((2,)), sem((2,))],
        compiler_params=pltpu.CompilerParams(collective_id=collective, has_side_effects=True),
    )(values, scales)


def deliver_kernel(plan, count, src, src_scale, dst, dst_scale, tmp, tmp_scale, send, recv, local):
    row, col = lax.axis_index("tm"), lax.axis_index("chan")
    size, lines = plan.slices, plan.keepers * plan.owners
    me = row * plan.owners + col
    barrier = pltpu.get_barrier_semaphore()

    def device(index):
        return {"tm": lax.div(index, plan.owners), "chan": lax.rem(index, plan.owners)}

    pieces = [(first, min(3, count - first)) for first in range(0, count, 3)]

    def value(index, mask, source, target):
        first, extent = pieces[index]
        return pltpu.make_async_remote_copy(
            src_ref=src.at[target, pl.ds(first, extent)],
            dst_ref=dst.at[source, pl.ds(first, extent)],
            send_sem=send.at[index, mask],
            recv_sem=recv.at[index, mask],
            device_id=device(me ^ mask),
        )

    def scale(mask, source, target):
        return pltpu.make_async_remote_copy(
            src_ref=src_scale.at[target],
            dst_ref=dst_scale.at[source],
            send_sem=send.at[len(pieces), mask],
            recv_sem=recv.at[len(pieces), mask],
            device_id=device(me ^ mask),
        )

    def targets(mask, act):
        @pl.when((me ^ mask) < lines)
        def _():
            act()

    @pl.when(row < plan.half)
    def _():
        for mask in plan.masks:
            pl.semaphore_signal(barrier, inc=1, device_id=device(me ^ mask))
        pl.semaphore_wait(barrier, size - 1)

        for mask in plan.masks:
            targets(mask, lambda: scale(mask, me, me ^ mask).start())
        for index in range(len(pieces)):
            for mask in plan.masks:
                targets(mask, lambda: value(index, mask, me, me ^ mask).start())

        @pl.when(me < lines)
        def _():
            moves = [
                (src.at[me, pl.ds(0, count)], tmp, dst.at[me, pl.ds(0, count)]),
                (src_scale.at[me], tmp_scale, dst_scale.at[me]),
            ]
            for index, (source, middle, target) in enumerate(moves):
                read = pltpu.make_async_copy(source, middle, local.at[2 * index])
                read.start()
                read.wait()
                write = pltpu.make_async_copy(middle, target, local.at[2 * index + 1])
                write.start()
                write.wait()

            for mask in plan.masks:
                scale(mask, me ^ mask, me).wait_recv()
                for index in range(len(pieces)):
                    value(index, mask, me ^ mask, me).wait_recv()

        for mask in plan.masks:

            def drain():
                scale(mask, me, me ^ mask).wait_send()
                for index in range(len(pieces)):
                    value(index, mask, me, me ^ mask).wait_send()

            targets(mask, drain)


def deliver(plan, values, scales, count, collective):
    sem = pltpu.SemaphoreType.DMA
    inner = values.shape[1:]
    return pl.pallas_call(
        functools.partial(deliver_kernel, plan, count),
        out_shape=(
            jax.ShapeDtypeStruct((plan.slices,) + inner, values.dtype),
            jax.ShapeDtypeStruct((plan.slices,) + scales.shape[1:], scales.dtype),
        ),
        in_specs=[ANY, ANY],
        out_specs=(ANY, ANY),
        scratch_shapes=[
            pltpu.VMEM((count,) + inner[1:], values.dtype),
            pltpu.VMEM(scales.shape[1:], scales.dtype),
            sem((-(-count // 3) + 1, plan.slices)),
            sem((-(-count // 3) + 1, plan.slices)),
            sem((4,)),
        ],
        compiler_params=pltpu.CompilerParams(collective_id=collective, has_side_effects=True),
    )(values, scales)


def transform_kernel(plan, omap, in_ref, scale_ref, table_ref, turn_ref, out_ref, ys, zs):
    entry = omap[pl.program_id(0)]

    @pl.when(entry < 0)
    def _():
        out_ref[...] = jnp.zeros_like(out_ref)

    @pl.when(entry >= 0)
    def _():
        chunk = 32

        def load(part, first):
            piece, line = divmod(first, plan.span)
            code = in_ref[piece, 0, part, line : line + chunk, :]
            scale = scale_ref[piece, pl.ds(entry, 1), :]
            return code.astype(jnp.int32).astype(jnp.float32) * scale

        for line in range(0, SUB, chunk):
            re = [load(0, SUB * a + line) for a in range(RADIX)]
            im = [load(1, SUB * a + line) for a in range(RADIX)]
            es, ed = re[0] + re[2], re[0] - re[2]
            fs, fd = im[0] + im[2], im[0] - im[2]
            gs, gd = re[1] + re[3], re[1] - re[3]
            hs, hd = im[1] + im[3], im[1] - im[3]
            mixed = [
                (es + gs, fs + hs),
                (ed + hd, fd - gd),
                (es - gs, fs - hs),
                (ed - hd, fd + gd),
            ]
            rows = slice(line, line + chunk)
            for q in range(RADIX):
                real, imag = mixed[q]
                if q:
                    cosine, sine = turn_ref[0, q - 1, rows, :], turn_ref[1, q - 1, rows, :]
                    real, imag = real * cosine + imag * sine, imag * cosine - real * sine
                for part, value in enumerate((real, imag)):
                    cols = slice(part * BLOCKW, (part + 1) * BLOCKW)
                    high = value.astype(jnp.bfloat16)
                    ys[q, rows, cols] = high
                    ys[q, SUB + line : SUB + line + chunk, cols] = (
                        value - high.astype(jnp.float32)
                    ).astype(jnp.bfloat16)
                    ys[q, 2 * SUB + line : 2 * SUB + line + chunk, cols] = high

        for q in range(RADIX):
            both = jnp.dot(table_ref[...], ys[q], preferred_element_type=jnp.float32)
            rows = pl.ds(q, SUB, stride=RADIX)
            zs[0, rows, :] = both[:SUB, :BLOCKW] + both[SUB:, BLOCKW:]
            zs[1, rows, :] = both[:SUB, BLOCKW:] - both[SUB:, :BLOCKW]

        out_ref[0, 0] = zs[...].astype(out_ref.dtype)


def transform_tables():
    line = np.arange(SUB)
    angles = (line[:, None] * line[None, :] % SUB) * (2.0 * np.pi / SUB)
    table = np.concatenate([np.cos(angles), np.sin(angles)], axis=0) / math.sqrt(NFINE)
    table = table.astype(np.float32)
    high = table.astype(jnp.bfloat16)
    low = (table - high.astype(np.float32)).astype(jnp.bfloat16)
    turns = np.arange(1, RADIX)[:, None] * line[None, :] * (2.0 * np.pi / NFINE)
    turn = np.stack([np.cos(turns), np.sin(turns)]).astype(np.float32)
    return np.concatenate([high, high, low], axis=1), turn


def transform(plan, values, scales, omap):
    table, turn = transform_tables()
    turn = jnp.asarray(np.ascontiguousarray(np.broadcast_to(turn[..., None], turn.shape + (BLOCKW,))))
    return pl.pallas_call(
        functools.partial(transform_kernel, plan),
        out_shape=jax.ShapeDtypeStruct((plan.hops, MAXREQ, 2, NFINE, BLOCKW), jnp.bfloat16),
        grid_spec=pltpu.PrefetchScalarGridSpec(
            num_scalar_prefetch=1,
            grid=(plan.hops * MAXREQ,),
            in_specs=[
                pl.BlockSpec(
                    (plan.slices, 1, 2, plan.span, BLOCKW),
                    lambda i, o: (0, jnp.maximum(o[i], 0), 0, 0, 0),
                ),
                whole(*scales.shape),
                whole(2 * SUB, 3 * SUB),
                whole(2, RADIX - 1, SUB, BLOCKW),
            ],
            out_specs=pl.BlockSpec(
                (1, 1, 2, NFINE, BLOCKW), lambda i, o: (i // MAXREQ, i % MAXREQ, 0, 0, 0)
            ),
            scratch_shapes=[
                pltpu.VMEM((RADIX, 3 * SUB, 2 * BLOCKW), jnp.bfloat16),
                pltpu.VMEM((2, NFINE, BLOCKW), jnp.float32),
            ],
        ),
    )(omap, values, scales, jnp.asarray(table), turn)


def owners_power(value):
    return value & (value - 1) == 0


class Plan:
    def __init__(self, size, owners, hops, per_column):
        self.size, self.owners, self.hops, self.per_column = size, owners, hops, per_column
        self.all_hops = hops * size
        self.frames = self.all_hops - TAPS + 1
        self.keepers = -(-self.frames // hops)
        self.half = size // 2
        self.slices = self.half * owners
        self.span = NFINE // self.slices
        self.fill = owners * PAIR
        self.deep = round_up(hops * MAXREQ, 8)
        self.lead = min(2, self.fill)
        self.first = 40
        self.rest = round_up(owners * MAXREQ * self.frames, 8)
        more = self.fill - self.lead
        self.fills = sorted({max(1, round_up(more * i, 6) // 6) for i in (1, 2, 3, 4, 6)})
        near = {min(8 * i, self.rest) for i in (1, 2, 3, 4, 5, 7, 9)}
        self.counts = sorted(near | {self.rest})
        most = hops * MAXREQ
        self.depths = sorted({round_up(most * i, 12) // 12 for i in (5, 6, 7, 8, 9, 10, 11, 12)})

        spread = sorted(range(2, self.slices), key=lambda mask: bin(mask >> 1).count("1"))
        self.masks = spread + [1]

    def fits(self):
        powers = self.slices & (self.slices - 1) == 0 and owners_power(self.owners)
        even = powers and self.size % 2 == 0 and NFINE % self.slices == 0 and self.span % 32 == 0
        return even and self.keepers <= self.half


def shards(coarse, prototype, req_block, req_start, req_frames, req_count):
    owners, size = lax.axis_size("chan"), lax.axis_size("tm")
    plan = Plan(size, owners, coarse.shape[1] // NFINE, coarse.shape[2] // BLOCKW)
    if not plan.fits():
        return shards_general(coarse, prototype, req_block, req_start, req_frames, req_count)
    tables = make_tables(plan, req_block, req_start, req_frames, req_count)
    meta, chosen, reqs, pos, omap, pick_a, pick_b, pick_c = tables
    packed = gather(plan, coarse, meta, chosen)

    me = lax.axis_index("tm") % plan.half * owners + lax.axis_index("chan")
    mine = lax.dynamic_slice(prototype, (0, me * plan.span), (TAPS, plan.span))
    mine = jnp.pad(mine, ((plan.frames - 1, plan.all_hops - TAPS), (0, 0)))
    weights = jnp.broadcast_to(mine[:, :, None], mine.shape + (BLOCKW,))

    def split(value):
        return value.reshape((plan.half, owners) + value.shape[1:])

    spreaded = spread(plan, packed, 0, plan.lead, 0)[0]
    early = filter_upper(plan, False, split(spreaded), weights, meta, reqs)

    def second(count, collective, *operands):
        return spread(plan, operands[0], plan.lead, count, collective, *operands[1:])

    branches = [functools.partial(second, size, 1 + i) for i, size in enumerate(plan.fills)]
    spreaded, *got = lax.switch(pick_a[0], branches, packed, spreaded, *early)
    spreaded = split(spreaded)
    late = filter_upper(plan, True, spreaded, weights, meta, reqs)
    base = 1 + len(branches)
    branches = [
        functools.partial(lambda n, c, *x: lift(plan, *x, n, c), size, base + i)
        for i, size in enumerate(plan.counts)
    ]
    got += lax.switch(pick_b[0], branches, *late)
    values, scales = filter_lower(plan, spreaded, weights, got, meta, reqs, pos)
    lines = plan.keepers * owners
    values = values.reshape((lines, plan.deep) + values.shape[1:])
    scales = scales.reshape((lines, plan.deep) + scales.shape[1:])
    base += len(branches)
    branches = [
        functools.partial(lambda n, c, *x: deliver(plan, *x, n, c), size, base + i)
        for i, size in enumerate(plan.depths)
    ]
    values, scales = lax.switch(pick_c[0], branches, values, scales)
    return transform(plan, values, scales, omap)[:, None]


def solution(mesh):
    return jax.shard_map(
        shards,
        mesh=mesh,
        in_specs=(P(None, "tm", "chan"), P(), P(), P(), P(), P()),
        out_specs=P("tm", "chan", None, None, None, None),
        check_vma=False,
    )
```

```python
import functools
import math

import jax
import jax.numpy as jnp
import numpy as np
from jax import lax
from jax.experimental import pallas as pl
from jax.experimental.pallas import tpu as pltpu
from jax.sharding import PartitionSpec as P

BLOCKW = 128
NFINE = 1024
TAPS = 16
MAXREQ = 4
PAIR = 2
ROWS = 128
STEP = 16
ANY = pl.BlockSpec(memory_space=pl.ANY)


def build_table():
    line = jnp.arange(NFINE, dtype=jnp.int32)
    products = line[:, None] * line[None, :] % NFINE
    angles = products.astype(jnp.float32) * (2.0 * math.pi / NFINE)
    scale = 1.0 / math.sqrt(NFINE)
    return jnp.concatenate([jnp.cos(angles) * scale, jnp.sin(angles) * scale], axis=0)


def pack_kernel(chosen, coarse_ref, out_ref):
    out_ref[...] = coarse_ref[...].reshape(out_ref.shape)


def pack(coarse, chosen, first, hops):
    count = chosen.shape[0]
    return pl.pallas_call(
        pack_kernel,
        out_shape=jax.ShapeDtypeStruct((count, 2, hops * NFINE, BLOCKW), coarse.dtype),
        grid_spec=pltpu.PrefetchScalarGridSpec(
            num_scalar_prefetch=1,
            grid=(count,),
            in_specs=[pl.BlockSpec((2, hops * NFINE, BLOCKW), lambda i, c: (0, first, c[i]))],
            out_specs=pl.BlockSpec((1, 2, hops * NFINE, BLOCKW), lambda i, c: (i, 0, 0, 0)),
        ),
        cost_estimate=pl.CostEstimate(
            flops=0, transcendentals=0, bytes_accessed=count * 8 * hops * NFINE * BLOCKW
        ),
    )(chosen, coarse)


def select_kernel(pieces, arrival, in_ref, out_ref):
    share = BLOCKW // pieces
    for piece in range(pieces):
        cols = slice(piece * share, (piece + 1) * share)
        out_ref[piece] = jnp.concatenate([in_ref[0, 0, :, cols], in_ref[0, 1, :, cols]], axis=-1)


def select(incoming, arrival, pieces, hops):
    width = 2 * BLOCKW // pieces
    rows = hops * NFINE
    return pl.pallas_call(
        functools.partial(select_kernel, pieces),
        out_shape=jax.ShapeDtypeStruct((MAXREQ * pieces, rows, width), incoming.dtype),
        grid_spec=pltpu.PrefetchScalarGridSpec(
            num_scalar_prefetch=1,
            grid=(MAXREQ, hops),
            in_specs=[pl.BlockSpec((1, 2, NFINE, BLOCKW), lambda q, h, a: (a[q], 0, h, 0))],
            out_specs=pl.BlockSpec((pieces, NFINE, width), lambda q, h, a: (q, h, 0)),
        ),
        cost_estimate=pl.CostEstimate(
            flops=0, transcendentals=0, bytes_accessed=MAXREQ * 8 * rows * BLOCKW
        ),
    )(arrival, incoming)


def exchange_kernel(
    owners, size, a_in, b_in, a_out, b_out, a_tmp, b_tmp, a_send, a_recv, b_send, b_recv, local
):
    column, row = lax.axis_index("chan"), lax.axis_index("tm")
    barrier = pltpu.get_barrier_semaphore()

    @pl.loop(1, owners)
    def _(step):
        other = lax.rem(column + step, owners)
        pl.semaphore_signal(barrier, inc=1, device_id={"chan": other})

    @pl.loop(1, size)
    def _(step):
        other = lax.rem(row + step, size)
        pl.semaphore_signal(barrier, inc=1, device_id={"tm": other})

    pl.semaphore_wait(barrier, owners + size - 2)

    def a_copy(step, source, target, device):
        return pltpu.make_async_remote_copy(
            src_ref=a_in.at[pl.ds(target * PAIR, PAIR)],
            dst_ref=a_out.at[pl.ds(source * PAIR, PAIR)],
            send_sem=a_send.at[step],
            recv_sem=a_recv.at[step],
            device_id={"chan": device},
        )

    def b_copy(step, source, target, device):
        return pltpu.make_async_remote_copy(
            src_ref=b_in.at[target],
            dst_ref=b_out.at[source],
            send_sem=b_send.at[step],
            recv_sem=b_recv.at[step],
            device_id={"tm": device},
        )

    @pl.loop(1, size)
    def _(step):
        target = lax.rem(row + step, size)
        b_copy(step, row, target, target).start()

    @pl.loop(1, owners)
    def _(step):
        target = lax.rem(column + step, owners)
        a_copy(step, column, target, target).start()

    a_read = pltpu.make_async_copy(a_in.at[pl.ds(column * PAIR, PAIR)], a_tmp, local.at[0])
    b_read = pltpu.make_async_copy(b_in.at[row], b_tmp, local.at[1])
    a_read.start()
    b_read.start()
    a_read.wait()
    b_read.wait()
    a_write = pltpu.make_async_copy(a_tmp, a_out.at[pl.ds(column * PAIR, PAIR)], local.at[2])
    b_write = pltpu.make_async_copy(b_tmp, b_out.at[row], local.at[3])
    a_write.start()
    b_write.start()
    a_write.wait()
    b_write.wait()

    @pl.loop(1, owners)
    def _(step):
        source = lax.rem(column + owners - step, owners)
        copy = a_copy(step, source, column, source)
        copy.wait_recv()
        copy.wait_send()

    @pl.loop(1, size)
    def _(step):
        source = lax.rem(row + size - step, size)
        copy = b_copy(step, source, row, source)
        copy.wait_recv()
        copy.wait_send()


def exchange(outgoing, sending, owners, size, collective):
    sem = pltpu.SemaphoreType.DMA
    return pl.pallas_call(
        functools.partial(exchange_kernel, owners, size),
        out_shape=(
            jax.ShapeDtypeStruct(outgoing.shape, outgoing.dtype),
            jax.ShapeDtypeStruct(sending.shape, sending.dtype),
        ),
        in_specs=[ANY, ANY],
        out_specs=(ANY, ANY),
        scratch_shapes=[
            pltpu.VMEM((PAIR,) + outgoing.shape[1:], outgoing.dtype),
            pltpu.VMEM(sending.shape[1:], sending.dtype),
            sem((owners,)),
            sem((owners,)),
            sem((size,)),
            sem((size,)),
            sem((4,)),
        ],
        compiler_params=pltpu.CompilerParams(collective_id=collective, has_side_effects=True),
    )(outgoing, sending)


def filter_kernel(hops, frames, weights_ref, *refs):
    out_ref = refs[-1]
    width = refs[0].shape[-1]

    @pl.loop(0, ROWS // STEP)
    def _(step):
        rows = pl.ds(pl.multiple_of(step * STEP, STEP), STEP)
        weights = [
            jnp.broadcast_to(weights_ref[rows, tap : tap + 1], (STEP, width)) for tap in range(TAPS)
        ]
        for frame in range(frames):
            total = None
            for tap in range(TAPS):
                hop = frame + tap
                term = weights[tap] * refs[hop % hops][hop // hops, rows, :].astype(jnp.float32)
                total = term if total is None else total + term
            out_ref[rows, frame * width : (frame + 1) * width] = total


def polyphase(parts, prototype, frames):
    hops = len(parts)
    size, _, width = parts[0].shape
    return pl.pallas_call(
        functools.partial(filter_kernel, hops, frames),
        out_shape=jax.ShapeDtypeStruct((NFINE, frames * width), jnp.float32),
        grid=(NFINE // ROWS,),
        in_specs=[pl.BlockSpec((ROWS, TAPS), lambda i: (i, 0))]
        + [pl.BlockSpec((size, ROWS, width), lambda i: (0, i, 0))] * hops,
        out_specs=pl.BlockSpec((ROWS, frames * width), lambda i: (i, 0)),
    )(prototype.T, *parts)


def combine_kernel(frames, share, both_ref, out_ref):
    frame = pl.program_id(0)

    @pl.when(frame < frames)
    def _():
        sine = both_ref[1]
        turned = jnp.concatenate([sine[:, share:], -sine[:, :share]], axis=-1)
        out_ref[0] = (both_ref[0] + turned).astype(out_ref.dtype)

    @pl.when(frame >= frames)
    def _():
        out_ref[...] = jnp.zeros_like(out_ref)


def combine(both, frames, padded, width):
    return pl.pallas_call(
        functools.partial(combine_kernel, frames, width // 2),
        out_shape=jax.ShapeDtypeStruct((padded, NFINE, width), jnp.bfloat16),
        grid=(padded,),
        in_specs=[
            pl.BlockSpec((2, NFINE, width), lambda f: (0, 0, jnp.minimum(f, frames - 1))),
        ],
        out_specs=pl.BlockSpec((1, NFINE, width), lambda f: (f, 0, 0)),
    )(both)


def return_kernel(size, keepers, hops, res_ref, out_ref, send_sems, recv_sems):
    me = lax.axis_index("tm")
    barrier = pltpu.get_barrier_semaphore()

    @pl.loop(1, size)
    def _(step):
        other = lax.rem(me + step, size)
        pl.semaphore_signal(barrier, inc=1, device_id={"tm": other})

    pl.semaphore_wait(barrier, size - 1)

    def copy(step):
        target = lax.rem(me + step, size)
        return pltpu.make_async_remote_copy(
            src_ref=res_ref.at[pl.ds(target * hops, hops)],
            dst_ref=out_ref.at[me],
            send_sem=send_sems.at[step],
            recv_sem=recv_sems.at[step],
            device_id={"tm": target},
        )

    def arriving(step):
        source = lax.rem(me + size - step, size)
        return pltpu.make_async_remote_copy(
            src_ref=res_ref.at[pl.ds(0, hops)],
            dst_ref=out_ref.at[source],
            send_sem=send_sems.at[step],
            recv_sem=recv_sems.at[step],
            device_id={"tm": source},
        )

    @pl.loop(1, size)
    def _(step):
        @pl.when(lax.rem(me + step, size) < keepers)
        def _():
            copy(step).start()

    @pl.when(me < keepers)
    def _():
        @pl.loop(1, size)
        def _(step):
            arriving(step).wait_recv()

    @pl.loop(1, size)
    def _(step):
        @pl.when(lax.rem(me + step, size) < keepers)
        def _():
            copy(step).wait_send()


def give_back(result, size, keepers, hops):
    shape = (size, hops) + result.shape[1:]
    return pl.pallas_call(
        functools.partial(return_kernel, size, keepers, hops),
        out_shape=jax.ShapeDtypeStruct(shape, result.dtype),
        in_specs=[ANY],
        out_specs=ANY,
        scratch_shapes=[pltpu.SemaphoreType.DMA((size,)), pltpu.SemaphoreType.DMA((size,))],
        compiler_params=pltpu.CompilerParams(collective_id=0, has_side_effects=True),
    )(result)


def final_kernel(pieces, meta, got_ref, own_ref, out_ref):
    share = BLOCKW // pieces
    slot, hop = pl.program_id(0), pl.program_id(1)
    row = meta[0]
    active = meta[2 + slot * pl.num_programs(1) + hop] > 0

    @pl.when(jnp.logical_not(active))
    def _():
        out_ref[...] = jnp.zeros_like(out_ref)

    @pl.when(active)
    def _():
        data = [
            jnp.where(slot * pieces + piece == row, own_ref[0], got_ref[piece, 0])
            for piece in range(pieces)
        ]
        for part in range(2):
            cols = slice(part * share, (part + 1) * share)
            out_ref[0, 0, part] = jnp.concatenate([d[:, cols] for d in data], axis=-1)


def assemble(got, result, active, row, keepers, pieces):
    size, hops, _, width = got.shape
    base = jnp.minimum(row, keepers - 1) * hops
    meta = jnp.concatenate(
        [jnp.stack([row, base]).astype(jnp.int32), active.astype(jnp.int32).reshape(-1)]
    )
    return pl.pallas_call(
        functools.partial(final_kernel, pieces),
        out_shape=jax.ShapeDtypeStruct((hops, MAXREQ, 2, NFINE, BLOCKW), got.dtype),
        grid_spec=pltpu.PrefetchScalarGridSpec(
            num_scalar_prefetch=1,
            grid=(MAXREQ, hops),
            in_specs=[
                pl.BlockSpec((pieces, 1, NFINE, width), lambda q, h, m: (q, h, 0, 0)),
                pl.BlockSpec((1, NFINE, width), lambda q, h, m: (m[1] + h, 0, 0)),
            ],
            out_specs=pl.BlockSpec((1, 1, 2, NFINE, BLOCKW), lambda q, h, m: (h, q, 0, 0, 0)),
        ),
    )(meta, got, result)


def shards_general(coarse, prototype, req_block, req_start, req_frames, req_count):
    owners = lax.axis_size("chan")
    column = lax.axis_index("chan")
    row = lax.axis_index("tm")
    size = lax.axis_size("tm")
    per_column = coarse.shape[2] // BLOCKW
    hops = coarse.shape[1] // NFINE
    all_hops = hops * size
    frames = all_hops - TAPS + 1
    keepers = -(-frames // hops)
    pieces = size // MAXREQ
    width = 2 * BLOCKW // pieces
    share = BLOCKW // pieces

    slot_ids = jnp.arange(MAXREQ, dtype=jnp.int32)
    live = slot_ids[None, :] < req_count[:, None]
    sources = req_block // per_column
    same = (
        live[:, :, None]
        & live[:, None, :]
        & (sources[:, :, None] == sources[:, None, :])
        & (slot_ids[None, None, :] < slot_ids[None, :, None])
    )
    rank = jnp.sum(same.astype(jnp.int32), axis=2)
    picked = (
        (live & (sources == column))[:, None, :]
        & (rank[:, None, :] == jnp.arange(PAIR, dtype=jnp.int32)[None, :, None])
    )
    local = req_block - column * per_column
    chosen = jnp.sum(jnp.where(picked, local[:, None, :], 0), axis=2).reshape(-1)
    chosen = jnp.clip(chosen, 0, per_column - 1).astype(jnp.int32)
    mine = (jnp.arange(owners, dtype=jnp.int32) == column)[:, None]

    def own(table):
        return jnp.sum(jnp.where(mine, table, 0), axis=0)

    my_live = slot_ids < own(req_count[:, None])[0]
    arrival = jnp.where(my_live, own(sources) * PAIR + own(rank), 0)
    arrival = jnp.clip(arrival, 0, owners * PAIR - 1).astype(jnp.int32)
    my_start, my_frames = own(req_start), own(req_frames)
    hop_ids = row * hops + jnp.arange(hops, dtype=jnp.int32)
    active = (
        my_live[:, None]
        & (hop_ids[None, :] >= my_start[:, None])
        & (hop_ids[None, :] < (my_start + my_frames)[:, None])
    )

    table = build_table()
    outgoing = [pack(coarse, chosen, hop, 1) for hop in range(hops)]
    incoming = lax.all_to_all(outgoing[0], "chan", split_axis=0, concat_axis=0, tiled=True)
    parts = []
    for hop in range(1, hops):
        sending = select(incoming, arrival, pieces, 1)
        incoming, gathered = exchange(outgoing[hop], sending, owners, size, hop)
        parts.append(gathered)
    sending = select(incoming, arrival, pieces, 1)
    parts.append(lax.all_to_all(sending, "tm", split_axis=0, concat_axis=0, tiled=True))
    flat = polyphase(parts, prototype, frames)
    both = jnp.dot(table, flat, precision=lax.Precision.HIGH, preferred_element_type=jnp.float32)
    padded = keepers * hops
    if width % 128 == 0:
        result = combine(both.reshape(2, NFINE, frames * width), frames, padded, width)
    else:
        both = both.reshape(2, NFINE, frames, 2, share)
        cosine, sine = both[0], both[1]
        result = jnp.stack(
            [cosine[:, :, 0] + sine[:, :, 1], cosine[:, :, 1] - sine[:, :, 0]], axis=2
        ).astype(jnp.bfloat16)
        result = result.reshape(NFINE, frames, width).transpose(1, 0, 2)
        if padded > frames:
            zeros = jnp.zeros((padded - frames, NFINE, width), result.dtype)
            result = jnp.concatenate([result, zeros], axis=0)
    got = give_back(result, size, keepers, hops)
    return assemble(got, result, active, row, keepers, pieces)[:, None]


SMEM = pl.BlockSpec(memory_space=pltpu.SMEM)
TOP = 32767.0
RADIX = 4
SUB = NFINE // RADIX


def round_up(value, unit):
    return -(-value // unit) * unit


def picked(value, sizes):
    return sum((value > size).astype(jnp.int32) for size in sizes[:-1])


def tables_kernel(
    plan, blk, start, nfr, cnt, meta, chosen, reqs, pos, omap, pick_a, pick_b, pick_c,
    columns, lists, early_lists, order, places, buckets
):
    row, col = lax.axis_index("tm"), lax.axis_index("chan")
    total = plan.owners * MAXREQ
    for i in range(plan.owners):
        columns[i] = 0
    for i in range(plan.keepers * plan.owners):
        lists[i] = 0
        early_lists[i] = 0
    for i in range(plan.hops * MAXREQ):
        omap[i] = -1
    for i in range(plan.fill):
        chosen[i] = 0

    for i in range(plan.frames + 1):
        buckets[i] = 0

    def fresh(item):
        owner, slot = lax.div(item, MAXREQ), lax.rem(item, MAXREQ)
        return slot < cnt[owner], nfr[owner, slot]

    @pl.loop(0, total)
    def _(item):
        alive, size = fresh(item)

        @pl.when(alive)
        def _():
            buckets[size] = buckets[size] + 1

    live = jnp.int32(0)
    for size in range(plan.frames, 0, -1):
        amount = buckets[size]
        buckets[size] = live
        live = live + amount

    @pl.loop(0, total)
    def _(item):
        alive, size = fresh(item)

        @pl.when(alive)
        def _():
            spot = buckets[size]
            buckets[size] = spot + 1
            order[spot] = item

    @pl.loop(0, live)
    def _(index):
        item = order[index]
        block = blk[lax.div(item, MAXREQ), lax.rem(item, MAXREQ)]
        source = lax.div(block, plan.per_column)
        place = columns[source]
        columns[source] = place + 1
        places[index] = place

        @pl.when(source == col)
        def _():
            chosen[place] = block - source * plan.per_column

    def request(index, carry, early):
        item = order[index]
        owner, slot = lax.div(item, MAXREQ), lax.rem(item, MAXREQ)

        def add(carry):
            count, units = carry
            first = start[owner, slot]
            last = first + nfr[owner, slot]
            reqs[0, count] = lax.div(blk[owner, slot], plan.per_column)
            reqs[1, count] = places[index]
            reqs[2, count] = first
            reqs[3, count] = last
            reqs[4, count] = units

            def frame(hop, carry):
                keeper = lax.div(hop, plan.hops)
                line = keeper * plan.owners + owner
                soon = early_lists[line]
                is_soon = (units + hop - first < plan.first) & (soon < plan.soon)
                late_entry = lists[line]
                early_lists[line] = soon + is_soon.astype(jnp.int32)
                lists[line] = late_entry + 1 - is_soon.astype(jnp.int32)
                pos[count * plan.frames + hop] = jnp.where(
                    is_soon, line * plan.soon + soon, -1 - (line * plan.deep + late_entry)
                )

                @pl.when((keeper == row) & (owner == col))
                def _():
                    omap[(hop - keeper * plan.hops) * MAXREQ + slot] = jnp.where(
                        is_soon, soon, plan.soon + late_entry
                    )

                return carry

            lax.fori_loop(first, last, frame, 0)
            return count + 1, units + last - first

        return lax.cond((places[index] < plan.lead) == early, add, lambda carry: carry, carry)

    zero = jnp.int32(0)
    early, units = lax.fori_loop(
        0, live, functools.partial(request, early=True), (zero, zero)
    )
    units = jnp.maximum(units, plan.first)
    count, units = lax.fori_loop(
        0, live, functools.partial(request, early=False), (early, units)
    )
    longest, deepest = jnp.int32(0), jnp.int32(0)
    for i in range(plan.owners):
        longest = jnp.maximum(longest, columns[i])
    for i in range(plan.keepers * plan.owners):
        deepest = jnp.maximum(deepest, lists[i])

    def before(index, found):
        return found + (reqs[3, index] - reqs[2, index] + reqs[4, index] <= plan.first).astype(
            jnp.int32
        )

    late = lax.fori_loop(0, early, before, zero)
    meta[0] = columns[col]
    meta[1] = count
    meta[2] = row
    meta[3] = early
    upper = row >= plan.half
    meta[4] = jnp.where(upper, late, 0)
    meta[5] = jnp.where(upper, count, early)
    pick_a[0] = picked(longest - plan.lead, plan.fills)
    pick_b[0] = picked(units - plan.first, plan.counts)
    pick_c[0] = picked(deepest, plan.depths)


def make_tables(plan, req_block, req_start, req_frames, req_count):
    total = plan.owners * MAXREQ
    shape = lambda *dims: jax.ShapeDtypeStruct(dims, jnp.int32)
    return pl.pallas_call(
        functools.partial(tables_kernel, plan),
        out_shape=(
            shape(8),
            shape(plan.fill),
            shape(5, total),
            shape(total * plan.frames),
            shape(plan.hops * MAXREQ),
            shape(1),
            shape(1),
            shape(1),
        ),
        in_specs=[SMEM] * 4,
        out_specs=(SMEM,) * 8,
        scratch_shapes=[
            pltpu.SMEM((plan.owners,), jnp.int32),
            pltpu.SMEM((plan.keepers * plan.owners,), jnp.int32),
            pltpu.SMEM((plan.keepers * plan.owners,), jnp.int32),
            pltpu.SMEM((total,), jnp.int32),
            pltpu.SMEM((total,), jnp.int32),
            pltpu.SMEM((plan.frames + 1,), jnp.int32),
        ],
    )(req_block, req_start, req_frames, req_count)


def gather_kernel(plan, meta, chosen, in_ref, out_ref):
    @pl.when(pl.program_id(1) < jnp.maximum(meta[0], 1))
    def _():
        for piece in range(plan.slices):
            out_ref[piece, 0, 0] = in_ref[:, piece * plan.span : (piece + 1) * plan.span, :]


def gather(plan, coarse, meta, chosen):
    def place(i, m):
        return jnp.minimum(i, jnp.maximum(m[0] - 1, 0))

    return pl.pallas_call(
        functools.partial(gather_kernel, plan),
        out_shape=jax.ShapeDtypeStruct(
            (plan.slices, plan.fill, plan.hops, 2, plan.span, BLOCKW), coarse.dtype
        ),
        grid_spec=pltpu.PrefetchScalarGridSpec(
            num_scalar_prefetch=2,
            grid=(plan.hops, plan.fill),
            in_specs=[
                pl.BlockSpec((2, NFINE, BLOCKW), lambda h, i, m, c: (0, h, c[place(i, m)]))
            ],
            out_specs=pl.BlockSpec(
                (plan.slices, 1, 1, 2, plan.span, BLOCKW),
                lambda h, i, m, c: (0, place(i, m), h, 0, 0, 0),
            ),
        ),
    )(meta, chosen, coarse)


def spread_kernel(plan, begin, count, lifting, *refs):
    if lifting:
        src, _, code, scale, dst, got, got_scale, tmp, send, recv, local, up, down = refs
    else:
        src, dst, tmp, send, recv, local = refs
    row, col = lax.axis_index("tm"), lax.axis_index("chan")
    base = lax.div(row, plan.half) * plan.half
    me = (row - base) * plan.owners + col
    upper = row >= plan.half
    other = jnp.where(upper, row - plan.half, row + plan.half)
    barrier = pltpu.get_barrier_semaphore()
    order = plan.masks

    def device(index):
        return {"tm": base + lax.div(index, plan.owners), "chan": lax.rem(index, plan.owners)}

    for mask in order:
        pl.semaphore_signal(barrier, inc=1, device_id=device(me ^ mask))
    if lifting:
        pl.semaphore_signal(barrier, inc=1, device_id={"tm": other})
    pl.semaphore_wait(barrier, len(order) + int(lifting))

    lifts = []
    if lifting:
        lifts = [
            pltpu.make_async_remote_copy(
                src_ref=source,
                dst_ref=target,
                send_sem=up.at[index],
                recv_sem=down.at[index],
                device_id={"tm": other},
            )
            for index, (source, target) in enumerate([(code, got), (scale, got_scale)])
        ]

        @pl.when(upper)
        def _():
            for copy in lifts:
                copy.start()

    def copy(place, mask, source, target):
        return pltpu.make_async_remote_copy(
            src_ref=src.at[target, begin + place],
            dst_ref=dst.at[source, begin + place],
            send_sem=send.at[place, mask],
            recv_sem=recv.at[place, mask],
            device_id=device(me ^ mask),
        )

    @pl.loop(0, count)
    def _(place):
        for mask in order:
            copy(place, mask, me, me ^ mask).start()

    read = pltpu.make_async_copy(src.at[me, pl.ds(begin, count)], tmp, local.at[0])
    read.start()
    read.wait()
    write = pltpu.make_async_copy(tmp, dst.at[me, pl.ds(begin, count)], local.at[1])
    write.start()
    write.wait()

    @pl.loop(0, count)
    def _(place):
        for mask in order:
            copy(place, mask, me ^ mask, me).wait_recv()
            copy(place, mask, me, me ^ mask).wait_send()

    if lifting:

        @pl.when(upper)
        def _():
            for copy in lifts:
                copy.wait_send()

        @pl.when(jnp.logical_not(upper))
        def _():
            for copy in lifts:
                copy.wait_recv()


def spread(plan, packed, begin, count, collective, *more):
    sem = pltpu.SemaphoreType.DMA
    lifting = bool(more)
    shape = lambda value: jax.ShapeDtypeStruct(value.shape, value.dtype)
    scratch = [
        pltpu.VMEM((count,) + packed.shape[2:], packed.dtype),
        sem((count, plan.slices)),
        sem((count, plan.slices)),
        sem((2,)),
    ]
    if lifting:
        scratch += [sem((2,)), sem((2,))]
    return pl.pallas_call(
        functools.partial(spread_kernel, plan, begin, count, lifting),
        out_shape=tuple(shape(value) for value in (more or (packed,))),
        in_specs=[ANY] * (1 + len(more)),
        out_specs=(ANY,) * max(1, len(more)),
        scratch_shapes=scratch,
        input_output_aliases={1: 0} if lifting else {},
        compiler_params=pltpu.CompilerParams(collective_id=collective, has_side_effects=True),
    )(packed, *more)


def partial_sum(plan, upper, hop, w_ref, in_ref, part):
    first = (plan.half * plan.hops if upper else 0) + plan.frames - 1
    total = None
    for index in range(plan.half * plan.hops):
        source, local = divmod(index, plan.hops)
        term = w_ref[first + index - hop] * in_ref[source, 0, 0, local, part].astype(jnp.float32)
        total = term if total is None else total + term
    return total


def encode(parts, out_ref, scale_ref, place, scale_row):
    top = jnp.max(jnp.maximum(jnp.abs(parts[0]), jnp.abs(parts[1])), axis=0, keepdims=True)
    top = jnp.maximum(top, 1e-30)
    factor = TOP / top
    for part in range(2):
        code = jnp.round(parts[part] * factor).astype(jnp.int32)
        out_ref[place, part] = code.astype(jnp.int16)
    scale_ref[pl.ds(scale_row, 1), :] = top * (1.0 / TOP)


def upper_loop(plan, index, begin, low, high, reqs, in_ref, w_ref, out_ref, scale_ref):
    offset = reqs[4, index] - reqs[2, index] - begin

    @pl.loop(low, high)
    def _(hop):
        parts = [partial_sum(plan, True, hop, w_ref, in_ref, part) for part in range(2)]
        encode(parts, out_ref, scale_ref, offset + hop, offset + hop)


def first_kernel(plan, meta, reqs, in_ref, w_ref, out_ref, scale_ref):
    index = pl.program_id(0)

    @pl.when((index < meta[3]) & (meta[2] >= plan.half))
    def _():
        first, last = reqs[2, index], reqs[3, index]
        split = jnp.clip(first + plan.first - reqs[4, index], first, last)
        upper_loop(plan, index, 0, first, split, reqs, in_ref, w_ref, out_ref, scale_ref)


def add_lower(plan, hop, unit, in_ref, w_ref, got_ref, got_scale, out_ref, scale_ref, place, line):
    scale = got_scale[pl.ds(unit, 1), :]
    parts = []
    for part in range(2):
        other = got_ref[unit, part].astype(jnp.int32).astype(jnp.float32) * scale
        parts.append(partial_sum(plan, False, hop, w_ref, in_ref, part) + other)
    encode(parts, out_ref, scale_ref, place, line)


def middle_kernel(
    plan, meta, reqs, pos, in_ref, w_ref, got_ref, got_scale, out_ref, scale_ref, sum_ref, sum_scale
):
    index = pl.program_id(0)
    first, last, offset = reqs[2, index], reqs[3, index], reqs[4, index]
    split = jnp.clip(first + plan.first - offset, first, last)

    @pl.when((index < meta[1]) & (meta[2] >= plan.half))
    def _():
        upper_loop(plan, index, plan.first, split, last, reqs, in_ref, w_ref, out_ref, scale_ref)

    @pl.when((index < meta[3]) & (meta[2] < plan.half))
    def _():
        @pl.loop(first, split)
        def _(hop):
            place = pos[index * plan.frames + hop]

            @pl.when(place >= 0)
            def _():
                line = place + lax.div(place, plan.soon) * (plan.soon_rows - plan.soon)
                unit = offset + hop - first
                add_lower(
                    plan, hop, unit, in_ref, w_ref, got_ref, got_scale, sum_ref, sum_scale, place, line
                )


def lower_kernel(
    plan, meta, reqs, pos, in_ref, w_ref, got_0, scale_0, got_1, scale_1, out_ref, scale_ref
):
    index = pl.program_id(0)

    @pl.when((index < meta[1]) & (meta[2] < plan.half))
    def _():
        first, last, offset = reqs[2, index], reqs[3, index], reqs[4, index]
        split = jnp.clip(first + plan.first - offset, first, last)

        def add(got_ref, got_scale, begin, hop):
            place = -1 - pos[index * plan.frames + hop]

            @pl.when(place >= 0)
            def _():
                unit = offset + hop - first - begin
                add_lower(
                    plan, hop, unit, in_ref, w_ref, got_ref, got_scale, out_ref, scale_ref, place, place
                )

        @pl.loop(first, split)
        def _(hop):
            add(got_0, scale_0, 0, hop)

        @pl.loop(split, last)
        def _(hop):
            add(got_1, scale_1, plan.first, hop)


def filter_specs(plan, low, high):
    def request(i, m):
        bottom = m[low] if low else 0
        return jnp.maximum(jnp.clip(i, bottom, m[high] - 1), 0)

    taps = plan.frames - 1 + plan.all_hops
    return [
        pl.BlockSpec(
            (plan.half, 1, 1, plan.hops, 2, plan.span, BLOCKW),
            lambda i, m, r, *_: (0, r[0, request(i, m)], r[1, request(i, m)], 0, 0, 0, 0),
        ),
        pl.BlockSpec((taps, plan.span, BLOCKW), lambda i, *_: (0, 0, 0)),
    ]


def whole(*dims):
    return pl.BlockSpec(dims, lambda i, *_: (0,) * len(dims))


def coded(units, plan, rows=None):
    return (
        jax.ShapeDtypeStruct((units, 2, plan.span, BLOCKW), jnp.int16),
        jax.ShapeDtypeStruct((rows or units, BLOCKW), jnp.float32),
    )


def wholes(values):
    return [whole(*value.shape) for value in values]


def filter_first(plan, spreaded, weights, meta, reqs):
    outs = coded(plan.first, plan)
    return pl.pallas_call(
        functools.partial(first_kernel, plan),
        out_shape=outs,
        grid_spec=pltpu.PrefetchScalarGridSpec(
            num_scalar_prefetch=2,
            grid=(plan.owners * MAXREQ,),
            in_specs=filter_specs(plan, 0, 3),
            out_specs=tuple(wholes(outs)),
        ),
    )(meta, reqs, spreaded, weights)


def filter_middle(plan, spreaded, weights, got, meta, reqs, pos):
    lines = plan.keepers * plan.owners
    outs = coded(plan.rest, plan) + coded(lines * plan.soon, plan, lines * plan.soon_rows)
    return pl.pallas_call(
        functools.partial(middle_kernel, plan),
        out_shape=outs,
        grid_spec=pltpu.PrefetchScalarGridSpec(
            num_scalar_prefetch=3,
            grid=(plan.owners * MAXREQ,),
            in_specs=filter_specs(plan, 4, 5) + wholes(got),
            out_specs=tuple(wholes(outs)),
        ),
    )(meta, reqs, pos, spreaded, weights, *got)


def filter_lower(plan, spreaded, weights, got, meta, reqs, pos):
    rows = plan.keepers * plan.owners * plan.deep
    return pl.pallas_call(
        functools.partial(lower_kernel, plan),
        out_shape=(
            jax.ShapeDtypeStruct((rows, 2, plan.span, BLOCKW), jnp.int16),
            jax.ShapeDtypeStruct((rows, BLOCKW), jnp.float32),
        ),
        grid_spec=pltpu.PrefetchScalarGridSpec(
            num_scalar_prefetch=3,
            grid=(plan.owners * MAXREQ,),
            in_specs=filter_specs(plan, 0, 1) + [whole(*value.shape) for value in got],
            out_specs=(whole(rows, 2, plan.span, BLOCKW), whole(rows, BLOCKW)),
        ),
    )(meta, reqs, pos, spreaded, weights, *got)


def deliver_kernel(plan, begin, count, lifted, *refs):
    if lifted:
        src, src_scale, code, code_scale, dst, dst_scale, got, got_scale = refs[:8]
        tmp, tmp_scale, send, recv, local, up, down = refs[8:]
    else:
        src, src_scale, _, dst, dst_scale, tmp, tmp_scale, send, recv, local = refs
    row, col = lax.axis_index("tm"), lax.axis_index("chan")
    size, lines = plan.slices, plan.keepers * plan.owners
    me = row * plan.owners + col
    upper = row >= plan.half
    other = jnp.where(upper, row - plan.half, row + plan.half)
    barrier = pltpu.get_barrier_semaphore()
    pieces = [(first, min(3, count - first)) for first in range(0, count, 3)]

    def device(index):
        return {"tm": lax.div(index, plan.owners), "chan": lax.rem(index, plan.owners)}

    def mask_of(step):
        return lax.rem(step * 7, size)

    def value(index, mask, source, target):
        first, extent = pieces[index]
        return pltpu.make_async_remote_copy(
            src_ref=src.at[target, pl.ds(first, extent)],
            dst_ref=dst.at[source, pl.ds(begin + first, extent)],
            send_sem=send.at[index, mask],
            recv_sem=recv.at[index, mask],
            device_id=device(me ^ mask),
        )

    def scale(mask, source, target):
        return pltpu.make_async_remote_copy(
            src_ref=src_scale.at[target],
            dst_ref=dst_scale.at[source],
            send_sem=send.at[len(pieces), mask],
            recv_sem=recv.at[len(pieces), mask],
            device_id=device(me ^ mask),
        )

    lifts = []
    if lifted:
        extent = lifted
        lifts = [
            pltpu.make_async_remote_copy(
                src_ref=source.at[pl.ds(0, extent)],
                dst_ref=target.at[pl.ds(0, extent)],
                send_sem=up.at[index],
                recv_sem=down.at[index],
                device_id={"tm": other},
            )
            for index, (source, target) in enumerate([(code, got), (code_scale, got_scale)])
        ]
        pl.semaphore_signal(barrier, inc=1, device_id={"tm": other})

        @pl.when(upper)
        def _():
            pl.semaphore_wait(barrier, 1)
            for copy in lifts:
                copy.start()
            for copy in lifts:
                copy.wait_send()

    @pl.when(jnp.logical_not(upper))
    def _():
        @pl.loop(1, size)
        def _(step):
            pl.semaphore_signal(barrier, inc=1, device_id=device(me ^ mask_of(step)))

        pl.semaphore_wait(barrier, size - 1 + int(bool(lifted)))

        @pl.loop(1, size)
        def _(step):
            mask = mask_of(step)

            @pl.when((me ^ mask) < lines)
            def _():
                scale(mask, me, me ^ mask).start()

        for index in range(len(pieces)):

            @pl.loop(1, size)
            def _(step):
                mask = mask_of(step)

                @pl.when((me ^ mask) < lines)
                def _():
                    value(index, mask, me, me ^ mask).start()

        @pl.when(me < lines)
        def _():
            moves = [
                (src.at[me, pl.ds(0, count)], tmp, dst.at[me, pl.ds(begin, count)]),
                (src_scale.at[me], tmp_scale, dst_scale.at[me]),
            ]
            for index, (source, middle, target) in enumerate(moves):
                read = pltpu.make_async_copy(source, middle, local.at[2 * index])
                read.start()
                read.wait()
                write = pltpu.make_async_copy(middle, target, local.at[2 * index + 1])
                write.start()
                write.wait()

            @pl.loop(1, size)
            def _(step):
                mask = mask_of(step)
                scale(mask, me ^ mask, me).wait_recv()
                for index in range(len(pieces)):
                    value(index, mask, me ^ mask, me).wait_recv()

        @pl.loop(1, size)
        def _(step):
            mask = mask_of(step)

            @pl.when((me ^ mask) < lines)
            def _():
                scale(mask, me, me ^ mask).wait_send()
                for index in range(len(pieces)):
                    value(index, mask, me, me ^ mask).wait_send()

        for copy in lifts:
            copy.wait_recv()


def deliver(plan, begin, count, lifted, collective, values, scales, *more):
    sem = pltpu.SemaphoreType.DMA
    inner = values.shape[2:]
    pieces = -(-count // 3)
    outs = (
        jax.ShapeDtypeStruct((plan.slices, plan.soon + plan.deep) + inner, values.dtype),
        jax.ShapeDtypeStruct((plan.slices,) + scales.shape[1:], scales.dtype),
    )
    scratch = [
        pltpu.VMEM((count,) + inner, values.dtype),
        pltpu.VMEM(scales.shape[1:], scales.dtype),
        sem((pieces + 1, plan.slices)),
        sem((pieces + 1, plan.slices)),
        sem((4,)),
    ]
    if lifted:
        outs += tuple(jax.ShapeDtypeStruct(value.shape, value.dtype) for value in more)
        scratch += [sem((2,)), sem((2,))]
    return pl.pallas_call(
        functools.partial(deliver_kernel, plan, begin, count, lifted),
        out_shape=outs,
        in_specs=[ANY] * (2 + len(more)),
        out_specs=(ANY,) * len(outs),
        scratch_shapes=scratch,
        input_output_aliases={} if lifted else {2: 0},
        compiler_params=pltpu.CompilerParams(collective_id=collective, has_side_effects=True),
    )(values, scales, *more)


def transform_kernel(plan, omap, in_ref, soon_ref, late_ref, table_ref, turn_ref, out_ref, ys, zs):
    entry = omap[pl.program_id(0)]

    @pl.when(entry < 0)
    def _():
        out_ref[...] = jnp.zeros_like(out_ref)

    @pl.when(entry >= 0)
    def _():
        chunk = 32

        def load(part, first):
            piece, line = divmod(first, plan.span)
            code = in_ref[piece, 0, part, line : line + chunk, :]
            scale = jnp.where(
                entry < plan.soon,
                soon_ref[piece, pl.ds(jnp.minimum(entry, plan.soon - 1), 1), :],
                late_ref[piece, pl.ds(jnp.maximum(entry - plan.soon, 0), 1), :],
            )
            return code.astype(jnp.int32).astype(jnp.float32) * scale

        for line in range(0, SUB, chunk):
            re = [load(0, SUB * a + line) for a in range(RADIX)]
            im = [load(1, SUB * a + line) for a in range(RADIX)]
            es, ed = re[0] + re[2], re[0] - re[2]
            fs, fd = im[0] + im[2], im[0] - im[2]
            gs, gd = re[1] + re[3], re[1] - re[3]
            hs, hd = im[1] + im[3], im[1] - im[3]
            mixed = [
                (es + gs, fs + hs),
                (ed + hd, fd - gd),
                (es - gs, fs - hs),
                (ed - hd, fd + gd),
            ]
            rows = slice(line, line + chunk)
            for q in range(RADIX):
                real, imag = mixed[q]
                if q:
                    cosine, sine = turn_ref[0, q - 1, rows, :], turn_ref[1, q - 1, rows, :]
                    real, imag = real * cosine + imag * sine, imag * cosine - real * sine
                for part, value in enumerate((real, imag)):
                    cols = slice(part * BLOCKW, (part + 1) * BLOCKW)
                    high = value.astype(jnp.bfloat16)
                    ys[q, rows, cols] = high
                    ys[q, SUB + line : SUB + line + chunk, cols] = (
                        value - high.astype(jnp.float32)
                    ).astype(jnp.bfloat16)
                    ys[q, 2 * SUB + line : 2 * SUB + line + chunk, cols] = high

        for q in range(RADIX):
            both = jnp.dot(table_ref[...], ys[q], preferred_element_type=jnp.float32)
            rows = pl.ds(q, SUB, stride=RADIX)
            zs[0, rows, :] = both[:SUB, :BLOCKW] + both[SUB:, BLOCKW:]
            zs[1, rows, :] = both[:SUB, BLOCKW:] - both[SUB:, :BLOCKW]

        out_ref[0, 0] = zs[...].astype(out_ref.dtype)


def transform_tables():
    line = np.arange(SUB)
    angles = (line[:, None] * line[None, :] % SUB) * (2.0 * np.pi / SUB)
    table = np.concatenate([np.cos(angles), np.sin(angles)], axis=0) / math.sqrt(NFINE)
    table = table.astype(np.float32)
    high = table.astype(jnp.bfloat16)
    low = (table - high.astype(np.float32)).astype(jnp.bfloat16)
    turns = np.arange(1, RADIX)[:, None] * line[None, :] * (2.0 * np.pi / NFINE)
    turn = np.stack([np.cos(turns), np.sin(turns)]).astype(np.float32)
    return np.concatenate([high, high, low], axis=1), turn


def transform(plan, values, soon, late, omap):
    table, turn = transform_tables()
    turn = jnp.asarray(np.ascontiguousarray(np.broadcast_to(turn[..., None], turn.shape + (BLOCKW,))))
    return pl.pallas_call(
        functools.partial(transform_kernel, plan),
        out_shape=jax.ShapeDtypeStruct((plan.hops, MAXREQ, 2, NFINE, BLOCKW), jnp.bfloat16),
        grid_spec=pltpu.PrefetchScalarGridSpec(
            num_scalar_prefetch=1,
            grid=(plan.hops * MAXREQ,),
            in_specs=[
                pl.BlockSpec(
                    (plan.slices, 1, 2, plan.span, BLOCKW),
                    lambda i, o: (0, jnp.maximum(o[i], 0), 0, 0, 0),
                ),
                whole(*soon.shape),
                whole(*late.shape),
                whole(2 * SUB, 3 * SUB),
                whole(2, RADIX - 1, SUB, BLOCKW),
            ],
            out_specs=pl.BlockSpec(
                (1, 1, 2, NFINE, BLOCKW), lambda i, o: (i // MAXREQ, i % MAXREQ, 0, 0, 0)
            ),
            scratch_shapes=[
                pltpu.VMEM((RADIX, 3 * SUB, 2 * BLOCKW), jnp.bfloat16),
                pltpu.VMEM((2, NFINE, BLOCKW), jnp.float32),
            ],
        ),
    )(omap, values, soon, late, jnp.asarray(table), turn)


def owners_power(value):
    return value & (value - 1) == 0


class Plan:
    def __init__(self, size, owners, hops, per_column):
        self.size, self.owners, self.hops, self.per_column = size, owners, hops, per_column
        self.all_hops = hops * size
        self.frames = self.all_hops - TAPS + 1
        self.keepers = -(-self.frames // hops)
        self.half = size // 2
        self.slices = self.half * owners
        self.span = NFINE // self.slices
        self.fill = owners * PAIR
        self.deep = round_up(hops * MAXREQ, 8)
        self.lead = min(2, self.fill)
        self.first = 40
        self.rest = round_up(owners * MAXREQ * self.frames, 8)
        more = self.fill - self.lead
        self.fills = sorted({max(1, round_up(more * i, 6) // 6) for i in (1, 2, 3, 4, 6)})
        near = {min(8 * i, self.rest) for i in (1, 2, 3, 4, 5, 7, 9)}
        self.counts = sorted(near | {self.rest})
        most = hops * MAXREQ
        self.soon = min(4, most)
        self.soon_rows = round_up(self.soon, 8)
        self.depths = sorted({round_up(most * i, 12) // 12 for i in (2, 3, 4, 5, 6, 7, 8, 10, 12)})

        spread = sorted(range(2, self.slices), key=lambda mask: bin(mask >> 1).count("1"))
        self.masks = spread + [1]

    def fits(self):
        powers = self.slices & (self.slices - 1) == 0 and owners_power(self.owners)
        even = powers and self.size % 2 == 0 and NFINE % self.slices == 0 and self.span % 32 == 0
        return even and self.keepers <= self.half


def shards(coarse, prototype, req_block, req_start, req_frames, req_count):
    owners, size = lax.axis_size("chan"), lax.axis_size("tm")
    plan = Plan(size, owners, coarse.shape[1] // NFINE, coarse.shape[2] // BLOCKW)
    if not plan.fits():
        return shards_general(coarse, prototype, req_block, req_start, req_frames, req_count)
    tables = make_tables(plan, req_block, req_start, req_frames, req_count)
    meta, chosen, reqs, pos, omap, pick_a, pick_b, pick_c = tables
    packed = gather(plan, coarse, meta, chosen)

    me = lax.axis_index("tm") % plan.half * owners + lax.axis_index("chan")
    mine = lax.dynamic_slice(prototype, (0, me * plan.span), (TAPS, plan.span))
    mine = jnp.pad(mine, ((plan.frames - 1, plan.all_hops - TAPS), (0, 0)))
    weights = jnp.broadcast_to(mine[:, :, None], mine.shape + (BLOCKW,))

    def split(value):
        return value.reshape((plan.half, owners) + value.shape[1:])

    spreaded = spread(plan, packed, 0, plan.lead, 0)[0]
    early = filter_first(plan, split(spreaded), weights, meta, reqs)

    def second(count, collective, *operands):
        return spread(plan, operands[0], plan.lead, count, collective, *operands[1:])

    branches = [functools.partial(second, size, 1 + i) for i, size in enumerate(plan.fills)]
    spreaded, *got = lax.switch(pick_a[0], branches, packed, spreaded, *early)
    spreaded = split(spreaded)
    middle = filter_middle(plan, spreaded, weights, got, meta, reqs, pos)
    lines = plan.keepers * owners

    def by_line(value):
        return value.reshape((lines, value.shape[0] // lines) + value.shape[1:])

    sums = [by_line(value) for value in middle[2:]]
    base = 1 + len(branches)

    def third(extent, collective, *operands):
        return deliver(plan, 0, plan.soon, extent, collective, *operands)

    branches = [functools.partial(third, size, base + i) for i, size in enumerate(plan.counts)]
    values, soon, *more = lax.switch(pick_b[0], branches, *sums, *middle[:2])
    sums = filter_lower(plan, spreaded, weights, list(got) + more, meta, reqs, pos)
    sums = [by_line(value) for value in sums]
    base += len(branches)

    def fourth(count, collective, *operands):
        return deliver(plan, plan.soon, count, 0, collective, *operands)

    branches = [functools.partial(fourth, size, base + i) for i, size in enumerate(plan.depths)]
    values, late = lax.switch(pick_c[0], branches, *sums, values)
    return transform(plan, values, soon, late, omap)[:, None]


def solution(mesh):
    return jax.shard_map(
        shards,
        mesh=mesh,
        in_specs=(P(None, "tm", "chan"), P(), P(), P(), P(), P()),
        out_specs=P("tm", "chan", None, None, None, None),
        check_vma=False,
    )
```

```python
import functools
import math

import jax
import jax.numpy as jnp
import numpy as np
from jax import lax
from jax.experimental import pallas as pl
from jax.experimental.pallas import tpu as pltpu
from jax.sharding import PartitionSpec as P

BLOCKW = 128
NFINE = 1024
TAPS = 16
MAXREQ = 4
PAIR = 2
ROWS = 128
STEP = 16
ANY = pl.BlockSpec(memory_space=pl.ANY)


def build_table():
    line = jnp.arange(NFINE, dtype=jnp.int32)
    products = line[:, None] * line[None, :] % NFINE
    angles = products.astype(jnp.float32) * (2.0 * math.pi / NFINE)
    scale = 1.0 / math.sqrt(NFINE)
    return jnp.concatenate([jnp.cos(angles) * scale, jnp.sin(angles) * scale], axis=0)


def pack_kernel(chosen, coarse_ref, out_ref):
    out_ref[...] = coarse_ref[...].reshape(out_ref.shape)


def pack(coarse, chosen, first, hops):
    count = chosen.shape[0]
    return pl.pallas_call(
        pack_kernel,
        out_shape=jax.ShapeDtypeStruct((count, 2, hops * NFINE, BLOCKW), coarse.dtype),
        grid_spec=pltpu.PrefetchScalarGridSpec(
            num_scalar_prefetch=1,
            grid=(count,),
            in_specs=[pl.BlockSpec((2, hops * NFINE, BLOCKW), lambda i, c: (0, first, c[i]))],
            out_specs=pl.BlockSpec((1, 2, hops * NFINE, BLOCKW), lambda i, c: (i, 0, 0, 0)),
        ),
        cost_estimate=pl.CostEstimate(
            flops=0, transcendentals=0, bytes_accessed=count * 8 * hops * NFINE * BLOCKW
        ),
    )(chosen, coarse)


def select_kernel(pieces, arrival, in_ref, out_ref):
    share = BLOCKW // pieces
    for piece in range(pieces):
        cols = slice(piece * share, (piece + 1) * share)
        out_ref[piece] = jnp.concatenate([in_ref[0, 0, :, cols], in_ref[0, 1, :, cols]], axis=-1)


def select(incoming, arrival, pieces, hops):
    width = 2 * BLOCKW // pieces
    rows = hops * NFINE
    return pl.pallas_call(
        functools.partial(select_kernel, pieces),
        out_shape=jax.ShapeDtypeStruct((MAXREQ * pieces, rows, width), incoming.dtype),
        grid_spec=pltpu.PrefetchScalarGridSpec(
            num_scalar_prefetch=1,
            grid=(MAXREQ, hops),
            in_specs=[pl.BlockSpec((1, 2, NFINE, BLOCKW), lambda q, h, a: (a[q], 0, h, 0))],
            out_specs=pl.BlockSpec((pieces, NFINE, width), lambda q, h, a: (q, h, 0)),
        ),
        cost_estimate=pl.CostEstimate(
            flops=0, transcendentals=0, bytes_accessed=MAXREQ * 8 * rows * BLOCKW
        ),
    )(arrival, incoming)


def exchange_kernel(
    owners, size, a_in, b_in, a_out, b_out, a_tmp, b_tmp, a_send, a_recv, b_send, b_recv, local
):
    column, row = lax.axis_index("chan"), lax.axis_index("tm")
    barrier = pltpu.get_barrier_semaphore()

    @pl.loop(1, owners)
    def _(step):
        other = lax.rem(column + step, owners)
        pl.semaphore_signal(barrier, inc=1, device_id={"chan": other})

    @pl.loop(1, size)
    def _(step):
        other = lax.rem(row + step, size)
        pl.semaphore_signal(barrier, inc=1, device_id={"tm": other})

    pl.semaphore_wait(barrier, owners + size - 2)

    def a_copy(step, source, target, device):
        return pltpu.make_async_remote_copy(
            src_ref=a_in.at[pl.ds(target * PAIR, PAIR)],
            dst_ref=a_out.at[pl.ds(source * PAIR, PAIR)],
            send_sem=a_send.at[step],
            recv_sem=a_recv.at[step],
            device_id={"chan": device},
        )

    def b_copy(step, source, target, device):
        return pltpu.make_async_remote_copy(
            src_ref=b_in.at[target],
            dst_ref=b_out.at[source],
            send_sem=b_send.at[step],
            recv_sem=b_recv.at[step],
            device_id={"tm": device},
        )

    @pl.loop(1, size)
    def _(step):
        target = lax.rem(row + step, size)
        b_copy(step, row, target, target).start()

    @pl.loop(1, owners)
    def _(step):
        target = lax.rem(column + step, owners)
        a_copy(step, column, target, target).start()

    a_read = pltpu.make_async_copy(a_in.at[pl.ds(column * PAIR, PAIR)], a_tmp, local.at[0])
    b_read = pltpu.make_async_copy(b_in.at[row], b_tmp, local.at[1])
    a_read.start()
    b_read.start()
    a_read.wait()
    b_read.wait()
    a_write = pltpu.make_async_copy(a_tmp, a_out.at[pl.ds(column * PAIR, PAIR)], local.at[2])
    b_write = pltpu.make_async_copy(b_tmp, b_out.at[row], local.at[3])
    a_write.start()
    b_write.start()
    a_write.wait()
    b_write.wait()

    @pl.loop(1, owners)
    def _(step):
        source = lax.rem(column + owners - step, owners)
        copy = a_copy(step, source, column, source)
        copy.wait_recv()
        copy.wait_send()

    @pl.loop(1, size)
    def _(step):
        source = lax.rem(row + size - step, size)
        copy = b_copy(step, source, row, source)
        copy.wait_recv()
        copy.wait_send()


def exchange(outgoing, sending, owners, size, collective):
    sem = pltpu.SemaphoreType.DMA
    return pl.pallas_call(
        functools.partial(exchange_kernel, owners, size),
        out_shape=(
            jax.ShapeDtypeStruct(outgoing.shape, outgoing.dtype),
            jax.ShapeDtypeStruct(sending.shape, sending.dtype),
        ),
        in_specs=[ANY, ANY],
        out_specs=(ANY, ANY),
        scratch_shapes=[
            pltpu.VMEM((PAIR,) + outgoing.shape[1:], outgoing.dtype),
            pltpu.VMEM(sending.shape[1:], sending.dtype),
            sem((owners,)),
            sem((owners,)),
            sem((size,)),
            sem((size,)),
            sem((4,)),
        ],
        compiler_params=pltpu.CompilerParams(collective_id=collective, has_side_effects=True),
    )(outgoing, sending)


def filter_kernel(hops, frames, weights_ref, *refs):
    out_ref = refs[-1]
    width = refs[0].shape[-1]

    @pl.loop(0, ROWS // STEP)
    def _(step):
        rows = pl.ds(pl.multiple_of(step * STEP, STEP), STEP)
        weights = [
            jnp.broadcast_to(weights_ref[rows, tap : tap + 1], (STEP, width)) for tap in range(TAPS)
        ]
        for frame in range(frames):
            total = None
            for tap in range(TAPS):
                hop = frame + tap
                term = weights[tap] * refs[hop % hops][hop // hops, rows, :].astype(jnp.float32)
                total = term if total is None else total + term
            out_ref[rows, frame * width : (frame + 1) * width] = total


def polyphase(parts, prototype, frames):
    hops = len(parts)
    size, _, width = parts[0].shape
    return pl.pallas_call(
        functools.partial(filter_kernel, hops, frames),
        out_shape=jax.ShapeDtypeStruct((NFINE, frames * width), jnp.float32),
        grid=(NFINE // ROWS,),
        in_specs=[pl.BlockSpec((ROWS, TAPS), lambda i: (i, 0))]
        + [pl.BlockSpec((size, ROWS, width), lambda i: (0, i, 0))] * hops,
        out_specs=pl.BlockSpec((ROWS, frames * width), lambda i: (i, 0)),
    )(prototype.T, *parts)


def combine_kernel(frames, share, both_ref, out_ref):
    frame = pl.program_id(0)

    @pl.when(frame < frames)
    def _():
        sine = both_ref[1]
        turned = jnp.concatenate([sine[:, share:], -sine[:, :share]], axis=-1)
        out_ref[0] = (both_ref[0] + turned).astype(out_ref.dtype)

    @pl.when(frame >= frames)
    def _():
        out_ref[...] = jnp.zeros_like(out_ref)


def combine(both, frames, padded, width):
    return pl.pallas_call(
        functools.partial(combine_kernel, frames, width // 2),
        out_shape=jax.ShapeDtypeStruct((padded, NFINE, width), jnp.bfloat16),
        grid=(padded,),
        in_specs=[
            pl.BlockSpec((2, NFINE, width), lambda f: (0, 0, jnp.minimum(f, frames - 1))),
        ],
        out_specs=pl.BlockSpec((1, NFINE, width), lambda f: (f, 0, 0)),
    )(both)


def return_kernel(size, keepers, hops, res_ref, out_ref, send_sems, recv_sems):
    me = lax.axis_index("tm")
    barrier = pltpu.get_barrier_semaphore()

    @pl.loop(1, size)
    def _(step):
        other = lax.rem(me + step, size)
        pl.semaphore_signal(barrier, inc=1, device_id={"tm": other})

    pl.semaphore_wait(barrier, size - 1)

    def copy(step):
        target = lax.rem(me + step, size)
        return pltpu.make_async_remote_copy(
            src_ref=res_ref.at[pl.ds(target * hops, hops)],
            dst_ref=out_ref.at[me],
            send_sem=send_sems.at[step],
            recv_sem=recv_sems.at[step],
            device_id={"tm": target},
        )

    def arriving(step):
        source = lax.rem(me + size - step, size)
        return pltpu.make_async_remote_copy(
            src_ref=res_ref.at[pl.ds(0, hops)],
            dst_ref=out_ref.at[source],
            send_sem=send_sems.at[step],
            recv_sem=recv_sems.at[step],
            device_id={"tm": source},
        )

    @pl.loop(1, size)
    def _(step):
        @pl.when(lax.rem(me + step, size) < keepers)
        def _():
            copy(step).start()

    @pl.when(me < keepers)
    def _():
        @pl.loop(1, size)
        def _(step):
            arriving(step).wait_recv()

    @pl.loop(1, size)
    def _(step):
        @pl.when(lax.rem(me + step, size) < keepers)
        def _():
            copy(step).wait_send()


def give_back(result, size, keepers, hops):
    shape = (size, hops) + result.shape[1:]
    return pl.pallas_call(
        functools.partial(return_kernel, size, keepers, hops),
        out_shape=jax.ShapeDtypeStruct(shape, result.dtype),
        in_specs=[ANY],
        out_specs=ANY,
        scratch_shapes=[pltpu.SemaphoreType.DMA((size,)), pltpu.SemaphoreType.DMA((size,))],
        compiler_params=pltpu.CompilerParams(collective_id=0, has_side_effects=True),
    )(result)


def final_kernel(pieces, meta, got_ref, own_ref, out_ref):
    share = BLOCKW // pieces
    slot, hop = pl.program_id(0), pl.program_id(1)
    row = meta[0]
    active = meta[2 + slot * pl.num_programs(1) + hop] > 0

    @pl.when(jnp.logical_not(active))
    def _():
        out_ref[...] = jnp.zeros_like(out_ref)

    @pl.when(active)
    def _():
        data = [
            jnp.where(slot * pieces + piece == row, own_ref[0], got_ref[piece, 0])
            for piece in range(pieces)
        ]
        for part in range(2):
            cols = slice(part * share, (part + 1) * share)
            out_ref[0, 0, part] = jnp.concatenate([d[:, cols] for d in data], axis=-1)


def assemble(got, result, active, row, keepers, pieces):
    size, hops, _, width = got.shape
    base = jnp.minimum(row, keepers - 1) * hops
    meta = jnp.concatenate(
        [jnp.stack([row, base]).astype(jnp.int32), active.astype(jnp.int32).reshape(-1)]
    )
    return pl.pallas_call(
        functools.partial(final_kernel, pieces),
        out_shape=jax.ShapeDtypeStruct((hops, MAXREQ, 2, NFINE, BLOCKW), got.dtype),
        grid_spec=pltpu.PrefetchScalarGridSpec(
            num_scalar_prefetch=1,
            grid=(MAXREQ, hops),
            in_specs=[
                pl.BlockSpec((pieces, 1, NFINE, width), lambda q, h, m: (q, h, 0, 0)),
                pl.BlockSpec((1, NFINE, width), lambda q, h, m: (m[1] + h, 0, 0)),
            ],
            out_specs=pl.BlockSpec((1, 1, 2, NFINE, BLOCKW), lambda q, h, m: (h, q, 0, 0, 0)),
        ),
    )(meta, got, result)


def shards_general(coarse, prototype, req_block, req_start, req_frames, req_count):
    owners = lax.axis_size("chan")
    column = lax.axis_index("chan")
    row = lax.axis_index("tm")
    size = lax.axis_size("tm")
    per_column = coarse.shape[2] // BLOCKW
    hops = coarse.shape[1] // NFINE
    all_hops = hops * size
    frames = all_hops - TAPS + 1
    keepers = -(-frames // hops)
    pieces = size // MAXREQ
    width = 2 * BLOCKW // pieces
    share = BLOCKW // pieces

    slot_ids = jnp.arange(MAXREQ, dtype=jnp.int32)
    live = slot_ids[None, :] < req_count[:, None]
    sources = req_block // per_column
    same = (
        live[:, :, None]
        & live[:, None, :]
        & (sources[:, :, None] == sources[:, None, :])
        & (slot_ids[None, None, :] < slot_ids[None, :, None])
    )
    rank = jnp.sum(same.astype(jnp.int32), axis=2)
    picked = (
        (live & (sources == column))[:, None, :]
        & (rank[:, None, :] == jnp.arange(PAIR, dtype=jnp.int32)[None, :, None])
    )
    local = req_block - column * per_column
    chosen = jnp.sum(jnp.where(picked, local[:, None, :], 0), axis=2).reshape(-1)
    chosen = jnp.clip(chosen, 0, per_column - 1).astype(jnp.int32)
    mine = (jnp.arange(owners, dtype=jnp.int32) == column)[:, None]

    def own(table):
        return jnp.sum(jnp.where(mine, table, 0), axis=0)

    my_live = slot_ids < own(req_count[:, None])[0]
    arrival = jnp.where(my_live, own(sources) * PAIR + own(rank), 0)
    arrival = jnp.clip(arrival, 0, owners * PAIR - 1).astype(jnp.int32)
    my_start, my_frames = own(req_start), own(req_frames)
    hop_ids = row * hops + jnp.arange(hops, dtype=jnp.int32)
    active = (
        my_live[:, None]
        & (hop_ids[None, :] >= my_start[:, None])
        & (hop_ids[None, :] < (my_start + my_frames)[:, None])
    )

    table = build_table()
    outgoing = [pack(coarse, chosen, hop, 1) for hop in range(hops)]
    incoming = lax.all_to_all(outgoing[0], "chan", split_axis=0, concat_axis=0, tiled=True)
    parts = []
    for hop in range(1, hops):
        sending = select(incoming, arrival, pieces, 1)
        incoming, gathered = exchange(outgoing[hop], sending, owners, size, hop)
        parts.append(gathered)
    sending = select(incoming, arrival, pieces, 1)
    parts.append(lax.all_to_all(sending, "tm", split_axis=0, concat_axis=0, tiled=True))
    flat = polyphase(parts, prototype, frames)
    both = jnp.dot(table, flat, precision=lax.Precision.HIGH, preferred_element_type=jnp.float32)
    padded = keepers * hops
    if width % 128 == 0:
        result = combine(both.reshape(2, NFINE, frames * width), frames, padded, width)
    else:
        both = both.reshape(2, NFINE, frames, 2, share)
        cosine, sine = both[0], both[1]
        result = jnp.stack(
            [cosine[:, :, 0] + sine[:, :, 1], cosine[:, :, 1] - sine[:, :, 0]], axis=2
        ).astype(jnp.bfloat16)
        result = result.reshape(NFINE, frames, width).transpose(1, 0, 2)
        if padded > frames:
            zeros = jnp.zeros((padded - frames, NFINE, width), result.dtype)
            result = jnp.concatenate([result, zeros], axis=0)
    got = give_back(result, size, keepers, hops)
    return assemble(got, result, active, row, keepers, pieces)[:, None]


SMEM = pl.BlockSpec(memory_space=pltpu.SMEM)
TOP = 32767.0
RADIX = 4
SUB = NFINE // RADIX


def round_up(value, unit):
    return -(-value // unit) * unit


def picked(value, sizes):
    return sum((value > size).astype(jnp.int32) for size in sizes[:-1])


def tables_kernel(
    plan, blk, start, nfr, cnt, meta, chosen, reqs, pos, omap, pick_a, pick_b, pick_c,
    columns, lists, early_lists, order, places, buckets
):
    row, col = lax.axis_index("tm"), lax.axis_index("chan")
    total = plan.owners * MAXREQ
    for i in range(plan.owners):
        columns[i] = 0
    for i in range(plan.keepers * plan.owners):
        lists[i] = 0
        early_lists[i] = 0
    for i in range(plan.hops * MAXREQ):
        omap[i] = -1
    for i in range(plan.fill):
        chosen[i] = 0

    for i in range(plan.frames + 1):
        buckets[i] = 0

    def fresh(item):
        owner, slot = lax.div(item, MAXREQ), lax.rem(item, MAXREQ)
        return slot < cnt[owner], nfr[owner, slot]

    @pl.loop(0, total)
    def _(item):
        alive, size = fresh(item)

        @pl.when(alive)
        def _():
            buckets[size] = buckets[size] + 1

    live = jnp.int32(0)
    for size in range(plan.frames, 0, -1):
        amount = buckets[size]
        buckets[size] = live
        live = live + amount

    @pl.loop(0, total)
    def _(item):
        alive, size = fresh(item)

        @pl.when(alive)
        def _():
            spot = buckets[size]
            buckets[size] = spot + 1
            order[spot] = item

    @pl.loop(0, live)
    def _(index):
        item = order[index]
        block = blk[lax.div(item, MAXREQ), lax.rem(item, MAXREQ)]
        source = lax.div(block, plan.per_column)
        place = columns[source]
        columns[source] = place + 1
        places[index] = place

        @pl.when(source == col)
        def _():
            chosen[place] = block - source * plan.per_column

    def request(index, carry, early):
        item = order[index]
        owner, slot = lax.div(item, MAXREQ), lax.rem(item, MAXREQ)

        def add(carry):
            count, units = carry
            first = start[owner, slot]
            last = first + nfr[owner, slot]
            reqs[0, count] = lax.div(blk[owner, slot], plan.per_column)
            reqs[1, count] = places[index]
            reqs[2, count] = first
            reqs[3, count] = last
            reqs[4, count] = units

            def frame(hop, carry):
                keeper = lax.div(hop, plan.hops)
                line = keeper * plan.owners + owner
                soon = early_lists[line]
                is_soon = (units + hop - first < plan.first) & (soon < plan.soon)
                late_entry = lists[line]
                early_lists[line] = soon + is_soon.astype(jnp.int32)
                lists[line] = late_entry + 1 - is_soon.astype(jnp.int32)
                pos[count * plan.frames + hop] = jnp.where(
                    is_soon, line * plan.soon + soon, -1 - (line * plan.deep + late_entry)
                )

                @pl.when((keeper == row) & (owner == col))
                def _():
                    omap[(hop - keeper * plan.hops) * MAXREQ + slot] = jnp.where(
                        is_soon, soon, plan.soon + late_entry
                    )

                return carry

            lax.fori_loop(first, last, frame, 0)
            return count + 1, units + last - first

        return lax.cond((places[index] < plan.lead) == early, add, lambda carry: carry, carry)

    zero = jnp.int32(0)
    early, units = lax.fori_loop(
        0, live, functools.partial(request, early=True), (zero, zero)
    )
    units = jnp.maximum(units, plan.first)
    count, units = lax.fori_loop(
        0, live, functools.partial(request, early=False), (early, units)
    )
    longest, deepest = [jnp.int32(0)] * 2, jnp.int32(0)
    for i in range(plan.owners):
        longest[i % 2] = jnp.maximum(longest[i % 2], columns[i])
    for i in range(plan.keepers * plan.owners):
        deepest = jnp.maximum(deepest, lists[i])

    def before(index, found):
        return found + (reqs[3, index] - reqs[2, index] + reqs[4, index] <= plan.first).astype(
            jnp.int32
        )

    late = lax.fori_loop(0, early, before, zero)
    meta[0] = columns[col]
    meta[1] = count
    meta[2] = row
    meta[3] = early
    upper = row >= plan.half
    meta[4] = jnp.where(upper, late, 0)
    meta[5] = jnp.where(upper, count, early)
    even, odd = [picked(value - plan.lead, plan.fills) for value in longest]
    pick_a[0] = even * len(plan.fills) + odd
    pick_b[0] = picked(units - plan.first, plan.counts)
    pick_c[0] = picked(deepest, plan.depths)


def make_tables(plan, req_block, req_start, req_frames, req_count):
    total = plan.owners * MAXREQ
    shape = lambda *dims: jax.ShapeDtypeStruct(dims, jnp.int32)
    return pl.pallas_call(
        functools.partial(tables_kernel, plan),
        out_shape=(
            shape(8),
            shape(plan.fill),
            shape(5, total),
            shape(total * plan.frames),
            shape(plan.hops * MAXREQ),
            shape(1),
            shape(1),
            shape(1),
        ),
        in_specs=[SMEM] * 4,
        out_specs=(SMEM,) * 8,
        scratch_shapes=[
            pltpu.SMEM((plan.owners,), jnp.int32),
            pltpu.SMEM((plan.keepers * plan.owners,), jnp.int32),
            pltpu.SMEM((plan.keepers * plan.owners,), jnp.int32),
            pltpu.SMEM((total,), jnp.int32),
            pltpu.SMEM((total,), jnp.int32),
            pltpu.SMEM((plan.frames + 1,), jnp.int32),
        ],
    )(req_block, req_start, req_frames, req_count)


def gather_kernel(plan, meta, chosen, in_ref, out_ref):
    @pl.when(pl.program_id(1) < jnp.maximum(meta[0], 1))
    def _():
        for piece in range(plan.slices):
            out_ref[piece, 0, 0] = in_ref[:, piece * plan.span : (piece + 1) * plan.span, :]


def gather(plan, coarse, meta, chosen):
    def place(i, m):
        return jnp.minimum(i, jnp.maximum(m[0] - 1, 0))

    return pl.pallas_call(
        functools.partial(gather_kernel, plan),
        out_shape=jax.ShapeDtypeStruct(
            (plan.slices, plan.fill, plan.hops, 2, plan.span, BLOCKW), coarse.dtype
        ),
        grid_spec=pltpu.PrefetchScalarGridSpec(
            num_scalar_prefetch=2,
            grid=(plan.hops, plan.fill),
            in_specs=[
                pl.BlockSpec((2, NFINE, BLOCKW), lambda h, i, m, c: (0, h, c[place(i, m)]))
            ],
            out_specs=pl.BlockSpec(
                (plan.slices, 1, 1, 2, plan.span, BLOCKW),
                lambda h, i, m, c: (0, place(i, m), h, 0, 0, 0),
            ),
        ),
    )(meta, chosen, coarse)


def spread_kernel(plan, begin, counts, lifting, *refs):
    common, most = min(counts), max(counts)
    longer = int(counts[1] > counts[0])
    if lifting:
        src, _, code, scale, dst, got, got_scale, tmp, send, recv, local, up, down = refs
    else:
        src, dst, tmp, send, recv, local = refs
    row, col = lax.axis_index("tm"), lax.axis_index("chan")
    base = lax.div(row, plan.half) * plan.half
    me = (row - base) * plan.owners + col
    upper = row >= plan.half
    other = jnp.where(upper, row - plan.half, row + plan.half)
    barrier = pltpu.get_barrier_semaphore()
    size = plan.slices

    def device(index):
        return {"tm": base + lax.div(index, plan.owners), "chan": lax.rem(index, plan.owners)}

    def mask_of(step):
        return lax.rem(step * 7, size)

    @pl.loop(1, size)
    def _(step):
        pl.semaphore_signal(barrier, inc=1, device_id=device(me ^ mask_of(step)))

    if lifting:
        pl.semaphore_signal(barrier, inc=1, device_id={"tm": other})
    pl.semaphore_wait(barrier, size - 1 + int(lifting))

    lifts = []
    if lifting:
        lifts = [
            pltpu.make_async_remote_copy(
                src_ref=source,
                dst_ref=target,
                send_sem=up.at[index],
                recv_sem=down.at[index],
                device_id={"tm": other},
            )
            for index, (source, target) in enumerate([(code, got), (scale, got_scale)])
        ]

        @pl.when(upper)
        def _():
            for copy in lifts:
                copy.start()

    def copy(place, mask, source, target):
        return pltpu.make_async_remote_copy(
            src_ref=src.at[target, begin + place],
            dst_ref=dst.at[source, begin + place],
            send_sem=send.at[place, mask],
            recv_sem=recv.at[place, mask],
            device_id=device(me ^ mask),
        )

    def every(first, last, act):
        @pl.loop(first, last)
        def _(place):
            @pl.loop(1, size)
            def _(step):
                act(place, mask_of(step))

    def begin_send(place, mask):
        copy(place, mask, me, me ^ mask).start()

    def end_send(place, mask):
        copy(place, mask, me, me ^ mask).wait_send()

    def end_recv(place, mask):
        copy(place, mask, me ^ mask, me).wait_recv()

    def more_recv(place, mask):
        @pl.when(lax.rem(me ^ mask, 2) == longer)
        def _():
            end_recv(place, mask)

    def more(act):
        if most > common:

            @pl.when(lax.rem(me, 2) == longer)
            def _():
                every(common, most, act)

    every(0, common, begin_send)
    more(begin_send)
    read = pltpu.make_async_copy(src.at[me, pl.ds(begin, most)], tmp, local.at[0])
    read.start()
    read.wait()
    write = pltpu.make_async_copy(tmp, dst.at[me, pl.ds(begin, most)], local.at[1])
    write.start()
    write.wait()
    every(0, common, end_recv)
    if most > common:
        every(common, most, more_recv)
    every(0, common, end_send)
    more(end_send)

    if lifting:

        @pl.when(upper)
        def _():
            for copy in lifts:
                copy.wait_send()

        @pl.when(jnp.logical_not(upper))
        def _():
            for copy in lifts:
                copy.wait_recv()


def spread(plan, packed, begin, counts, collective, *more):
    sem = pltpu.SemaphoreType.DMA
    lifting = bool(more)
    most = max(counts)
    shape = lambda value: jax.ShapeDtypeStruct(value.shape, value.dtype)
    scratch = [
        pltpu.VMEM((most,) + packed.shape[2:], packed.dtype),
        sem((most, plan.slices)),
        sem((most, plan.slices)),
        sem((2,)),
    ]
    if lifting:
        scratch += [sem((2,)), sem((2,))]
    return pl.pallas_call(
        functools.partial(spread_kernel, plan, begin, counts, lifting),
        out_shape=tuple(shape(value) for value in (more or (packed,))),
        in_specs=[ANY] * (1 + len(more)),
        out_specs=(ANY,) * max(1, len(more)),
        scratch_shapes=scratch,
        input_output_aliases={1: 0} if lifting else {},
        compiler_params=pltpu.CompilerParams(collective_id=collective, has_side_effects=True),
    )(packed, *more)


def partial_sum(plan, upper, hop, w_ref, in_ref, part):
    first = (plan.half * plan.hops if upper else 0) + plan.frames - 1
    total = None
    for index in range(plan.half * plan.hops):
        source, local = divmod(index, plan.hops)
        term = w_ref[first + index - hop] * in_ref[source, 0, 0, local, part].astype(jnp.float32)
        total = term if total is None else total + term
    return total


def encode(parts, out_ref, scale_ref, place, scale_row):
    top = jnp.max(jnp.maximum(jnp.abs(parts[0]), jnp.abs(parts[1])), axis=0, keepdims=True)
    top = jnp.maximum(top, 1e-30)
    factor = TOP / top
    for part in range(2):
        code = jnp.round(parts[part] * factor).astype(jnp.int32)
        out_ref[place, part] = code.astype(jnp.int16)
    scale_ref[pl.ds(scale_row, 1), :] = top * (1.0 / TOP)


def upper_loop(plan, index, begin, low, high, reqs, in_ref, w_ref, out_ref, scale_ref):
    offset = reqs[4, index] - reqs[2, index] - begin

    @pl.loop(low, high)
    def _(hop):
        parts = [partial_sum(plan, True, hop, w_ref, in_ref, part) for part in range(2)]
        encode(parts, out_ref, scale_ref, offset + hop, offset + hop)


def first_kernel(plan, meta, reqs, in_ref, w_ref, out_ref, scale_ref):
    index = pl.program_id(0)

    @pl.when((index < meta[3]) & (meta[2] >= plan.half))
    def _():
        first, last = reqs[2, index], reqs[3, index]
        split = jnp.clip(first + plan.first - reqs[4, index], first, last)
        upper_loop(plan, index, 0, first, split, reqs, in_ref, w_ref, out_ref, scale_ref)


def add_lower(plan, hop, unit, in_ref, w_ref, got_ref, got_scale, out_ref, scale_ref, place, line):
    scale = got_scale[pl.ds(unit, 1), :]
    parts = []
    for part in range(2):
        other = got_ref[unit, part].astype(jnp.int32).astype(jnp.float32) * scale
        parts.append(partial_sum(plan, False, hop, w_ref, in_ref, part) + other)
    encode(parts, out_ref, scale_ref, place, line)


def middle_kernel(
    plan, meta, reqs, pos, in_ref, w_ref, got_ref, got_scale, out_ref, scale_ref, sum_ref, sum_scale
):
    index = pl.program_id(0)
    first, last, offset = reqs[2, index], reqs[3, index], reqs[4, index]
    split = jnp.clip(first + plan.first - offset, first, last)

    @pl.when((index < meta[1]) & (meta[2] >= plan.half))
    def _():
        upper_loop(plan, index, plan.first, split, last, reqs, in_ref, w_ref, out_ref, scale_ref)

    @pl.when((index < meta[3]) & (meta[2] < plan.half))
    def _():
        @pl.loop(first, split)
        def _(hop):
            place = pos[index * plan.frames + hop]

            @pl.when(place >= 0)
            def _():
                line = place + lax.div(place, plan.soon) * (plan.soon_rows - plan.soon)
                unit = offset + hop - first
                add_lower(
                    plan, hop, unit, in_ref, w_ref, got_ref, got_scale, sum_ref, sum_scale, place, line
                )


def lower_kernel(
    plan, meta, reqs, pos, in_ref, w_ref, got_0, scale_0, got_1, scale_1, out_ref, scale_ref
):
    index = pl.program_id(0)

    @pl.when((index < meta[1]) & (meta[2] < plan.half))
    def _():
        first, last, offset = reqs[2, index], reqs[3, index], reqs[4, index]
        split = jnp.clip(first + plan.first - offset, first, last)

        def add(got_ref, got_scale, begin, hop):
            place = -1 - pos[index * plan.frames + hop]

            @pl.when(place >= 0)
            def _():
                unit = offset + hop - first - begin
                add_lower(
                    plan, hop, unit, in_ref, w_ref, got_ref, got_scale, out_ref, scale_ref, place, place
                )

        @pl.loop(first, split)
        def _(hop):
            add(got_0, scale_0, 0, hop)

        @pl.loop(split, last)
        def _(hop):
            add(got_1, scale_1, plan.first, hop)


def filter_specs(plan, low, high):
    def request(i, m):
        bottom = m[low] if low else 0
        return jnp.maximum(jnp.clip(i, bottom, m[high] - 1), 0)

    taps = plan.frames - 1 + plan.all_hops
    return [
        pl.BlockSpec(
            (plan.half, 1, 1, plan.hops, 2, plan.span, BLOCKW),
            lambda i, m, r, *_: (0, r[0, request(i, m)], r[1, request(i, m)], 0, 0, 0, 0),
        ),
        pl.BlockSpec((taps, plan.span, BLOCKW), lambda i, *_: (0, 0, 0)),
    ]


def whole(*dims):
    return pl.BlockSpec(dims, lambda i, *_: (0,) * len(dims))


def coded(units, plan, rows=None):
    return (
        jax.ShapeDtypeStruct((units, 2, plan.span, BLOCKW), jnp.int16),
        jax.ShapeDtypeStruct((rows or units, BLOCKW), jnp.float32),
    )


def wholes(values):
    return [whole(*value.shape) for value in values]


def filter_first(plan, spreaded, weights, meta, reqs):
    outs = coded(plan.first, plan)
    return pl.pallas_call(
        functools.partial(first_kernel, plan),
        out_shape=outs,
        grid_spec=pltpu.PrefetchScalarGridSpec(
            num_scalar_prefetch=2,
            grid=(plan.owners * MAXREQ,),
            in_specs=filter_specs(plan, 0, 3),
            out_specs=tuple(wholes(outs)),
        ),
    )(meta, reqs, spreaded, weights)


def filter_middle(plan, spreaded, weights, got, meta, reqs, pos):
    lines = plan.keepers * plan.owners
    outs = coded(plan.rest, plan) + coded(lines * plan.soon, plan, lines * plan.soon_rows)
    return pl.pallas_call(
        functools.partial(middle_kernel, plan),
        out_shape=outs,
        grid_spec=pltpu.PrefetchScalarGridSpec(
            num_scalar_prefetch=3,
            grid=(plan.owners * MAXREQ,),
            in_specs=filter_specs(plan, 4, 5) + wholes(got),
            out_specs=tuple(wholes(outs)),
        ),
    )(meta, reqs, pos, spreaded, weights, *got)


def filter_lower(plan, spreaded, weights, got, meta, reqs, pos):
    rows = plan.keepers * plan.owners * plan.deep
    return pl.pallas_call(
        functools.partial(lower_kernel, plan),
        out_shape=(
            jax.ShapeDtypeStruct((rows, 2, plan.span, BLOCKW), jnp.int16),
            jax.ShapeDtypeStruct((rows, BLOCKW), jnp.float32),
        ),
        grid_spec=pltpu.PrefetchScalarGridSpec(
            num_scalar_prefetch=3,
            grid=(plan.owners * MAXREQ,),
            in_specs=filter_specs(plan, 0, 1) + [whole(*value.shape) for value in got],
            out_specs=(whole(rows, 2, plan.span, BLOCKW), whole(rows, BLOCKW)),
        ),
    )(meta, reqs, pos, spreaded, weights, *got)


def deliver_kernel(plan, begin, count, lifted, *refs):
    if lifted:
        src, src_scale, code, code_scale, dst, dst_scale, got, got_scale = refs[:8]
        tmp, tmp_scale, send, recv, local, up, down = refs[8:]
    else:
        src, src_scale, _, dst, dst_scale, tmp, tmp_scale, send, recv, local = refs
    row, col = lax.axis_index("tm"), lax.axis_index("chan")
    size, lines = plan.slices, plan.keepers * plan.owners
    me = row * plan.owners + col
    upper = row >= plan.half
    other = jnp.where(upper, row - plan.half, row + plan.half)
    barrier = pltpu.get_barrier_semaphore()
    pieces = [(first, min(3, count - first)) for first in range(0, count, 3)]

    def device(index):
        return {"tm": lax.div(index, plan.owners), "chan": lax.rem(index, plan.owners)}

    def mask_of(step):
        return lax.rem(step * 7, size)

    def value(index, mask, source, target):
        first, extent = pieces[index]
        return pltpu.make_async_remote_copy(
            src_ref=src.at[target, pl.ds(first, extent)],
            dst_ref=dst.at[source, pl.ds(begin + first, extent)],
            send_sem=send.at[index, mask],
            recv_sem=recv.at[index, mask],
            device_id=device(me ^ mask),
        )

    def scale(mask, source, target):
        return pltpu.make_async_remote_copy(
            src_ref=src_scale.at[target],
            dst_ref=dst_scale.at[source],
            send_sem=send.at[len(pieces), mask],
            recv_sem=recv.at[len(pieces), mask],
            device_id=device(me ^ mask),
        )

    lifts = []
    if lifted:
        extent = lifted
        lifts = [
            pltpu.make_async_remote_copy(
                src_ref=source.at[pl.ds(0, extent)],
                dst_ref=target.at[pl.ds(0, extent)],
                send_sem=up.at[index],
                recv_sem=down.at[index],
                device_id={"tm": other},
            )
            for index, (source, target) in enumerate([(code, got), (code_scale, got_scale)])
        ]
        pl.semaphore_signal(barrier, inc=1, device_id={"tm": other})

        @pl.when(upper)
        def _():
            pl.semaphore_wait(barrier, 1)
            for copy in lifts:
                copy.start()
            for copy in lifts:
                copy.wait_send()

    @pl.when(jnp.logical_not(upper))
    def _():
        @pl.loop(1, size)
        def _(step):
            pl.semaphore_signal(barrier, inc=1, device_id=device(me ^ mask_of(step)))

        pl.semaphore_wait(barrier, size - 1 + int(bool(lifted)))

        @pl.loop(1, size)
        def _(step):
            mask = mask_of(step)

            @pl.when((me ^ mask) < lines)
            def _():
                scale(mask, me, me ^ mask).start()

        for index in range(len(pieces)):

            @pl.loop(1, size)
            def _(step):
                mask = mask_of(step)

                @pl.when((me ^ mask) < lines)
                def _():
                    value(index, mask, me, me ^ mask).start()

        @pl.when(me < lines)
        def _():
            moves = [
                (src.at[me, pl.ds(0, count)], tmp, dst.at[me, pl.ds(begin, count)]),
                (src_scale.at[me], tmp_scale, dst_scale.at[me]),
            ]
            for index, (source, middle, target) in enumerate(moves):
                read = pltpu.make_async_copy(source, middle, local.at[2 * index])
                read.start()
                read.wait()
                write = pltpu.make_async_copy(middle, target, local.at[2 * index + 1])
                write.start()
                write.wait()

            @pl.loop(1, size)
            def _(step):
                mask = mask_of(step)
                scale(mask, me ^ mask, me).wait_recv()
                for index in range(len(pieces)):
                    value(index, mask, me ^ mask, me).wait_recv()

        @pl.loop(1, size)
        def _(step):
            mask = mask_of(step)

            @pl.when((me ^ mask) < lines)
            def _():
                scale(mask, me, me ^ mask).wait_send()
                for index in range(len(pieces)):
                    value(index, mask, me, me ^ mask).wait_send()

        for copy in lifts:
            copy.wait_recv()


def deliver(plan, begin, count, lifted, collective, values, scales, *more):
    sem = pltpu.SemaphoreType.DMA
    inner = values.shape[2:]
    pieces = -(-count // 3)
    outs = (
        jax.ShapeDtypeStruct((plan.slices, plan.soon + plan.deep) + inner, values.dtype),
        jax.ShapeDtypeStruct((plan.slices,) + scales.shape[1:], scales.dtype),
    )
    scratch = [
        pltpu.VMEM((count,) + inner, values.dtype),
        pltpu.VMEM(scales.shape[1:], scales.dtype),
        sem((pieces + 1, plan.slices)),
        sem((pieces + 1, plan.slices)),
        sem((4,)),
    ]
    if lifted:
        outs += tuple(jax.ShapeDtypeStruct(value.shape, value.dtype) for value in more)
        scratch += [sem((2,)), sem((2,))]
    return pl.pallas_call(
        functools.partial(deliver_kernel, plan, begin, count, lifted),
        out_shape=outs,
        in_specs=[ANY] * (2 + len(more)),
        out_specs=(ANY,) * len(outs),
        scratch_shapes=scratch,
        input_output_aliases={} if lifted else {2: 0},
        compiler_params=pltpu.CompilerParams(collective_id=collective, has_side_effects=True),
    )(values, scales, *more)


def transform_kernel(plan, omap, in_ref, soon_ref, late_ref, table_ref, turn_ref, out_ref, ys, zs):
    entry = omap[pl.program_id(0)]

    @pl.when(entry < 0)
    def _():
        out_ref[...] = jnp.zeros_like(out_ref)

    @pl.when(entry >= 0)
    def _():
        chunk = 32

        def load(part, first):
            piece, line = divmod(first, plan.span)
            code = in_ref[piece, 0, part, line : line + chunk, :]
            scale = jnp.where(
                entry < plan.soon,
                soon_ref[piece, pl.ds(jnp.minimum(entry, plan.soon - 1), 1), :],
                late_ref[piece, pl.ds(jnp.maximum(entry - plan.soon, 0), 1), :],
            )
            return code.astype(jnp.int32).astype(jnp.float32) * scale

        for line in range(0, SUB, chunk):
            re = [load(0, SUB * a + line) for a in range(RADIX)]
            im = [load(1, SUB * a + line) for a in range(RADIX)]
            es, ed = re[0] + re[2], re[0] - re[2]
            fs, fd = im[0] + im[2], im[0] - im[2]
            gs, gd = re[1] + re[3], re[1] - re[3]
            hs, hd = im[1] + im[3], im[1] - im[3]
            mixed = [
                (es + gs, fs + hs),
                (ed + hd, fd - gd),
                (es - gs, fs - hs),
                (ed - hd, fd + gd),
            ]
            rows = slice(line, line + chunk)
            for q in range(RADIX):
                real, imag = mixed[q]
                if q:
                    cosine, sine = turn_ref[0, q - 1, rows, :], turn_ref[1, q - 1, rows, :]
                    real, imag = real * cosine + imag * sine, imag * cosine - real * sine
                for part, value in enumerate((real, imag)):
                    cols = slice(part * BLOCKW, (part + 1) * BLOCKW)
                    high = value.astype(jnp.bfloat16)
                    ys[q, rows, cols] = high
                    ys[q, SUB + line : SUB + line + chunk, cols] = (
                        value - high.astype(jnp.float32)
                    ).astype(jnp.bfloat16)
                    ys[q, 2 * SUB + line : 2 * SUB + line + chunk, cols] = high

        for q in range(RADIX):
            both = jnp.dot(table_ref[...], ys[q], preferred_element_type=jnp.float32)
            rows = pl.ds(q, SUB, stride=RADIX)
            zs[0, rows, :] = both[:SUB, :BLOCKW] + both[SUB:, BLOCKW:]
            zs[1, rows, :] = both[:SUB, BLOCKW:] - both[SUB:, :BLOCKW]

        out_ref[0, 0] = zs[...].astype(out_ref.dtype)


def transform_tables():
    line = np.arange(SUB)
    angles = (line[:, None] * line[None, :] % SUB) * (2.0 * np.pi / SUB)
    table = np.concatenate([np.cos(angles), np.sin(angles)], axis=0) / math.sqrt(NFINE)
    table = table.astype(np.float32)
    high = table.astype(jnp.bfloat16)
    low = (table - high.astype(np.float32)).astype(jnp.bfloat16)
    turns = np.arange(1, RADIX)[:, None] * line[None, :] * (2.0 * np.pi / NFINE)
    turn = np.stack([np.cos(turns), np.sin(turns)]).astype(np.float32)
    return np.concatenate([high, high, low], axis=1), turn


def transform(plan, values, soon, late, omap):
    table, turn = transform_tables()
    turn = jnp.asarray(np.ascontiguousarray(np.broadcast_to(turn[..., None], turn.shape + (BLOCKW,))))
    return pl.pallas_call(
        functools.partial(transform_kernel, plan),
        out_shape=jax.ShapeDtypeStruct((plan.hops, MAXREQ, 2, NFINE, BLOCKW), jnp.bfloat16),
        grid_spec=pltpu.PrefetchScalarGridSpec(
            num_scalar_prefetch=1,
            grid=(plan.hops * MAXREQ,),
            in_specs=[
                pl.BlockSpec(
                    (plan.slices, 1, 2, plan.span, BLOCKW),
                    lambda i, o: (0, jnp.maximum(o[i], 0), 0, 0, 0),
                ),
                whole(*soon.shape),
                whole(*late.shape),
                whole(2 * SUB, 3 * SUB),
                whole(2, RADIX - 1, SUB, BLOCKW),
            ],
            out_specs=pl.BlockSpec(
                (1, 1, 2, NFINE, BLOCKW), lambda i, o: (i // MAXREQ, i % MAXREQ, 0, 0, 0)
            ),
            scratch_shapes=[
                pltpu.VMEM((RADIX, 3 * SUB, 2 * BLOCKW), jnp.bfloat16),
                pltpu.VMEM((2, NFINE, BLOCKW), jnp.float32),
            ],
        ),
    )(omap, values, soon, late, jnp.asarray(table), turn)


def owners_power(value):
    return value & (value - 1) == 0


class Plan:
    def __init__(self, size, owners, hops, per_column):
        self.size, self.owners, self.hops, self.per_column = size, owners, hops, per_column
        self.all_hops = hops * size
        self.frames = self.all_hops - TAPS + 1
        self.keepers = -(-self.frames // hops)
        self.half = size // 2
        self.slices = self.half * owners
        self.span = NFINE // self.slices
        self.fill = owners * PAIR
        self.deep = round_up(hops * MAXREQ, 8)
        self.lead = min(2, self.fill)
        self.first = 40
        self.rest = round_up(owners * MAXREQ * self.frames, 8)
        more = self.fill - self.lead
        self.fills = sorted({max(1, round_up(more * i, 6) // 6) for i in (1, 2, 3, 4, 6)})
        near = {min(8 * i, self.rest) for i in (1, 2, 3, 4, 5, 7, 9)}
        self.counts = sorted(near | {self.rest})
        most = hops * MAXREQ
        self.soon = min(4, most)
        self.soon_rows = round_up(self.soon, 8)
        self.depths = sorted({round_up(most * i, 12) // 12 for i in (2, 3, 4, 5, 6, 7, 8, 10, 12)})

    def fits(self):
        powers = self.slices & (self.slices - 1) == 0 and owners_power(self.owners)
        even = powers and self.size % 2 == 0 and self.owners % 2 == 0 and NFINE % self.slices == 0 and self.span % 32 == 0
        return even and self.keepers <= self.half


def shards(coarse, prototype, req_block, req_start, req_frames, req_count):
    owners, size = lax.axis_size("chan"), lax.axis_size("tm")
    plan = Plan(size, owners, coarse.shape[1] // NFINE, coarse.shape[2] // BLOCKW)
    if not plan.fits():
        return shards_general(coarse, prototype, req_block, req_start, req_frames, req_count)
    tables = make_tables(plan, req_block, req_start, req_frames, req_count)
    meta, chosen, reqs, pos, omap, pick_a, pick_b, pick_c = tables
    packed = gather(plan, coarse, meta, chosen)

    me = lax.axis_index("tm") % plan.half * owners + lax.axis_index("chan")
    mine = lax.dynamic_slice(prototype, (0, me * plan.span), (TAPS, plan.span))
    mine = jnp.pad(mine, ((plan.frames - 1, plan.all_hops - TAPS), (0, 0)))
    weights = jnp.broadcast_to(mine[:, :, None], mine.shape + (BLOCKW,))

    def split(value):
        return value.reshape((plan.half, owners) + value.shape[1:])

    spreaded = spread(plan, packed, 0, (plan.lead, plan.lead), 0)[0]
    early = filter_first(plan, split(spreaded), weights, meta, reqs)

    def second(count, collective, *operands):
        return spread(plan, operands[0], plan.lead, count, collective, *operands[1:])

    pairs = [(even, odd) for even in plan.fills for odd in plan.fills]
    branches = [functools.partial(second, pair, 1 + i) for i, pair in enumerate(pairs)]
    spreaded, *got = lax.switch(pick_a[0], branches, packed, spreaded, *early)
    spreaded = split(spreaded)
    middle = filter_middle(plan, spreaded, weights, got, meta, reqs, pos)
    lines = plan.keepers * owners

    def by_line(value):
        return value.reshape((lines, value.shape[0] // lines) + value.shape[1:])

    sums = [by_line(value) for value in middle[2:]]
    base = 1 + len(branches)

    def third(extent, collective, *operands):
        return deliver(plan, 0, plan.soon, extent, collective, *operands)

    branches = [functools.partial(third, size, base + i) for i, size in enumerate(plan.counts)]
    values, soon, *more = lax.switch(pick_b[0], branches, *sums, *middle[:2])
    sums = filter_lower(plan, spreaded, weights, list(got) + more, meta, reqs, pos)
    sums = [by_line(value) for value in sums]
    base += len(branches)

    def fourth(count, collective, *operands):
        return deliver(plan, plan.soon, count, 0, collective, *operands)

    branches = [functools.partial(fourth, size, base + i) for i, size in enumerate(plan.depths)]
    values, late = lax.switch(pick_c[0], branches, *sums, values)
    return transform(plan, values, soon, late, omap)[:, None]


def solution(mesh):
    return jax.shard_map(
        shards,
        mesh=mesh,
        in_specs=(P(None, "tm", "chan"), P(), P(), P(), P(), P()),
        out_specs=P("tm", "chan", None, None, None, None),
        check_vma=False,
    )
```
